8 devices in a mesh: fsdp: 8 (over z, y, x, core).
Axes of the slice: x: 2, y: 2, z: 1, core: 2. Of those that a mesh axis runs over, the one named last changes fastest.
Arguments:
- hidden: bfloat16 [8, 1024, 1024], P('fsdp')
- positions: int32 [1024], replicated
- grad_out: bfloat16 [8, 1024, 1024], P('fsdp')
- ln_gain: bfloat16 [2, 1024], P(None, 'fsdp')
- ln_bias: bfloat16 [2, 1024], P(None, 'fsdp')
- w_query: bfloat16 [2, 1024, 16, 64], P(None, 'fsdp')
- b_query: bfloat16 [2, 1024], P(None, 'fsdp')
- w_key: bfloat16 [2, 1024, 16, 64], P(None, 'fsdp')
- b_key: bfloat16 [2, 1024], P(None, 'fsdp')
- w_value: bfloat16 [2, 1024, 16, 64], P(None, 'fsdp')
- b_value: bfloat16 [2, 1024], P(None, 'fsdp')
- w_out: bfloat16 [2, 1024, 1024], P(None, 'fsdp')
- b_out: bfloat16 [2, 1024], P(None, 'fsdp')
- w_up: bfloat16 [2, 1024, 4096], P(None, 'fsdp')
- b_up: bfloat16 [2, 4096], P(None, 'fsdp')
- w_down: bfloat16 [2, 4096, 1024], P(None, 'fsdp')
- b_down: bfloat16 [2, 1024], P(None, 'fsdp')
Outputs:
- output 1: bfloat16 [8, 1024, 1024], P('fsdp')
- output 2: bfloat16 [8, 1024, 1024], P('fsdp')
- output 3: float32 [2, 1024], P(None, 'fsdp')
- output 4: float32 [2, 1024], P(None, 'fsdp')
- output 5: float32 [2, 1024, 16, 64], P(None, 'fsdp')
- output 6: float32 [2, 1024], P(None, 'fsdp')
- output 7: float32 [2, 1024, 16, 64], P(None, 'fsdp')
- output 8: float32 [2, 1024], P(None, 'fsdp')
- output 9: float32 [2, 1024, 16, 64], P(None, 'fsdp')
- output 10: float32 [2, 1024], P(None, 'fsdp')
- output 11: float32 [2, 1024, 1024], P(None, 'fsdp')
- output 12: float32 [2, 1024], P(None, 'fsdp')
- output 13: float32 [2, 1024, 4096], P(None, 'fsdp')
- output 14: float32 [2, 4096], P(None, 'fsdp')
- output 15: float32 [2, 4096, 1024], P(None, 'fsdp')
- output 16: float32 [2, 1024], P(None, 'fsdp')
All inputs are finite; a program needn't handle non-finite values.
Results may differ from the reference program's by a relative error of at most 0.02.
Values are sent between devices in bfloat16 or wider.
A program may use at most 1 GiB of HBM per device.

```python
import jax
import jax.numpy as jnp
from jax import lax

D = 1024
HEADS = 16
HEAD = 64
FF = 4096
ROT = 32
LAYERS = 2
SEQ = 1024
BATCH = 8
LN_EPS = 1e-5
THETA = 10000.0


def rope_tables(positions):
    half_rot = ROT // 2
    inv_freq = THETA ** (-2.0 * jnp.arange(half_rot, dtype=jnp.float32) / ROT)
    angles = positions.astype(jnp.float32)[:, None] * inv_freq[None, :]
    return jnp.cos(angles)[:, None, :], jnp.sin(angles)[:, None, :]


def apply_rope(vectors, cos_t, sin_t):
    half_rot = ROT // 2
    first = vectors[..., :half_rot]
    second = vectors[..., half_rot:ROT]
    return jnp.concatenate([first * cos_t - second * sin_t, second * cos_t + first * sin_t, vectors[..., ROT:]], axis=-1)


def attend_one(qkv_heads):
    q_heads, k_heads, v_heads = qkv_heads
    scores = jnp.einsum('qhk,shk->hqs', q_heads.astype(jnp.float32), k_heads.astype(jnp.float32)) * HEAD ** -0.5
    causal = jnp.arange(SEQ)[:, None] >= jnp.arange(SEQ)[None, :]
    attn_probs = jax.nn.softmax(jnp.where(causal[None, :, :], scores, -1e30), axis=-1).astype(jnp.bfloat16)
    mixed = jnp.einsum('hqs,shk->qhk', attn_probs.astype(jnp.float32), v_heads.astype(jnp.float32))
    return mixed.astype(jnp.bfloat16)


def layer_forward(hidden, weights, cos_t, sin_t):
    (ln_gain, ln_bias, w_query, b_query, w_key, b_key, w_value, b_value, w_out, b_out, w_up, b_up, w_down, b_down) = weights
    n_seqs = hidden.shape[0]
    tokens = hidden.reshape(n_seqs * SEQ, D).astype(jnp.float32)
    centred = tokens - jnp.mean(tokens, axis=-1, keepdims=True)
    variance = jnp.mean(centred * centred, axis=-1, keepdims=True)
    normed = (centred * lax.rsqrt(variance + LN_EPS) * ln_gain.astype(jnp.float32) + ln_bias.astype(jnp.float32)).astype(jnp.bfloat16)

    def project(weight, bias_vec):
        flat = jnp.dot(normed, weight.reshape(D, D), preferred_element_type=jnp.float32) + bias_vec.astype(jnp.float32)
        return flat.reshape(n_seqs, SEQ, HEADS, HEAD)

    q_heads = apply_rope(project(w_query, b_query), cos_t, sin_t).astype(jnp.bfloat16)
    k_heads = apply_rope(project(w_key, b_key), cos_t, sin_t).astype(jnp.bfloat16)
    v_heads = project(w_value, b_value).astype(jnp.bfloat16)
    mixed = lax.map(jax.checkpoint(attend_one), (q_heads, k_heads, v_heads)).reshape(n_seqs * SEQ, D)
    attn_out = jnp.dot(mixed, w_out, preferred_element_type=jnp.float32) + b_out.astype(jnp.float32)
    up_pre = jnp.dot(normed, w_up, preferred_element_type=jnp.float32) + b_up.astype(jnp.float32)
    up_act = jax.nn.gelu(up_pre, approximate=True).astype(jnp.bfloat16)
    mlp_out = jnp.dot(up_act, w_down, preferred_element_type=jnp.float32) + b_down.astype(jnp.float32)
    return (tokens + attn_out + mlp_out).astype(jnp.bfloat16).reshape(n_seqs, SEQ, D)


def setup_inputs(seed: int = 0) -> dict:
    keys = jax.random.split(jax.random.key(seed), 17)
    steps = jax.random.randint(keys[1], (SEQ,), 1, 4)
    positions = (jnp.cumsum(steps) - steps[0]).astype(jnp.int32)

    def matrix(key_id, shape, fan_in):
        return (jax.random.normal(keys[key_id], shape, jnp.float32) * fan_in ** -0.5).astype(jnp.bfloat16)

    def vector(key_id, size, offset, spread):
        return (offset + spread * jax.random.normal(keys[key_id], (LAYERS, size), jnp.float32)).astype(jnp.bfloat16)

    return {
        'hidden': jax.random.normal(keys[0], (BATCH, SEQ, D), jnp.float32).astype(jnp.bfloat16),
        'positions': positions,
        'grad_out': jax.random.normal(keys[2], (BATCH, SEQ, D), jnp.float32).astype(jnp.bfloat16),
        'ln_gain': vector(3, D, 1.0, 0.3),
        'ln_bias': vector(4, D, 0.0, 0.3),
        'w_query': matrix(5, (LAYERS, D, HEADS, HEAD), D),
        'b_query': vector(6, D, 0.0, 0.5),
        'w_key': matrix(7, (LAYERS, D, HEADS, HEAD), D),
        'b_key': vector(8, D, 0.0, 1.0),
        'w_value': matrix(9, (LAYERS, D, HEADS, HEAD), D),
        'b_value': vector(10, D, 0.0, 0.5),
        'w_out': matrix(11, (LAYERS, D, D), D),
        'b_out': vector(12, D, 0.0, 0.3),
        'w_up': matrix(13, (LAYERS, D, FF), D),
        'b_up': vector(14, FF, 0.0, 0.5),
        'w_down': matrix(15, (LAYERS, FF, D), FF),
        'b_down': vector(16, D, 0.0, 0.3),
    }


def reference(hidden, positions, grad_out, ln_gain, ln_bias, w_query, b_query, w_key, b_key, w_value, b_value, w_out, b_out, w_up, b_up, w_down, b_down):
    cos_t, sin_t = rope_tables(positions)

    def stack_forward(weights, first_hidden):
        def body(carry, layer_weights):
            return layer_forward(carry, layer_weights, cos_t, sin_t), None
        return lax.scan(body, first_hidden, weights)[0]

    weights = (ln_gain, ln_bias, w_query, b_query, w_key, b_key, w_value, b_value, w_out, b_out, w_up, b_up, w_down, b_down)
    out_hidden, pullback = jax.vjp(stack_forward, weights, hidden)
    grad_weights, grad_hidden = pullback(grad_out)
    (g_ln_gain, g_ln_bias, g_w_query, g_b_query, g_w_key, g_b_key, g_w_value, g_b_value, g_w_out, g_b_out, g_w_up, g_b_up, g_w_down, g_b_down) = grad_weights
    scale = 1.0 / (hidden.shape[0] * hidden.shape[1])
    return (out_hidden, grad_hidden,
            g_ln_gain.astype(jnp.float32) * scale, g_ln_bias.astype(jnp.float32) * scale,
            g_w_query.astype(jnp.float32) * scale, g_b_query.astype(jnp.float32) * scale,
            g_w_key.astype(jnp.float32) * scale, g_b_key.astype(jnp.float32) * scale,
            g_w_value.astype(jnp.float32) * scale, g_b_value.astype(jnp.float32) * scale,
            g_w_out.astype(jnp.float32) * scale, g_b_out.astype(jnp.float32) * scale,
            g_w_up.astype(jnp.float32) * scale, g_b_up.astype(jnp.float32) * scale,
            g_w_down.astype(jnp.float32) * scale, g_b_down.astype(jnp.float32) * scale)
```

```python
import jax
import jax.numpy as jnp
from jax import lax
from jax.experimental import pallas as pl
from jax.experimental.pallas import tpu as pltpu
from jax.sharding import PartitionSpec as P

ROT = 32
LN_EPS = 1e-5
THETA = 10000.0
AXIS_NAME = 'fsdp'
F32 = jnp.float32
BF16 = jnp.bfloat16
SEQ = 1024
D = 1024
FF = 4096
HEAD = 64
GROUP = 4
GW = GROUP * HEAD
STEPS = 4
QB = 256
VMEM_LIMIT = 60 * 1024 * 1024


def rope_tables(positions):
    half_rot = ROT // 2
    inv_freq = THETA ** (-2.0 * jnp.arange(half_rot, dtype=F32) / ROT)
    angles = positions.astype(F32)[:, None] * inv_freq[None, :]
    cos, sin = jnp.cos(angles), jnp.sin(angles)
    ones = jnp.ones((SEQ, HEAD - ROT), F32)
    zeros = jnp.zeros((SEQ, half_rot), F32)
    wide = jnp.zeros((SEQ, HEAD - ROT), F32)
    keep = jnp.concatenate([cos, cos, ones], axis=1)
    left = jnp.concatenate([-sin, zeros, wide], axis=1)
    right = jnp.concatenate([zeros, sin, wide], axis=1)
    return tuple(jnp.tile(t, (1, GROUP)) for t in (keep, left, right))


def head_mask(head):
    lane = lax.broadcasted_iota(jnp.int32, (1, GW), 1)
    return (lane >= head * HEAD) & (lane < (head + 1) * HEAD)


def causal_mask():
    return lax.broadcasted_iota(jnp.int32, (QB, QB), 0) <= lax.broadcasted_iota(jnp.int32, (QB, QB), 1)


def nt(a, b):
    return lax.dot_general(a, b, (((1,), (1,)), ((), ())), preferred_element_type=F32)


def nn(a, b):
    return lax.dot_general(a, b, (((1,), (0,)), ((), ())), preferred_element_type=F32)


def spin(x, keep, left, right):
    return x * keep + pltpu.roll(x, GW - ROT // 2, 1) * left + pltpu.roll(x, ROT // 2, 1) * right


def unspin(x, keep, left, right):
    return x * keep - pltpu.roll(x, GW - ROT // 2, 1) * left - pltpu.roll(x, ROT // 2, 1) * right


def attn_fwd_kernel(h_ref, w_ref, b_ref, keep_ref, left_ref, right_ref, qkv_ref, mixed_ref, lse_ref):
    h = h_ref[...]
    keep, left, right = keep_ref[...], left_ref[...], right_ref[...]
    q = spin(nn(h, w_ref[:, 0:GW]) + b_ref[:, 0:GW], keep, left, right).astype(BF16)
    qkv_ref[:, 0:GW] = q
    k = spin(nn(h, w_ref[:, GW:2 * GW]) + b_ref[:, GW:2 * GW], keep, left, right).astype(BF16)
    qkv_ref[:, GW:2 * GW] = k
    v = nn(h, w_ref[:, 2 * GW:]) + b_ref[:, 2 * GW:]
    qkv_ref[:, 2 * GW:] = v.astype(BF16)
    v_t = v.T.astype(BF16)
    mask = causal_mask()
    for blk in range(SEQ // QB):
        lo, hi = blk * QB, (blk + 1) * QB
        q_blk = q[lo:hi] * jnp.asarray(HEAD ** -0.5, BF16)
        outs = []
        for head in range(GROUP):
            q_h = jnp.where(head_mask(head), q_blk, jnp.zeros_like(q_blk))
            diag = jnp.where(mask, nt(k[lo:hi], q_h), -1e30)
            top = jnp.max(diag, axis=0, keepdims=True)
            if blk:
                off = nt(k[:lo], q_h)
                top = jnp.maximum(top, jnp.max(off, axis=0, keepdims=True))
            e_diag = jnp.exp(diag - top)
            total = jnp.sum(e_diag, axis=0, keepdims=True)
            if blk:
                e_off = jnp.exp(off - top)
                total = total + jnp.sum(e_off, axis=0, keepdims=True)
            inv = 1.0 / total
            rows = slice(head * HEAD, (head + 1) * HEAD)
            out = nn(v_t[rows, lo:hi], (e_diag * inv).astype(BF16))
            if blk:
                out = out + nn(v_t[rows, :lo], (e_off * inv).astype(BF16))
            outs.append(out)
            lse_ref[0, head:head + 1, lo:hi] = top + jnp.log(total)
        mixed_ref[lo:hi, :] = jnp.concatenate(outs, axis=0).T.astype(BF16)


def attn_fwd(h, w_qkv, b_qkv, tables):
    full = pl.BlockSpec((SEQ, D), lambda i: (0, 0))
    table = pl.BlockSpec((SEQ, GW), lambda i: (0, 0))
    return pl.pallas_call(
        attn_fwd_kernel,
        grid=(STEPS,),
        in_specs=[full, pl.BlockSpec((D, 3 * GW), lambda i: (0, i)), pl.BlockSpec((1, 3 * GW), lambda i: (0, i)), table, table, table],
        out_specs=[pl.BlockSpec((SEQ, 3 * GW), lambda i: (0, i)), pl.BlockSpec((SEQ, GW), lambda i: (0, i)), pl.BlockSpec((1, 8, SEQ), lambda i: (i, 0, 0))],
        out_shape=[jax.ShapeDtypeStruct((SEQ, 3 * D), BF16), jax.ShapeDtypeStruct((SEQ, D), BF16), jax.ShapeDtypeStruct((STEPS, 8, SEQ), F32)],
        compiler_params=pltpu.CompilerParams(vmem_limit_bytes=VMEM_LIMIT),
        cost_estimate=pl.CostEstimate(flops=20_000_000_000, bytes_accessed=20_000_000, transcendentals=10_000_000),
        name='attn_fwd',
    )(h, w_qkv, b_qkv, *tables)


def attn_bwd_kernel(qkv_ref, go_ref, lse_ref, keep_ref, left_ref, right_ref, g_ref, bias_ref, dq_acc, dk_acc, dv_acc):
    q, k, v = qkv_ref[:, 0:GW], qkv_ref[:, GW:2 * GW], qkv_ref[:, 2 * GW:]
    k_t = k.astype(F32).T.astype(BF16)
    dk_acc[...] = jnp.zeros_like(dk_acc)
    dv_acc[...] = jnp.zeros_like(dv_acc)
    mask = causal_mask()
    scale = HEAD ** -0.5
    for blk in range(SEQ // QB):
        lo, hi = blk * QB, (blk + 1) * QB
        q_blk = q[lo:hi]
        go_blk = go_ref[lo:hi, :]
        probs, scores, q_heads, go_heads, dq_t = [], [], [], [], []
        for head in range(GROUP):
            keep_lanes = head_mask(head)
            q_h = jnp.where(keep_lanes, q_blk, jnp.zeros_like(q_blk))
            go_h = jnp.where(keep_lanes, go_blk, jnp.zeros_like(go_blk))
            lse = lse_ref[0, head:head + 1, lo:hi]
            q_s = q_h * jnp.asarray(scale, BF16)
            p = jnp.where(mask, jnp.exp(nt(k[lo:hi], q_s) - lse), 0.0)
            dp = nt(v[lo:hi], go_h)
            delta = jnp.sum(p * dp, axis=0, keepdims=True)
            if blk:
                p_off = jnp.exp(nt(k[:lo], q_s) - lse)
                dp_off = nt(v[:lo], go_h)
                delta = delta + jnp.sum(p_off * dp_off, axis=0, keepdims=True)
            ds = ((p * (dp - delta)) * scale).astype(BF16)
            p = p.astype(BF16)
            if blk:
                ds = jnp.concatenate([((p_off * (dp_off - delta)) * scale).astype(BF16), ds], axis=0)
                p = jnp.concatenate([p_off.astype(BF16), p], axis=0)
            probs.append(p)
            scores.append(ds)
            q_heads.append(q_h)
            go_heads.append(go_h)
            dq_t.append(nn(k_t[head * HEAD:(head + 1) * HEAD, :hi], ds))
        dv_acc[:hi, :] += nn(jnp.concatenate(probs, axis=1), jnp.concatenate(go_heads, axis=0))
        dk_acc[:hi, :] += nn(jnp.concatenate(scores, axis=1), jnp.concatenate(q_heads, axis=0))
        dq_acc[lo:hi, :] = jnp.concatenate(dq_t, axis=0).T
    keep, left, right = keep_ref[...], left_ref[...], right_ref[...]
    sums = []
    for pos, grad in enumerate((unspin(dq_acc[...], keep, left, right), unspin(dk_acc[...], keep, left, right), dv_acc[...])):
        g_ref[:, pos * GW:(pos + 1) * GW] = grad.astype(BF16)
        sums.append(jnp.sum(grad, axis=0, keepdims=True))
    bias_ref[...] = jnp.concatenate([jnp.concatenate(sums, axis=1), jnp.zeros((7, 3 * GW), F32)], axis=0)


def attn_bwd(qkv, grad_mixed, lse, tables):
    wide = pl.BlockSpec((SEQ, 3 * GW), lambda i: (0, i))
    table = pl.BlockSpec((SEQ, GW), lambda i: (0, 0))
    return pl.pallas_call(
        attn_bwd_kernel,
        grid=(STEPS,),
        in_specs=[wide, pl.BlockSpec((SEQ, GW), lambda i: (0, i)), pl.BlockSpec((1, 8, SEQ), lambda i: (i, 0, 0)), table, table, table],
        out_specs=[wide, pl.BlockSpec((8, 3 * GW), lambda i: (0, i))],
        out_shape=[jax.ShapeDtypeStruct((SEQ, 3 * D), BF16), jax.ShapeDtypeStruct((8, 3 * D), F32)],
        scratch_shapes=[pltpu.VMEM((SEQ, GW), F32)] * 3,
        compiler_params=pltpu.CompilerParams(vmem_limit_bytes=VMEM_LIMIT),
        cost_estimate=pl.CostEstimate(flops=50_000_000_000, bytes_accessed=20_000_000, transcendentals=10_000_000),
        name='attn_bwd',
    )(qkv, grad_mixed, lse, *tables)


def wgrad_rows_kernel(core_ref, lhs_ref, lhs2_ref, rhs_ref, rhs2_ref, out_ref):
    out_ref[...] = nn(lhs_ref[...].T, rhs_ref[...]) + nn(lhs2_ref[...].T, rhs2_ref[...])


def wgrad_rows(core, lhs, lhs2, rhs, rhs2):
    tile = 256
    lhs_spec = pl.BlockSpec((SEQ, tile), lambda i, c: (0, (i // 2) * 4 + c[0] * 2 + i % 2))
    rhs_spec = pl.BlockSpec((SEQ, D), lambda i, c: (0, 0))
    return pl.pallas_call(
        wgrad_rows_kernel,
        grid_spec=pltpu.PrefetchScalarGridSpec(
            num_scalar_prefetch=1,
            grid=(FF // 2 // tile,),
            in_specs=[lhs_spec, lhs_spec, rhs_spec, rhs_spec],
            out_specs=pl.BlockSpec((tile, D), lambda i, c: (i, 0)),
        ),
        out_shape=jax.ShapeDtypeStruct((FF // 2, D), F32),
        compiler_params=pltpu.CompilerParams(vmem_limit_bytes=VMEM_LIMIT),
        cost_estimate=pl.CostEstimate(flops=2 * FF * D * SEQ, bytes_accessed=20_000_000, transcendentals=0),
        name='wgrad_rows',
    )(core, lhs, lhs2, rhs, rhs2)


def wgrad_up_kernel(lhs_ref, lhs2_ref, rhs_ref, rhs2_ref, out_ref, left):
    @pl.when(pl.program_id(0) == 0)
    def _():
        left[:, :SEQ] = lhs_ref[...].T
        left[:, SEQ:] = lhs2_ref[...].T

    out_ref[...] = nn(left[:, :SEQ], rhs_ref[...]) + nn(left[:, SEQ:], rhs2_ref[...])


def wgrad_up(lhs, lhs2, rhs, rhs2):
    tile = 512
    lhs_spec = pl.BlockSpec((SEQ, D // 2), lambda i: (0, 0))
    rhs_spec = pl.BlockSpec((SEQ, tile), lambda i: (0, i))
    return pl.pallas_call(
        wgrad_up_kernel,
        grid=(FF // tile,),
        in_specs=[lhs_spec, lhs_spec, rhs_spec, rhs_spec],
        out_specs=pl.BlockSpec((D // 2, tile), lambda i: (0, i)),
        out_shape=jax.ShapeDtypeStruct((D // 2, FF), F32),
        scratch_shapes=[pltpu.VMEM((D // 2, 2 * SEQ), BF16)],
        compiler_params=pltpu.CompilerParams(vmem_limit_bytes=VMEM_LIMIT),
        cost_estimate=pl.CostEstimate(flops=2 * FF * D * SEQ, bytes_accessed=26_000_000, transcendentals=0),
        name='wgrad_up',
    )(lhs, lhs2, rhs, rhs2)


def wgrad_qkvo_kernel(h_ref, h2_ref, mix_ref, mix2_ref, g_ref, g2_ref, tok_ref, tok2_ref, out_ref, left):
    step = pl.program_id(0)

    @pl.when(step == 0)
    def _():
        left[:, :SEQ] = h_ref[...].T
        left[:, SEQ:] = h2_ref[...].T

    @pl.when(step < 6)
    def _():
        out_ref[...] = nn(left[:, :SEQ], g_ref[...]) + nn(left[:, SEQ:], g2_ref[...])

    @pl.when(step == 6)
    def _():
        left[:, :SEQ] = mix_ref[...].T
        left[:, SEQ:] = mix2_ref[...].T

    @pl.when(step >= 6)
    def _():
        out_ref[...] = nn(left[:, :SEQ], tok_ref[...]) + nn(left[:, SEQ:], tok2_ref[...])


def wgrad_qkvo(h, h2, mix, mix2, g, g2, tok, tok2):
    tile = 512
    lhs_spec = pl.BlockSpec((SEQ, D // 2), lambda i: (0, 0))
    g_spec = pl.BlockSpec((SEQ, tile), lambda i: (0, jnp.minimum(i, 5)))
    tok_spec = pl.BlockSpec((SEQ, tile), lambda i: (0, jnp.maximum(i - 6, 0)))
    return pl.pallas_call(
        wgrad_qkvo_kernel,
        grid=(8,),
        in_specs=[lhs_spec] * 4 + [g_spec, g_spec, tok_spec, tok_spec],
        out_specs=pl.BlockSpec((D // 2, tile), lambda i: (0, i)),
        out_shape=jax.ShapeDtypeStruct((D // 2, 4 * D), F32),
        scratch_shapes=[pltpu.VMEM((D // 2, 2 * SEQ), BF16)],
        compiler_params=pltpu.CompilerParams(vmem_limit_bytes=VMEM_LIMIT),
        cost_estimate=pl.CostEstimate(flops=2 * FF * D * SEQ, bytes_accessed=26_000_000, transcendentals=0),
        name='wgrad_qkvo',
    )(h, h2, mix, mix2, g, g2, tok, tok2)


def gelu_tanh(values):
    return jax.nn.gelu(values, approximate=True)


def layer_norm(hidden, gain, bias):
    tok = hidden.astype(F32)
    centred = tok - jnp.mean(tok, axis=-1, keepdims=True)
    inv_std = lax.rsqrt(jnp.mean(centred * centred, axis=-1, keepdims=True) + LN_EPS)
    normed = centred * inv_std
    return normed, inv_std, (normed * gain + bias).astype(BF16)


def interleave(parts):
    return jnp.concatenate([p[:, i * GW:(i + 1) * GW] for i in range(STEPS) for p in parts], axis=1)


def pick_columns(values, core):
    return lax.dynamic_index_in_dim(values.reshape(SEQ, 4, 2, 128), core, 2, keepdims=False).reshape(SEQ, 512)


def solution(mesh):
    group_size = mesh.shape[AXIS_NAME]
    batch_spec = P(AXIS_NAME)
    param_specs = (P(None, AXIS_NAME),) * 14
    swap = [(i, i ^ 1) for i in range(group_size)]
    chips = [[i for i in range(group_size) if i % 2 == c] for c in range(2)]

    def exchange(values):
        return lax.ppermute(values, AXIS_NAME, swap)

    def gather(values):
        return lax.all_gather(values, AXIS_NAME, axis=0, tiled=True)

    def scatter(values):
        return lax.psum_scatter(values, AXIS_NAME, scatter_dimension=0, axis_index_groups=chips, tiled=True)

    def step(hidden, positions, grad_out, *shards):
        (ln_gain, ln_bias, w_query, b_query, w_key, b_key, w_value, b_value, w_out, b_out, w_up, b_up, w_down, b_down) = shards
        layers = ln_gain.shape[0]
        token_total = hidden.shape[0] * hidden.shape[1] * group_size
        rank = lax.axis_index(AXIS_NAME)
        core = lax.rem(rank, 2)
        core_arr = core.reshape(1).astype(jnp.int32)
        tables = rope_tables(positions)

        wide, down = [], []
        for layer in range(layers):
            flat = [w[layer].reshape(w.shape[1], D) for w in (w_query, w_key, w_value)]
            wide.append(gather(jnp.concatenate([interleave(flat), w_up[layer], w_out[layer]], axis=1)))
            down.append(gather(w_down[layer]))

        small = jnp.concatenate([b.reshape(layers, -1) for b in (ln_gain, ln_bias, b_query, b_key, b_value, b_out, b_down, b_up)], axis=1)
        small = gather(small[None])

        current = hidden.reshape(SEQ, D)
        saved = []
        for layer in range(layers):
            mine = small[:, layer]
            (gain, lbias, bq, bk, bv, bo, bd) = [mine[:, i * 128:(i + 1) * 128].reshape(1, D).astype(F32) for i in range(7)]
            bu = mine[:, 7 * 128:].reshape(1, FF).astype(F32)
            weights = wide[layer]
            wqkv, wup, wout, wdown = weights[:, :3 * D], weights[:, 3 * D:3 * D + FF], weights[:, 3 * D + FF:], down[layer]
            normed, inv_std, h = layer_norm(current, gain, lbias)
            up_pre = nn(h, wup) + bu
            act = gelu_tanh(up_pre).astype(BF16)
            qkv, mixed, lse = attn_fwd(h, wqkv, interleave((bq, bk, bv)), tables)
            new = current.astype(F32) + nn(mixed, wout) + bo + nn(act, wdown) + bd
            saved.append((gain, wqkv, wup, wout, wdown, normed, inv_std, h, up_pre, act, qkv, mixed, lse))
            current = new.astype(BF16)

        grad = grad_out.reshape(SEQ, D)
        big, little = [None] * layers, [None] * layers
        for layer in reversed(range(layers)):
            (gain, wqkv, wup, wout, wdown, normed, inv_std, h, up_pre, act, qkv, mixed, lse) = saved[layer]
            grad2 = exchange(grad)
            act2 = exchange(act)
            h2 = exchange(pick_columns(h, 1 - core))
            mixed2 = exchange(pick_columns(mixed, 1 - core))
            h1 = pick_columns(h, core)
            grad_f32 = grad.astype(F32)
            rs_down = scatter(wgrad_rows(core_arr, act, act2, grad, grad2))
            grad_act = nt(grad, wdown).astype(BF16)
            grad_pre = jax.vjp(gelu_tanh, up_pre)[1](grad_act.astype(F32))[0]
            g_b_up = jnp.sum(grad_pre, axis=0)
            grad_pre = grad_pre.astype(BF16)
            rs_up = scatter(wgrad_up(h1, h2, grad_pre, exchange(grad_pre)))
            grad_mixed = nt(grad, wout).astype(BF16)
            g_qkv, g_bias = attn_bwd(qkv, grad_mixed, lse, tables)
            rs_qkvo = scatter(wgrad_qkvo(h1, h2, pick_columns(mixed, core), mixed2, g_qkv, exchange(g_qkv), grad, grad2))
            grad_normed = nt(g_qkv, wqkv) + nt(grad_pre, wup)
            g_gain = jnp.sum(grad_normed * normed, axis=0)
            g_lbias = jnp.sum(grad_normed, axis=0)
            grad_hat = grad_normed * gain
            grad_in = inv_std * (grad_hat - jnp.mean(grad_hat, axis=-1, keepdims=True) - normed * jnp.mean(grad_hat * normed, axis=-1, keepdims=True))
            g_bias = g_bias[0].reshape(STEPS, 3, GW)
            pieces = [g_gain, g_lbias] + [g_bias[:, i].reshape(D) for i in range(3)] + [jnp.sum(grad_f32, axis=0)]
            little[layer] = jnp.concatenate([p.reshape(8, 128) for p in pieces] + [g_b_up.reshape(8, 512)], axis=1)
            big[layer] = (rs_down, rs_up, rs_qkvo)
            grad = (grad_f32 + grad_in).astype(BF16)

        scale = 1.0 / token_total
        everyone = gather(jnp.stack(little, axis=1)[None])
        own = jnp.sum(lax.dynamic_index_in_dim(everyone, rank, 1, keepdims=False), axis=0) * scale
        vec = [own[:, i * 128:(i + 1) * 128] for i in range(6)]

        def stacked(slot, view):
            return jnp.stack([view(big[layer][slot]) * scale for layer in range(layers)])

        def heads(pos):
            def view(rs):
                cols = [rs[:, i * 3 * GW + pos * GW:i * 3 * GW + (pos + 1) * GW] for i in range(STEPS)]
                return jnp.concatenate(cols, axis=1).reshape(-1, 16, HEAD)
            return stacked(2, view)

        return (current.reshape(hidden.shape), grad.reshape(hidden.shape), vec[0], vec[1],
                heads(0), vec[2], heads(1), vec[3], heads(2), vec[4],
                stacked(2, lambda rs: rs[:, 3 * D:]), vec[5],
                stacked(1, lambda rs: rs), own[:, 6 * 128:], stacked(0, lambda rs: rs), vec[5])

    return jax.shard_map(step, mesh=mesh, in_specs=(batch_spec, P(), batch_spec) + param_specs, out_specs=(batch_spec, batch_spec) + param_specs, check_vma=False)
```

```python
import functools

import jax
import jax.numpy as jnp
from jax import lax
from jax.experimental import pallas as pl
from jax.experimental.pallas import tpu as pltpu
from jax.sharding import PartitionSpec as P

ROT = 32
LN_EPS = 1e-5
THETA = 10000.0
AXIS_NAME = 'fsdp'
F32 = jnp.float32
BF16 = jnp.bfloat16
SEQ = 1024
D = 1024
FF = 4096
HEAD = 64
GROUP = 4
GW = GROUP * HEAD
STEPS = 4
QB = 256
VMEM_LIMIT = 60 * 1024 * 1024


def rope_tables(positions):
    half_rot = ROT // 2
    inv_freq = THETA ** (-2.0 * jnp.arange(half_rot, dtype=F32) / ROT)
    angles = positions.astype(F32)[:, None] * inv_freq[None, :]
    cos, sin = jnp.cos(angles), jnp.sin(angles)
    ones = jnp.ones((SEQ, HEAD - ROT), F32)
    zeros = jnp.zeros((SEQ, half_rot), F32)
    wide = jnp.zeros((SEQ, HEAD - ROT), F32)
    keep = jnp.concatenate([cos, cos, ones], axis=1)
    left = jnp.concatenate([-sin, zeros, wide], axis=1)
    right = jnp.concatenate([zeros, sin, wide], axis=1)
    return tuple(jnp.tile(t, (1, GROUP)) for t in (keep, left, right))


def head_mask(head):
    lane = lax.broadcasted_iota(jnp.int32, (1, GW), 1)
    return (lane >= head * HEAD) & (lane < (head + 1) * HEAD)


def causal_mask():
    return lax.broadcasted_iota(jnp.int32, (QB, QB), 0) <= lax.broadcasted_iota(jnp.int32, (QB, QB), 1)


def nt(a, b):
    return lax.dot_general(a, b, (((1,), (1,)), ((), ())), preferred_element_type=F32)


def nn(a, b):
    return lax.dot_general(a, b, (((1,), (0,)), ((), ())), preferred_element_type=F32)


def spin(x, keep, left, right):
    return x * keep + pltpu.roll(x, GW - ROT // 2, 1) * left + pltpu.roll(x, ROT // 2, 1) * right


def unspin(x, keep, left, right):
    return x * keep - pltpu.roll(x, GW - ROT // 2, 1) * left - pltpu.roll(x, ROT // 2, 1) * right


def attn_fwd_kernel(h_ref, wq_ref, wk_ref, wv_ref, bq_ref, bk_ref, bv_ref, keep_ref, left_ref, right_ref, qkv_ref, mixed_ref, lse_ref):
    h = h_ref[...]
    keep, left, right = keep_ref[...], left_ref[...], right_ref[...]
    q = spin(nn(h, wq_ref[...]) + bq_ref[...], keep, left, right).astype(BF16)
    qkv_ref[0] = q
    k = spin(nn(h, wk_ref[...]) + bk_ref[...], keep, left, right).astype(BF16)
    qkv_ref[1] = k
    v = nn(h, wv_ref[...]) + bv_ref[...]
    qkv_ref[2] = v.astype(BF16)
    v_t = v.T.astype(BF16)
    mask = causal_mask()
    for blk in range(SEQ // QB):
        lo, hi = blk * QB, (blk + 1) * QB
        q_blk = q[lo:hi] * jnp.asarray(HEAD ** -0.5, BF16)
        outs = []
        for head in range(GROUP):
            q_h = jnp.where(head_mask(head), q_blk, jnp.zeros_like(q_blk))
            diag = jnp.where(mask, nt(k[lo:hi], q_h), -1e30)
            top = jnp.max(diag, axis=0, keepdims=True)
            if blk:
                off = nt(k[:lo], q_h)
                top = jnp.maximum(top, jnp.max(off, axis=0, keepdims=True))
            e_diag = jnp.exp(diag - top)
            total = jnp.sum(e_diag, axis=0, keepdims=True)
            if blk:
                e_off = jnp.exp(off - top)
                total = total + jnp.sum(e_off, axis=0, keepdims=True)
            inv = 1.0 / total
            rows = slice(head * HEAD, (head + 1) * HEAD)
            out = nn(v_t[rows, lo:hi], (e_diag * inv).astype(BF16))
            if blk:
                out = out + nn(v_t[rows, :lo], (e_off * inv).astype(BF16))
            outs.append(out)
            lse_ref[0, head:head + 1, lo:hi] = top + jnp.log(total)
        mixed_ref[lo:hi, :] = jnp.concatenate(outs, axis=0).T.astype(BF16)


def attn_fwd(h, weights, biases, tables):
    full = pl.BlockSpec((SEQ, D), lambda i: (0, 0))
    table = pl.BlockSpec((SEQ, GW), lambda i: (0, 0))
    w_specs = [pl.BlockSpec((D, GW), lambda i, pos=pos: (0, pos * STEPS + i)) for pos in range(3)]
    b_spec = pl.BlockSpec((1, GW), lambda i: (0, i))
    return pl.pallas_call(
        attn_fwd_kernel,
        grid=(STEPS,),
        in_specs=[full] + w_specs + [b_spec] * 3 + [table] * 3,
        out_specs=[pl.BlockSpec((3, SEQ, GW), lambda i: (0, 0, i)), pl.BlockSpec((SEQ, GW), lambda i: (0, i)), pl.BlockSpec((1, 8, SEQ), lambda i: (i, 0, 0))],
        out_shape=[jax.ShapeDtypeStruct((3, SEQ, D), BF16), jax.ShapeDtypeStruct((SEQ, D), BF16), jax.ShapeDtypeStruct((STEPS, 8, SEQ), F32)],
        compiler_params=pltpu.CompilerParams(vmem_limit_bytes=VMEM_LIMIT),
        cost_estimate=pl.CostEstimate(flops=20_000_000_000, bytes_accessed=20_000_000, transcendentals=10_000_000),
        name='attn_fwd',
    )(h, weights, weights, weights, *biases, *tables)


def attn_bwd_kernel(qkv_ref, go_ref, lse_ref, keep_ref, left_ref, right_ref, g_ref, bias_ref, dq_acc, dk_acc, dv_acc):
    q, k, v = qkv_ref[0], qkv_ref[1], qkv_ref[2]
    k_t = k.astype(F32).T.astype(BF16)
    dk_acc[...] = jnp.zeros_like(dk_acc)
    dv_acc[...] = jnp.zeros_like(dv_acc)
    mask = causal_mask()
    scale = HEAD ** -0.5
    for blk in range(SEQ // QB):
        lo, hi = blk * QB, (blk + 1) * QB
        q_blk = q[lo:hi]
        go_blk = go_ref[lo:hi, :]
        probs, scores, q_heads, go_heads, dq_t = [], [], [], [], []
        for head in range(GROUP):
            keep_lanes = head_mask(head)
            q_h = jnp.where(keep_lanes, q_blk, jnp.zeros_like(q_blk))
            go_h = jnp.where(keep_lanes, go_blk, jnp.zeros_like(go_blk))
            lse = lse_ref[0, head:head + 1, lo:hi]
            q_s = q_h * jnp.asarray(scale, BF16)
            p = jnp.where(mask, jnp.exp(nt(k[lo:hi], q_s) - lse), 0.0)
            dp = nt(v[lo:hi], go_h)
            delta = jnp.sum(p * dp, axis=0, keepdims=True)
            if blk:
                p_off = jnp.exp(nt(k[:lo], q_s) - lse)
                dp_off = nt(v[:lo], go_h)
                delta = delta + jnp.sum(p_off * dp_off, axis=0, keepdims=True)
            ds = ((p * (dp - delta)) * scale).astype(BF16)
            p = p.astype(BF16)
            if blk:
                ds = jnp.concatenate([((p_off * (dp_off - delta)) * scale).astype(BF16), ds], axis=0)
                p = jnp.concatenate([p_off.astype(BF16), p], axis=0)
            probs.append(p)
            scores.append(ds)
            q_heads.append(q_h)
            go_heads.append(go_h)
            dq_t.append(nn(k_t[head * HEAD:(head + 1) * HEAD, :hi], ds))
        dv_acc[:hi, :] += nn(jnp.concatenate(probs, axis=1), jnp.concatenate(go_heads, axis=0))
        dk_acc[:hi, :] += nn(jnp.concatenate(scores, axis=1), jnp.concatenate(q_heads, axis=0))
        dq_acc[lo:hi, :] = jnp.concatenate(dq_t, axis=0).T
    keep, left, right = keep_ref[...], left_ref[...], right_ref[...]
    sums = []
    for pos, grad in enumerate((unspin(dq_acc[...], keep, left, right), unspin(dk_acc[...], keep, left, right), dv_acc[...])):
        g_ref[pos] = grad.astype(BF16)
        sums.append(jnp.sum(grad, axis=0, keepdims=True))
    bias_ref[...] = jnp.concatenate([jnp.concatenate(sums, axis=1), jnp.zeros((7, 3 * GW), F32)], axis=0)


def attn_bwd(qkv, grad_mixed, lse, tables):
    wide = pl.BlockSpec((3, SEQ, GW), lambda i: (0, 0, i))
    table = pl.BlockSpec((SEQ, GW), lambda i: (0, 0))
    return pl.pallas_call(
        attn_bwd_kernel,
        grid=(STEPS,),
        in_specs=[wide, pl.BlockSpec((SEQ, GW), lambda i: (0, i)), pl.BlockSpec((1, 8, SEQ), lambda i: (i, 0, 0)), table, table, table],
        out_specs=[wide, pl.BlockSpec((8, 3 * GW), lambda i: (0, i))],
        out_shape=[jax.ShapeDtypeStruct((3, SEQ, D), BF16), jax.ShapeDtypeStruct((8, 3 * D), F32)],
        scratch_shapes=[pltpu.VMEM((SEQ, GW), F32)] * 3,
        compiler_params=pltpu.CompilerParams(vmem_limit_bytes=VMEM_LIMIT),
        cost_estimate=pl.CostEstimate(flops=50_000_000_000, bytes_accessed=20_000_000, transcendentals=10_000_000),
        name='attn_bwd',
    )(qkv, grad_mixed, lse, *tables)


def wgrad_rows_kernel(core_ref, lhs_ref, lhs2_ref, rhs_ref, rhs2_ref, out_ref):
    out_ref[...] = nn(lhs_ref[...].T, rhs_ref[...]) + nn(lhs2_ref[...].T, rhs2_ref[...])


def wgrad_rows(core, lhs, lhs2, rhs, rhs2):
    tile = 256
    lhs_spec = pl.BlockSpec((SEQ, tile), lambda i, c: (0, (i // 2) * 4 + c[0] * 2 + i % 2))
    rhs_spec = pl.BlockSpec((SEQ, D), lambda i, c: (0, 0))
    return pl.pallas_call(
        wgrad_rows_kernel,
        grid_spec=pltpu.PrefetchScalarGridSpec(
            num_scalar_prefetch=1,
            grid=(FF // 2 // tile,),
            in_specs=[lhs_spec, lhs_spec, rhs_spec, rhs_spec],
            out_specs=pl.BlockSpec((tile, D), lambda i, c: (i, 0)),
        ),
        out_shape=jax.ShapeDtypeStruct((FF // 2, D), F32),
        compiler_params=pltpu.CompilerParams(vmem_limit_bytes=VMEM_LIMIT),
        cost_estimate=pl.CostEstimate(flops=2 * FF * D * SEQ, bytes_accessed=20_000_000, transcendentals=0),
        name='wgrad_rows',
    )(core, lhs, lhs2, rhs, rhs2)


TILE = 512


def segment_tiles(rhs):
    return rhs.size // (SEQ * TILE)


def wgrad_cols_kernel(plan, *refs):
    lefts = sorted({p[0] for p in plan}, reverse=False)
    n_left = 8 * len(lefts)
    rhs_refs = refs[1 + n_left:1 + n_left + 2 * len(plan)]
    out_ref, left = refs[-2], refs[-1]
    step = pl.program_id(0)
    loaded = None
    for seg, (which, first, last) in enumerate(plan):
        if which != loaded:
            blocks = refs[1 + 8 * lefts.index(which):1 + 8 * lefts.index(which) + 8]
            loaded = which

            @pl.when(step == first)
            def _(blocks=blocks):
                for j in range(4):
                    left[128 * j:128 * (j + 1), :SEQ] = blocks[j][...].T
                    left[128 * j:128 * (j + 1), SEQ:] = blocks[4 + j][...].T

        here, there = rhs_refs[2 * seg], rhs_refs[2 * seg + 1]

        @pl.when((step >= first) & (step < last))
        def _(here=here, there=there):
            a, b = (here[0], there[0]) if len(here.shape) == 3 else (here[...], there[...])
            out_ref[...] = nn(left[:, :SEQ], a) + nn(left[:, SEQ:], b)


def wgrad_cols(core, lefts, segments):
    plan, specs, args, first = [], [], [], 0
    for mine, partner in lefts:
        for values in (mine, partner):
            for j in range(4):
                specs.append(pl.BlockSpec((SEQ, 128), lambda i, c, j=j: (0, 2 * j + c[0])))
                args.append(values)
    for which, mine, partner in segments:
        tiles = segment_tiles(mine)

        def place(i, c, first=first, tiles=tiles, deep=mine.ndim == 3):
            pos = jnp.clip(i - first, 0, tiles - 1)
            return (pos // 2, 0, pos % 2) if deep else (0, pos)

        shape = (1, SEQ, TILE) if mine.ndim == 3 else (SEQ, TILE)
        specs += [pl.BlockSpec(shape, place)] * 2
        args += [mine, partner]
        plan.append((which, first, first + tiles))
        first += tiles
    return pl.pallas_call(
        functools.partial(wgrad_cols_kernel, tuple(plan)),
        grid_spec=pltpu.PrefetchScalarGridSpec(
            num_scalar_prefetch=1,
            grid=(first,),
            in_specs=specs,
            out_specs=pl.BlockSpec((D // 2, TILE), lambda i, c: (0, i)),
            scratch_shapes=[pltpu.VMEM((D // 2, 2 * SEQ), BF16)],
        ),
        out_shape=jax.ShapeDtypeStruct((D // 2, first * TILE), F32),
        compiler_params=pltpu.CompilerParams(vmem_limit_bytes=VMEM_LIMIT),
        cost_estimate=pl.CostEstimate(flops=2 * SEQ * D * first * TILE, bytes_accessed=3_200_000 * first, transcendentals=0),
        name='wgrad_cols',
    )(core, *args)


def gelu_tanh(values):
    return jax.nn.gelu(values, approximate=True)


def layer_norm(hidden, gain, bias):
    tok = hidden.astype(F32)
    centred = tok - jnp.mean(tok, axis=-1, keepdims=True)
    inv_std = lax.rsqrt(jnp.mean(centred * centred, axis=-1, keepdims=True) + LN_EPS)
    normed = centred * inv_std
    return normed, inv_std, (normed * gain + bias).astype(BF16)


def bar(*values):
    return lax.optimization_barrier(values)


def solution(mesh):
    group_size = mesh.shape[AXIS_NAME]
    batch_spec = P(AXIS_NAME)
    param_specs = (P(None, AXIS_NAME),) * 14
    swap = [(i, i ^ 1) for i in range(group_size)]
    chips = [[i for i in range(group_size) if i % 2 == c] for c in range(2)]

    def exchange(values):
        return lax.ppermute(values, AXIS_NAME, swap)

    def gather(values):
        return lax.all_gather(values, AXIS_NAME, axis=0, tiled=True)

    def scatter(values):
        return lax.psum_scatter(values, AXIS_NAME, scatter_dimension=0, axis_index_groups=chips, tiled=True)

    def step(hidden, positions, grad_out, *shards):
        (ln_gain, ln_bias, w_query, b_query, w_key, b_key, w_value, b_value, w_out, b_out, w_up, b_up, w_down, b_down) = shards
        layers = ln_gain.shape[0]
        token_total = hidden.shape[0] * hidden.shape[1] * group_size
        rank = lax.axis_index(AXIS_NAME)
        core = lax.rem(rank, 2)
        core_arr = core.reshape(1).astype(jnp.int32)
        tables = rope_tables(positions)

        wide, down = [], []
        sources = (w_query, w_key, w_value, w_up, w_out)
        for layer in range(layers):
            joined = jnp.concatenate([w[layer].reshape(w.shape[1], -1) for w in sources], axis=1)
            if layer == 0:
                joined, *sources = bar(joined, *sources)
            wide.append(gather(joined))
            down.append(gather(w_down[layer]))

        small = jnp.concatenate([b.reshape(layers, -1) for b in (ln_gain, ln_bias, b_query, b_key, b_value, b_out, b_down, b_up)], axis=1)
        small = gather(small[None])

        def split(layer):
            mine = small[:, layer]
            vecs = [mine[:, i * 128:(i + 1) * 128].reshape(1, D).astype(F32) for i in range(7)]
            return vecs + [mine[:, 7 * 128:].reshape(1, FF).astype(F32)]

        def mlp_up(h, wup, bu):
            up_pre = nn(h, wup) + bu
            return up_pre, gelu_tanh(up_pre).astype(BF16)

        def finish(current, mixed, wout, bo, act, wdown, bd):
            return (current.astype(F32) + nn(mixed, wout) + bo + nn(act, wdown) + bd).astype(BF16)

        def mlp_pull(grad, wdown, up_pre):
            grad_act = nt(grad, wdown).astype(BF16)
            grad_pre = jax.vjp(gelu_tanh, up_pre)[1](grad_act.astype(F32))[0]
            return grad_pre.astype(BF16), jnp.sum(grad_pre, axis=0)

        def norm_pull(grad, grad_normed, normed, inv_std, gain):
            grad_hat = grad_normed * gain
            grad_in = inv_std * (grad_hat - jnp.mean(grad_hat, axis=-1, keepdims=True) - normed * jnp.mean(grad_hat * normed, axis=-1, keepdims=True))
            return (grad.astype(F32) + grad_in).astype(BF16), jnp.sum(grad_normed * normed, axis=0), jnp.sum(grad_normed, axis=0)

        def back_qkv(g, weights):
            return sum(nt(g[pos], weights[:, pos * D:(pos + 1) * D]) for pos in range(3))

        def pack(g_gain, g_lbias, g_bias, grad, g_b_up):
            g_bias = g_bias[0].reshape(STEPS, 3, GW)
            pieces = [g_gain, g_lbias] + [g_bias[:, i].reshape(D) for i in range(3)] + [jnp.sum(grad.astype(F32), axis=0)]
            return jnp.concatenate([p.reshape(8, 128) for p in pieces] + [g_b_up.reshape(8, 512)], axis=1)

        up_cols, out_cols = slice(3 * D, 3 * D + FF), slice(3 * D + FF, None)

        x0 = hidden.reshape(SEQ, D)
        gain0, lbias0, bq, bk, bv, bo, bd, bu = split(0)
        normed0, inv0, h0 = layer_norm(x0, gain0, lbias0)
        qkv0, mixed0, lse0 = attn_fwd(h0, wide[0], (bq, bk, bv), tables)
        up_pre0, act0 = mlp_up(h0, wide[0][:, up_cols], bu)
        x1 = finish(x0, mixed0, wide[0][:, out_cols], bo, act0, down[0], bd)
        h0x, act0x, mixed0x = exchange(h0), exchange(act0), exchange(mixed0)

        top = grad_out.reshape(SEQ, D)
        topx = exchange(top)
        gain1, lbias1, bq, bk, bv, bo1, bd1, bu = split(1)
        normed1, inv1, h1 = layer_norm(x1, gain1, lbias1)
        up_pre1, act1 = mlp_up(h1, wide[1][:, up_cols], bu)
        h1x, act1x = exchange(h1), exchange(act1)
        dw, top_a = bar(wgrad_rows(core_arr, act1, act1x, top, topx), top)
        rs_down1 = scatter(dw)
        pre1, g_bup1 = mlp_pull(top_a, down[1], up_pre1)
        pre1x = exchange(pre1)
        pre1_a, h1_a = bar(pre1, h1)
        qkv1, mixed1, lse1 = attn_fwd(h1_a, wide[1], (bq, bk, bv), tables)
        mixed1x = exchange(mixed1)
        mixed1_a, pre1_b = bar(mixed1, pre1_a)
        dw, top_b = bar(wgrad_cols(core_arr, [(h1, h1x)], [(0, pre1_b, pre1x)]), top_a)
        rs_up1 = scatter(dw)
        g1, g_bias1 = attn_bwd(qkv1, nt(top_b, wide[1][:, out_cols]).astype(BF16), lse1, tables)
        g1x = exchange(g1)
        g1_a, pre1_c = bar(g1, pre1_b)
        back1 = nt(pre1_c, wide[1][:, up_cols])
        g1_b, back1 = bar(g1_a, back1)
        dw, g1_c = bar(wgrad_cols(core_arr, [(h1, h1x), (mixed1_a, mixed1x)], [(0, g1_b, g1x), (1, top, topx)]), g1_b)
        rs_qkvo1 = scatter(dw)
        mid, g_gain, g_lbias = norm_pull(top, back1 + back_qkv(g1_c, wide[1]), normed1, inv1, gain1)
        little1 = pack(g_gain, g_lbias, g_bias1, top, g_bup1)

        midx = exchange(mid)
        pre0, g_bup0 = mlp_pull(mid, down[0], up_pre0)
        pre0x = exchange(pre0)
        pre0_a, mid_a = bar(pre0, mid)
        dw, mid_b = bar(wgrad_rows(core_arr, act0, act0x, mid_a, midx), mid_a)
        rs_down0 = scatter(dw)
        g0, g_bias0 = attn_bwd(qkv0, nt(mid_b, wide[0][:, out_cols]).astype(BF16), lse0, tables)
        g0x = exchange(g0)
        g0_a, pre0_b = bar(g0, pre0_a)
        back0 = nt(pre0_b, wide[0][:, up_cols])
        g0_b, back0 = bar(g0_a, back0)
        dw = wgrad_cols(core_arr, [(h0, h0x), (mixed0, mixed0x)], [(0, g0_b, g0x), (0, pre0_b, pre0x), (1, mid_b, midx)])
        dw, g0_c, mixed1_b, act1_b = bar(dw, g0_b, mixed1_a, act1)
        rs_wide0 = scatter(dw)
        grad, g_gain, g_lbias = norm_pull(mid, back0 + back_qkv(g0_c, wide[0]), normed0, inv0, gain0)
        little0 = pack(g_gain, g_lbias, g_bias0, mid, g_bup0)
        current = finish(x1, mixed1_b, wide[1][:, out_cols], bo1, act1_b, down[1], bd1)
        little = [little0, little1]

        scale = 1.0 / token_total
        everyone = gather(jnp.stack(little, axis=1)[None])
        own = jnp.sum(lax.dynamic_index_in_dim(everyone, rank, 1, keepdims=False), axis=0) * scale
        vec = [own[:, i * 128:(i + 1) * 128] for i in range(6)]

        def stacked(first, second):
            return jnp.stack([first * scale, second * scale])

        def heads(pos):
            cols = slice(pos * D, (pos + 1) * D)
            return stacked(rs_wide0[:, cols].reshape(-1, 16, HEAD), rs_qkvo1[:, cols].reshape(-1, 16, HEAD))

        return (current.reshape(hidden.shape), grad.reshape(hidden.shape), vec[0], vec[1],
                heads(0), vec[2], heads(1), vec[3], heads(2), vec[4],
                stacked(rs_wide0[:, out_cols], rs_qkvo1[:, 3 * D:]), vec[5],
                stacked(rs_wide0[:, up_cols], rs_up1), own[:, 6 * 128:], stacked(rs_down0, rs_down1), vec[5])

    return jax.shard_map(step, mesh=mesh, in_specs=(batch_spec, P(), batch_spec) + param_specs, out_specs=(batch_spec, batch_spec) + param_specs, check_vma=False)
```

```python
import functools

import jax
import jax.numpy as jnp
from jax import lax
from jax.experimental import pallas as pl
from jax.experimental.pallas import tpu as pltpu
from jax.sharding import PartitionSpec as P


ROT = 32
LN_EPS = 1e-5
THETA = 10000.0
AXIS_NAME = 'fsdp'
F32 = jnp.float32
BF16 = jnp.bfloat16
SEQ = 1024
D = 1024
FF = 4096
HEAD = 64
GROUP = 4
GW = GROUP * HEAD
STEPS = 4
QB = 256
VMEM_LIMIT = 60 * 1024 * 1024


def rope_tables(positions):
    half_rot = ROT // 2
    inv_freq = THETA ** (-2.0 * jnp.arange(half_rot, dtype=F32) / ROT)
    angles = positions.astype(F32)[:, None] * inv_freq[None, :]
    cos, sin = jnp.cos(angles), jnp.sin(angles)
    ones = jnp.ones((SEQ, HEAD - ROT), F32)
    zeros = jnp.zeros((SEQ, half_rot), F32)
    wide = jnp.zeros((SEQ, HEAD - ROT), F32)
    keep = jnp.concatenate([cos, cos, ones], axis=1)
    left = jnp.concatenate([-sin, zeros, wide], axis=1)
    right = jnp.concatenate([zeros, sin, wide], axis=1)
    return tuple(jnp.tile(t, (1, GROUP)) for t in (keep, left, right))


def head_mask(head):
    lane = lax.broadcasted_iota(jnp.int32, (1, GW), 1)
    return (lane >= head * HEAD) & (lane < (head + 1) * HEAD)


def causal_mask():
    return lax.broadcasted_iota(jnp.int32, (QB, QB), 0) <= lax.broadcasted_iota(jnp.int32, (QB, QB), 1)


def nt(a, b):
    return lax.dot_general(a, b, (((1,), (1,)), ((), ())), preferred_element_type=F32)


def nn(a, b):
    return lax.dot_general(a, b, (((1,), (0,)), ((), ())), preferred_element_type=F32)


def spin(x, keep, left, right):
    return x * keep + pltpu.roll(x, GW - ROT // 2, 1) * left + pltpu.roll(x, ROT // 2, 1) * right


def unspin(x, keep, left, right):
    return x * keep - pltpu.roll(x, GW - ROT // 2, 1) * left - pltpu.roll(x, ROT // 2, 1) * right


def attn_fwd_kernel(h_ref, wq_ref, wk_ref, wv_ref, bq_ref, bk_ref, bv_ref, keep_ref, left_ref, right_ref, qkv_ref, mixed_ref, lse_ref):
    h = h_ref[...]
    keep, left, right = keep_ref[...], left_ref[...], right_ref[...]
    q = spin(nn(h, wq_ref[...]) + bq_ref[...], keep, left, right).astype(BF16)
    qkv_ref[0] = q
    k = spin(nn(h, wk_ref[...]) + bk_ref[...], keep, left, right).astype(BF16)
    qkv_ref[1] = k
    v = nn(h, wv_ref[...]) + bv_ref[...]
    qkv_ref[2] = v.astype(BF16)
    v_t = v.T.astype(BF16)
    mask = causal_mask()
    for blk in range(SEQ // QB):
        lo, hi = blk * QB, (blk + 1) * QB
        q_blk = q[lo:hi] * jnp.asarray(HEAD ** -0.5, BF16)
        outs = []
        for head in range(GROUP):
            q_h = jnp.where(head_mask(head), q_blk, jnp.zeros_like(q_blk))
            diag = jnp.where(mask, nt(k[lo:hi], q_h), -1e30)
            top = jnp.max(diag, axis=0, keepdims=True)
            if blk:
                off = nt(k[:lo], q_h)
                top = jnp.maximum(top, jnp.max(off, axis=0, keepdims=True))
            e_diag = jnp.exp(diag - top)
            total = jnp.sum(e_diag, axis=0, keepdims=True)
            if blk:
                e_off = jnp.exp(off - top)
                total = total + jnp.sum(e_off, axis=0, keepdims=True)
            inv = 1.0 / total
            rows = slice(head * HEAD, (head + 1) * HEAD)
            out = nn(v_t[rows, lo:hi], (e_diag * inv).astype(BF16))
            if blk:
                out = out + nn(v_t[rows, :lo], (e_off * inv).astype(BF16))
            outs.append(out)
            lse_ref[0, head:head + 1, lo:hi] = top + jnp.log(total)
        mixed_ref[lo:hi, :] = jnp.concatenate(outs, axis=0).T.astype(BF16)


def attn_fwd(h, weights, biases, tables):
    full = pl.BlockSpec((SEQ, D), lambda i: (0, 0))
    table = pl.BlockSpec((SEQ, GW), lambda i: (0, 0))
    w_specs = [pl.BlockSpec((D, GW), lambda i, pos=pos: (0, pos * STEPS + i)) for pos in range(3)]
    b_spec = pl.BlockSpec((1, GW), lambda i: (0, i))
    return pl.pallas_call(
        attn_fwd_kernel,
        grid=(STEPS,),
        in_specs=[full] + w_specs + [b_spec] * 3 + [table] * 3,
        out_specs=[pl.BlockSpec((3, SEQ, GW), lambda i: (0, 0, i)), pl.BlockSpec((SEQ, GW), lambda i: (0, i)), pl.BlockSpec((1, 8, SEQ), lambda i: (i, 0, 0))],
        out_shape=[jax.ShapeDtypeStruct((3, SEQ, D), BF16), jax.ShapeDtypeStruct((SEQ, D), BF16), jax.ShapeDtypeStruct((STEPS, 8, SEQ), F32)],
        compiler_params=pltpu.CompilerParams(vmem_limit_bytes=VMEM_LIMIT),
        cost_estimate=pl.CostEstimate(flops=20_000_000_000, bytes_accessed=20_000_000, transcendentals=10_000_000),
        name='attn_fwd',
    )(h, weights, weights, weights, *biases, *tables)


def attn_bwd_kernel(qkv_ref, go_ref, lse_ref, keep_ref, left_ref, right_ref, g_ref, bias_ref, dq_acc, dk_acc, dv_acc):
    q, k, v = qkv_ref[0], qkv_ref[1], qkv_ref[2]
    k_t = k.astype(F32).T.astype(BF16)
    dk_acc[...] = jnp.zeros_like(dk_acc)
    dv_acc[...] = jnp.zeros_like(dv_acc)
    mask = causal_mask()
    scale = HEAD ** -0.5
    for blk in range(SEQ // QB):
        lo, hi = blk * QB, (blk + 1) * QB
        q_blk = q[lo:hi]
        go_blk = go_ref[lo:hi, :]
        probs, scores, q_heads, go_heads, dq_t = [], [], [], [], []
        for head in range(GROUP):
            keep_lanes = head_mask(head)
            q_h = jnp.where(keep_lanes, q_blk, jnp.zeros_like(q_blk))
            go_h = jnp.where(keep_lanes, go_blk, jnp.zeros_like(go_blk))
            lse = lse_ref[0, head:head + 1, lo:hi]
            q_s = q_h * jnp.asarray(scale, BF16)
            p = jnp.where(mask, jnp.exp(nt(k[lo:hi], q_s) - lse), 0.0)
            dp = nt(v[lo:hi], go_h)
            delta = jnp.sum(p * dp, axis=0, keepdims=True)
            if blk:
                p_off = jnp.exp(nt(k[:lo], q_s) - lse)
                dp_off = nt(v[:lo], go_h)
                delta = delta + jnp.sum(p_off * dp_off, axis=0, keepdims=True)
            ds = ((p * (dp - delta)) * scale).astype(BF16)
            p = p.astype(BF16)
            if blk:
                ds = jnp.concatenate([((p_off * (dp_off - delta)) * scale).astype(BF16), ds], axis=0)
                p = jnp.concatenate([p_off.astype(BF16), p], axis=0)
            probs.append(p)
            scores.append(ds)
            q_heads.append(q_h)
            go_heads.append(go_h)
            dq_t.append(nn(k_t[head * HEAD:(head + 1) * HEAD, :hi], ds))
        dv_acc[:hi, :] += nn(jnp.concatenate(probs, axis=1), jnp.concatenate(go_heads, axis=0))
        dk_acc[:hi, :] += nn(jnp.concatenate(scores, axis=1), jnp.concatenate(q_heads, axis=0))
        dq_acc[lo:hi, :] = jnp.concatenate(dq_t, axis=0).T
    keep, left, right = keep_ref[...], left_ref[...], right_ref[...]
    sums = []
    for pos, grad in enumerate((unspin(dq_acc[...], keep, left, right), unspin(dk_acc[...], keep, left, right), dv_acc[...])):
        g_ref[pos] = grad.astype(BF16)
        sums.append(jnp.sum(grad, axis=0, keepdims=True))
    bias_ref[...] = jnp.concatenate([jnp.concatenate(sums, axis=1), jnp.zeros((7, 3 * GW), F32)], axis=0)


def attn_bwd(qkv, grad_mixed, lse, tables):
    wide = pl.BlockSpec((3, SEQ, GW), lambda i: (0, 0, i))
    table = pl.BlockSpec((SEQ, GW), lambda i: (0, 0))
    return pl.pallas_call(
        attn_bwd_kernel,
        grid=(STEPS,),
        in_specs=[wide, pl.BlockSpec((SEQ, GW), lambda i: (0, i)), pl.BlockSpec((1, 8, SEQ), lambda i: (i, 0, 0)), table, table, table],
        out_specs=[wide, pl.BlockSpec((8, 3 * GW), lambda i: (0, i))],
        out_shape=[jax.ShapeDtypeStruct((3, SEQ, D), BF16), jax.ShapeDtypeStruct((8, 3 * D), F32)],
        scratch_shapes=[pltpu.VMEM((SEQ, GW), F32)] * 3,
        compiler_params=pltpu.CompilerParams(vmem_limit_bytes=VMEM_LIMIT),
        cost_estimate=pl.CostEstimate(flops=50_000_000_000, bytes_accessed=20_000_000, transcendentals=10_000_000),
        name='attn_bwd',
    )(qkv, grad_mixed, lse, *tables)


def wgrad_rows_kernel(core_ref, lhs_ref, lhs2_ref, rhs_ref, rhs2_ref, out_ref):
    out_ref[...] = nn(lhs_ref[...].T, rhs_ref[...]) + nn(lhs2_ref[...].T, rhs2_ref[...])


def wgrad_rows(core, lhs, lhs2, rhs, rhs2):
    tile = 256
    lhs_spec = pl.BlockSpec((SEQ, tile), lambda i, c: (0, (i // 2) * 4 + c[0] * 2 + i % 2))
    rhs_spec = pl.BlockSpec((SEQ, D), lambda i, c: (0, 0))
    return pl.pallas_call(
        wgrad_rows_kernel,
        grid_spec=pltpu.PrefetchScalarGridSpec(
            num_scalar_prefetch=1,
            grid=(FF // 2 // tile,),
            in_specs=[lhs_spec, lhs_spec, rhs_spec, rhs_spec],
            out_specs=pl.BlockSpec((tile, D), lambda i, c: (i, 0)),
        ),
        out_shape=jax.ShapeDtypeStruct((FF // 2, D), F32),
        compiler_params=pltpu.CompilerParams(vmem_limit_bytes=VMEM_LIMIT),
        cost_estimate=pl.CostEstimate(flops=2 * FF * D * SEQ, bytes_accessed=20_000_000, transcendentals=0),
        name='wgrad_rows',
    )(core, lhs, lhs2, rhs, rhs2)


TILE = 512


def segment_tiles(rhs):
    return rhs.size // (SEQ * TILE)


def wgrad_cols_kernel(plan, *refs):
    lefts = sorted({p[0] for p in plan}, reverse=False)
    n_left = 8 * len(lefts)
    rhs_refs = refs[1 + n_left:1 + n_left + 2 * len(plan)]
    out_ref, left = refs[-2], refs[-1]
    step = pl.program_id(0)
    loaded = None
    for seg, (which, first, last) in enumerate(plan):
        if which != loaded:
            blocks = refs[1 + 8 * lefts.index(which):1 + 8 * lefts.index(which) + 8]
            loaded = which

            @pl.when(step == first)
            def _(blocks=blocks):
                for j in range(4):
                    left[128 * j:128 * (j + 1), :SEQ] = blocks[j][...].T
                    left[128 * j:128 * (j + 1), SEQ:] = blocks[4 + j][...].T

        here, there = rhs_refs[2 * seg], rhs_refs[2 * seg + 1]

        @pl.when((step >= first) & (step < last))
        def _(here=here, there=there):
            a, b = (here[0], there[0]) if len(here.shape) == 3 else (here[...], there[...])
            out_ref[...] = nn(left[:, :SEQ], a) + nn(left[:, SEQ:], b)


def wgrad_cols(core, lefts, segments):
    plan, specs, args, first = [], [], [], 0
    for mine, partner in lefts:
        for values in (mine, partner):
            for j in range(4):
                specs.append(pl.BlockSpec((SEQ, 128), lambda i, c, j=j: (0, 2 * j + c[0])))
                args.append(values)
    for which, mine, partner in segments:
        tiles = segment_tiles(mine)

        def place(i, c, first=first, tiles=tiles, deep=mine.ndim == 3):
            pos = jnp.clip(i - first, 0, tiles - 1)
            return (pos // 2, 0, pos % 2) if deep else (0, pos)

        shape = (1, SEQ, TILE) if mine.ndim == 3 else (SEQ, TILE)
        specs += [pl.BlockSpec(shape, place)] * 2
        args += [mine, partner]
        plan.append((which, first, first + tiles))
        first += tiles
    return pl.pallas_call(
        functools.partial(wgrad_cols_kernel, tuple(plan)),
        grid_spec=pltpu.PrefetchScalarGridSpec(
            num_scalar_prefetch=1,
            grid=(first,),
            in_specs=specs,
            out_specs=pl.BlockSpec((D // 2, TILE), lambda i, c: (0, i)),
            scratch_shapes=[pltpu.VMEM((D // 2, 2 * SEQ), BF16)],
        ),
        out_shape=jax.ShapeDtypeStruct((D // 2, first * TILE), F32),
        compiler_params=pltpu.CompilerParams(vmem_limit_bytes=VMEM_LIMIT),
        cost_estimate=pl.CostEstimate(flops=2 * SEQ * D * first * TILE, bytes_accessed=3_200_000 * first, transcendentals=0),
        name='wgrad_cols',
    )(core, *args)


def gelu_tanh(values):
    return jax.nn.gelu(values, approximate=True)


def layer_norm(hidden, gain, bias):
    tok = hidden.astype(F32)
    centred = tok - jnp.mean(tok, axis=-1, keepdims=True)
    inv_std = lax.rsqrt(jnp.mean(centred * centred, axis=-1, keepdims=True) + LN_EPS)
    normed = centred * inv_std
    return normed, inv_std, (normed * gain + bias).astype(BF16)


def bar(*values):
    return lax.optimization_barrier(values)


def solution(mesh):
    group_size = mesh.shape[AXIS_NAME]
    batch_spec = P(AXIS_NAME)
    param_specs = (P(None, AXIS_NAME),) * 14
    swap = [(i, i ^ 1) for i in range(group_size)]
    chips = [[i for i in range(group_size) if i % 2 == c] for c in range(2)]

    def exchange(values):
        return lax.ppermute(values, AXIS_NAME, swap)

    def hop(values, offset):
        return lax.ppermute(values, AXIS_NAME, [(i, i ^ offset) for i in range(group_size)])

    def gather(values):
        return lax.all_gather(values, AXIS_NAME, axis=0, tiled=True)

    def scatter(values):
        return lax.psum_scatter(values, AXIS_NAME, scatter_dimension=0, axis_index_groups=chips, tiled=True)

    def step(hidden, positions, grad_out, *shards):
        (ln_gain, ln_bias, w_query, b_query, w_key, b_key, w_value, b_value, w_out, b_out, w_up, b_up, w_down, b_down) = shards
        layers = ln_gain.shape[0]
        token_total = hidden.shape[0] * hidden.shape[1] * group_size
        rank = lax.axis_index(AXIS_NAME)
        core = lax.rem(rank, 2)
        core_arr = core.reshape(1).astype(jnp.int32)
        tables = rope_tables(positions)

        def rows(w, layer):
            return w[layer].reshape(w.shape[1], -1)

        def gather_down(shard):
            half = shard.shape[0] // 2
            first, second = shard[:half], shard[half:]
            first_x, first_y = hop(first, 2), hop(first, 4)
            second_y, second_x = hop(second, 4), hop(second, 2)
            pieces = {0: (first, second), 2: (first_x, second_x), 4: (first_y, second_y), 6: (hop(first_x, 4), hop(second_y, 2))}
            same = jnp.zeros((4,) + shard.shape, shard.dtype)
            for offset, pair in pieces.items():
                slot = lax.bitwise_xor(rank, offset) // 2
                for pos, piece in enumerate(pair):
                    same = lax.dynamic_update_slice(same, piece[None], (slot, pos * half, 0))
            other = exchange(same)
            mine = (jnp.arange(2) == core)[None, :, None, None]
            return jnp.where(mine, same[:, None], other[:, None]).reshape(8 * shard.shape[0], shard.shape[1])

        wide0 = gather(jnp.concatenate([rows(w, 0) for w in (w_query, w_key, w_value, w_up, w_out)], axis=1))
        down0 = gather_down(w_down[0])
        up1 = gather(w_up[1])
        qkvo1 = gather(jnp.concatenate([rows(w, 1) for w in (w_query, w_key, w_value, w_out)], axis=1))

        small = jnp.concatenate([b.reshape(layers, -1) for b in (ln_gain, ln_bias, b_query, b_key, b_value, b_out, b_down, b_up)], axis=1)
        small = gather(small[None])

        def split(layer):
            mine = small[:, layer]
            vecs = [mine[:, i * 128:(i + 1) * 128].reshape(1, D).astype(F32) for i in range(7)]
            return vecs + [mine[:, 7 * 128:].reshape(1, FF).astype(F32)]

        def mlp_up(h, wup, bu):
            up_pre = nn(h, wup) + bu
            return up_pre, gelu_tanh(up_pre).astype(BF16)

        def finish(current, mixed, wout, bo, act, wdown, bd):
            return (current.astype(F32) + nn(mixed, wout) + bo + nn(act, wdown) + bd).astype(BF16)

        def mlp_pull(grad, wdown, up_pre):
            grad_act = nt(grad, wdown).astype(BF16)
            grad_pre = jax.vjp(gelu_tanh, up_pre)[1](grad_act.astype(F32))[0]
            return grad_pre.astype(BF16), jnp.sum(grad_pre, axis=0)

        def norm_pull(grad, grad_normed, normed, inv_std, gain):
            grad_hat = grad_normed * gain
            grad_in = inv_std * (grad_hat - jnp.mean(grad_hat, axis=-1, keepdims=True) - normed * jnp.mean(grad_hat * normed, axis=-1, keepdims=True))
            return (grad.astype(F32) + grad_in).astype(BF16), jnp.sum(grad_normed * normed, axis=0), jnp.sum(grad_normed, axis=0)

        def back_qkv(g, weights):
            return sum(nt(g[pos], weights[:, pos * D:(pos + 1) * D]) for pos in range(3))

        def pack(g_gain, g_lbias, g_bias, grad, g_b_up):
            g_bias = g_bias[0].reshape(STEPS, 3, GW)
            pieces = [g_gain, g_lbias] + [g_bias[:, i].reshape(D) for i in range(3)] + [jnp.sum(grad.astype(F32), axis=0)]
            return jnp.concatenate([p.reshape(8, 128) for p in pieces] + [g_b_up.reshape(8, 512)], axis=1)

        up_cols, out_cols = slice(3 * D, 3 * D + FF), slice(3 * D + FF, None)

        x0 = hidden.reshape(SEQ, D)
        gain0, lbias0, bq, bk, bv, bo, bd, bu = split(0)
        normed0, inv0, h0 = layer_norm(x0, gain0, lbias0)
        shard1, wide0 = bar(w_down[1], wide0)
        down1 = gather_down(shard1)
        qkv0, mixed0, lse0 = attn_fwd(h0, wide0, (bq, bk, bv), tables)
        up_pre0, act0 = mlp_up(h0, wide0[:, up_cols], bu)
        x1 = finish(x0, mixed0, wide0[:, out_cols], bo, act0, down0, bd)
        h0x, act0x, mixed0x = exchange(h0), exchange(act0), exchange(mixed0)

        top = grad_out.reshape(SEQ, D)
        topx = exchange(top)
        gain1, lbias1, bq, bk, bv, bo1, bd1, bu = split(1)
        normed1, inv1, h1 = layer_norm(x1, gain1, lbias1)
        up_pre1, act1 = mlp_up(h1, up1, bu)
        h1x, act1x = exchange(h1), exchange(act1)
        pre1, g_bup1 = mlp_pull(top, down1, up_pre1)
        pre1x = exchange(pre1)
        pre1_a, top_a = bar(pre1, top)
        dw, pre1_b = bar(wgrad_rows(core_arr, act1, act1x, top_a, topx), pre1_a)
        rs_down1 = scatter(dw)
        dw, h1_a, top_b = bar(wgrad_cols(core_arr, [(h1, h1x)], [(0, pre1_b, pre1x)]), h1, top_a)
        rs_up1 = scatter(dw)
        qkv1, mixed1, lse1 = attn_fwd(h1_a, qkvo1, (bq, bk, bv), tables)
        mixed1x = exchange(mixed1)
        g1, g_bias1 = attn_bwd(qkv1, nt(top_b, qkvo1[:, 3 * D:]).astype(BF16), lse1, tables)
        g1x = exchange(g1)
        g1_a, pre1_c = bar(g1, pre1_b)
        back1 = nt(pre1_c, up1)
        g1_b, back1 = bar(g1_a, back1)
        dw, g1_c = bar(wgrad_cols(core_arr, [(h1, h1x), (mixed1, mixed1x)], [(0, g1_b, g1x), (1, top, topx)]), g1_b)
        rs_qkvo1 = scatter(dw)
        mid, g_gain, g_lbias = norm_pull(top, back1 + back_qkv(g1_c, qkvo1), normed1, inv1, gain1)
        little1 = pack(g_gain, g_lbias, g_bias1, top, g_bup1)

        midx = exchange(mid)
        pre0, g_bup0 = mlp_pull(mid, down0, up_pre0)
        pre0x = exchange(pre0)
        pre0_a, mid_a = bar(pre0, mid)
        dw, mid_b = bar(wgrad_rows(core_arr, act0, act0x, mid_a, midx), mid_a)
        rs_down0 = scatter(dw)
        g0, g_bias0 = attn_bwd(qkv0, nt(mid_b, wide0[:, out_cols]).astype(BF16), lse0, tables)
        g0x = exchange(g0)
        g0_a, pre0_b = bar(g0, pre0_a)
        back0 = nt(pre0_b, wide0[:, up_cols])
        g0_b, back0 = bar(g0_a, back0)
        dw = wgrad_cols(core_arr, [(h0, h0x), (mixed0, mixed0x)], [(0, g0_b, g0x), (0, pre0_b, pre0x), (1, mid_b, midx)])
        dw, g0_c, mixed1_b, act1_b = bar(dw, g0_b, mixed1, act1)
        rs_wide0 = scatter(dw)
        grad, g_gain, g_lbias = norm_pull(mid, back0 + back_qkv(g0_c, wide0), normed0, inv0, gain0)
        little0 = pack(g_gain, g_lbias, g_bias0, mid, g_bup0)
        current = finish(x1, mixed1_b, qkvo1[:, 3 * D:], bo1, act1_b, down1, bd1)
        little = [little0, little1]

        scale = 1.0 / token_total
        everyone = gather(jnp.stack(little, axis=1)[None])
        own = jnp.sum(lax.dynamic_index_in_dim(everyone, rank, 1, keepdims=False), axis=0) * scale
        vec = [own[:, i * 128:(i + 1) * 128] for i in range(6)]

        def stacked(first, second):
            return jnp.stack([first * scale, second * scale])

        def heads(pos):
            cols = slice(pos * D, (pos + 1) * D)
            return stacked(rs_wide0[:, cols].reshape(-1, 16, HEAD), rs_qkvo1[:, cols].reshape(-1, 16, HEAD))

        return (current.reshape(hidden.shape), grad.reshape(hidden.shape), vec[0], vec[1],
                heads(0), vec[2], heads(1), vec[3], heads(2), vec[4],
                stacked(rs_wide0[:, out_cols], rs_qkvo1[:, 3 * D:]), vec[5],
                stacked(rs_wide0[:, up_cols], rs_up1), own[:, 6 * 128:], stacked(rs_down0, rs_down1), vec[5])

    return jax.shard_map(step, mesh=mesh, in_specs=(batch_spec, P(), batch_spec) + param_specs, out_specs=(batch_spec, batch_spec) + param_specs, check_vma=False)
```

```python
import functools

import jax
import jax.numpy as jnp
from jax import lax
from jax.experimental import pallas as pl
from jax.experimental.pallas import tpu as pltpu
from jax.sharding import PartitionSpec as P


ROT = 32
LN_EPS = 1e-5
THETA = 10000.0
AXIS_NAME = 'fsdp'
F32 = jnp.float32
BF16 = jnp.bfloat16
SEQ = 1024
D = 1024
FF = 4096
HEAD = 64
GROUP = 4
GW = GROUP * HEAD
STEPS = 4
QB = 256
VMEM_LIMIT = 60 * 1024 * 1024


def rope_tables(positions):
    half_rot = ROT // 2
    inv_freq = THETA ** (-2.0 * jnp.arange(half_rot, dtype=F32) / ROT)
    angles = positions.astype(F32)[:, None] * inv_freq[None, :]
    cos, sin = jnp.cos(angles), jnp.sin(angles)
    ones = jnp.ones((SEQ, HEAD - ROT), F32)
    zeros = jnp.zeros((SEQ, half_rot), F32)
    wide = jnp.zeros((SEQ, HEAD - ROT), F32)
    keep = jnp.concatenate([cos, cos, ones], axis=1)
    left = jnp.concatenate([-sin, zeros, wide], axis=1)
    right = jnp.concatenate([zeros, sin, wide], axis=1)
    return tuple(jnp.tile(t, (1, GROUP)) for t in (keep, left, right))


def head_mask(head):
    lane = lax.broadcasted_iota(jnp.int32, (1, GW), 1)
    return (lane >= head * HEAD) & (lane < (head + 1) * HEAD)


def causal_mask():
    return lax.broadcasted_iota(jnp.int32, (QB, QB), 0) <= lax.broadcasted_iota(jnp.int32, (QB, QB), 1)


def nt(a, b):
    return lax.dot_general(a, b, (((1,), (1,)), ((), ())), preferred_element_type=F32)


def nn(a, b):
    return lax.dot_general(a, b, (((1,), (0,)), ((), ())), preferred_element_type=F32)


def spin(x, keep, left, right):
    return x * keep + pltpu.roll(x, GW - ROT // 2, 1) * left + pltpu.roll(x, ROT // 2, 1) * right


def unspin(x, keep, left, right):
    return x * keep - pltpu.roll(x, GW - ROT // 2, 1) * left - pltpu.roll(x, ROT // 2, 1) * right


def attn_fwd_kernel(h_ref, wq_ref, wk_ref, wv_ref, bq_ref, bk_ref, bv_ref, keep_ref, left_ref, right_ref, qkv_ref, mixed_ref, lse_ref):
    h = h_ref[...]
    keep, left, right = keep_ref[...], left_ref[...], right_ref[...]
    q = spin(nn(h, wq_ref[...]) + bq_ref[...], keep, left, right).astype(BF16)
    qkv_ref[0] = q
    k = spin(nn(h, wk_ref[...]) + bk_ref[...], keep, left, right).astype(BF16)
    qkv_ref[1] = k
    v = nn(h, wv_ref[...]) + bv_ref[...]
    qkv_ref[2] = v.astype(BF16)
    v_t = v.T.astype(BF16)
    mask = causal_mask()
    for blk in range(SEQ // QB):
        lo, hi = blk * QB, (blk + 1) * QB
        q_blk = q[lo:hi] * jnp.asarray(HEAD ** -0.5, BF16)
        outs = []
        for head in range(GROUP):
            q_h = jnp.where(head_mask(head), q_blk, jnp.zeros_like(q_blk))
            diag = jnp.where(mask, nt(k[lo:hi], q_h), -1e30)
            top = jnp.max(diag, axis=0, keepdims=True)
            if blk:
                off = nt(k[:lo], q_h)
                top = jnp.maximum(top, jnp.max(off, axis=0, keepdims=True))
            e_diag = jnp.exp(diag - top)
            total = jnp.sum(e_diag, axis=0, keepdims=True)
            if blk:
                e_off = jnp.exp(off - top)
                total = total + jnp.sum(e_off, axis=0, keepdims=True)
            inv = 1.0 / total
            rows = slice(head * HEAD, (head + 1) * HEAD)
            out = nn(v_t[rows, lo:hi], (e_diag * inv).astype(BF16))
            if blk:
                out = out + nn(v_t[rows, :lo], (e_off * inv).astype(BF16))
            outs.append(out)
            lse_ref[0, head:head + 1, lo:hi] = top + jnp.log(total)
        mixed_ref[lo:hi, :] = jnp.concatenate(outs, axis=0).T.astype(BF16)


def attn_fwd(h, weights, biases, tables):
    full = pl.BlockSpec((SEQ, D), lambda i: (0, 0))
    table = pl.BlockSpec((SEQ, GW), lambda i: (0, 0))
    w_specs = [pl.BlockSpec((D, GW), lambda i, pos=pos: (0, pos * STEPS + i)) for pos in range(3)]
    b_spec = pl.BlockSpec((1, GW), lambda i: (0, i))
    return pl.pallas_call(
        attn_fwd_kernel,
        grid=(STEPS,),
        in_specs=[full] + w_specs + [b_spec] * 3 + [table] * 3,
        out_specs=[pl.BlockSpec((3, SEQ, GW), lambda i: (0, 0, i)), pl.BlockSpec((SEQ, GW), lambda i: (0, i)), pl.BlockSpec((1, 8, SEQ), lambda i: (i, 0, 0))],
        out_shape=[jax.ShapeDtypeStruct((3, SEQ, D), BF16), jax.ShapeDtypeStruct((SEQ, D), BF16), jax.ShapeDtypeStruct((STEPS, 8, SEQ), F32)],
        compiler_params=pltpu.CompilerParams(vmem_limit_bytes=VMEM_LIMIT),
        cost_estimate=pl.CostEstimate(flops=20_000_000_000, bytes_accessed=20_000_000, transcendentals=10_000_000),
        name='attn_fwd',
    )(h, weights, weights, weights, *biases, *tables)


def attn_bwd_kernel(qkv_ref, go_ref, lse_ref, keep_ref, left_ref, right_ref, g_ref, bias_ref, dq_acc, dk_acc, dv_acc):
    q, k, v = qkv_ref[0], qkv_ref[1], qkv_ref[2]
    k_t = k.astype(F32).T.astype(BF16)
    dk_acc[...] = jnp.zeros_like(dk_acc)
    dv_acc[...] = jnp.zeros_like(dv_acc)
    mask = causal_mask()
    scale = HEAD ** -0.5
    for blk in range(SEQ // QB):
        lo, hi = blk * QB, (blk + 1) * QB
        q_blk = q[lo:hi]
        go_blk = go_ref[lo:hi, :]
        probs, scores, q_heads, go_heads, dq_t = [], [], [], [], []
        for head in range(GROUP):
            keep_lanes = head_mask(head)
            q_h = jnp.where(keep_lanes, q_blk, jnp.zeros_like(q_blk))
            go_h = jnp.where(keep_lanes, go_blk, jnp.zeros_like(go_blk))
            lse = lse_ref[0, head:head + 1, lo:hi]
            q_s = q_h * jnp.asarray(scale, BF16)
            p = jnp.where(mask, jnp.exp(nt(k[lo:hi], q_s) - lse), 0.0)
            dp = nt(v[lo:hi], go_h)
            delta = jnp.sum(p * dp, axis=0, keepdims=True)
            if blk:
                p_off = jnp.exp(nt(k[:lo], q_s) - lse)
                dp_off = nt(v[:lo], go_h)
                delta = delta + jnp.sum(p_off * dp_off, axis=0, keepdims=True)
            ds = ((p * (dp - delta)) * scale).astype(BF16)
            p = p.astype(BF16)
            if blk:
                ds = jnp.concatenate([((p_off * (dp_off - delta)) * scale).astype(BF16), ds], axis=0)
                p = jnp.concatenate([p_off.astype(BF16), p], axis=0)
            probs.append(p)
            scores.append(ds)
            q_heads.append(q_h)
            go_heads.append(go_h)
            dq_t.append(nn(k_t[head * HEAD:(head + 1) * HEAD, :hi], ds))
        dv_acc[:hi, :] += nn(jnp.concatenate(probs, axis=1), jnp.concatenate(go_heads, axis=0))
        dk_acc[:hi, :] += nn(jnp.concatenate(scores, axis=1), jnp.concatenate(q_heads, axis=0))
        dq_acc[lo:hi, :] = jnp.concatenate(dq_t, axis=0).T
    keep, left, right = keep_ref[...], left_ref[...], right_ref[...]
    sums = []
    for pos, grad in enumerate((unspin(dq_acc[...], keep, left, right), unspin(dk_acc[...], keep, left, right), dv_acc[...])):
        g_ref[pos] = grad.astype(BF16)
        sums.append(jnp.sum(grad, axis=0, keepdims=True))
    bias_ref[...] = jnp.concatenate([jnp.concatenate(sums, axis=1), jnp.zeros((7, 3 * GW), F32)], axis=0)


def attn_bwd(qkv, grad_mixed, lse, tables):
    wide = pl.BlockSpec((3, SEQ, GW), lambda i: (0, 0, i))
    table = pl.BlockSpec((SEQ, GW), lambda i: (0, 0))
    return pl.pallas_call(
        attn_bwd_kernel,
        grid=(STEPS,),
        in_specs=[wide, pl.BlockSpec((SEQ, GW), lambda i: (0, i)), pl.BlockSpec((1, 8, SEQ), lambda i: (i, 0, 0)), table, table, table],
        out_specs=[wide, pl.BlockSpec((8, 3 * GW), lambda i: (0, i))],
        out_shape=[jax.ShapeDtypeStruct((3, SEQ, D), BF16), jax.ShapeDtypeStruct((8, 3 * D), F32)],
        scratch_shapes=[pltpu.VMEM((SEQ, GW), F32)] * 3,
        compiler_params=pltpu.CompilerParams(vmem_limit_bytes=VMEM_LIMIT),
        cost_estimate=pl.CostEstimate(flops=50_000_000_000, bytes_accessed=20_000_000, transcendentals=10_000_000),
        name='attn_bwd',
    )(qkv, grad_mixed, lse, *tables)


def wgrad_rows_kernel(core_ref, lhs_ref, lhs2_ref, rhs_ref, rhs2_ref, out_ref):
    out_ref[...] = nn(lhs_ref[...].T, rhs_ref[...]) + nn(lhs2_ref[...].T, rhs2_ref[...])


def wgrad_rows(core, lhs, lhs2, rhs, rhs2):
    tile = 256
    lhs_spec = pl.BlockSpec((SEQ, tile), lambda i, c: (0, (i // 2) * 4 + c[0] * 2 + i % 2))
    rhs_spec = pl.BlockSpec((SEQ, D), lambda i, c: (0, 0))
    return pl.pallas_call(
        wgrad_rows_kernel,
        grid_spec=pltpu.PrefetchScalarGridSpec(
            num_scalar_prefetch=1,
            grid=(FF // 2 // tile,),
            in_specs=[lhs_spec, lhs_spec, rhs_spec, rhs_spec],
            out_specs=pl.BlockSpec((tile, D), lambda i, c: (i, 0)),
        ),
        out_shape=jax.ShapeDtypeStruct((FF // 2, D), F32),
        compiler_params=pltpu.CompilerParams(vmem_limit_bytes=VMEM_LIMIT),
        cost_estimate=pl.CostEstimate(flops=2 * FF * D * SEQ, bytes_accessed=20_000_000, transcendentals=0),
        name='wgrad_rows',
    )(core, lhs, lhs2, rhs, rhs2)


TILE = 512


def segment_tiles(rhs):
    return rhs.size // (SEQ * TILE)


def wgrad_cols_kernel(plan, *refs):
    lefts = sorted({p[0] for p in plan}, reverse=False)
    n_left = 8 * len(lefts)
    rhs_refs = refs[1 + n_left:1 + n_left + 2 * len(plan)]
    out_ref, left = refs[-2], refs[-1]
    step = pl.program_id(0)
    loaded = None
    for seg, (which, first, last) in enumerate(plan):
        if which != loaded:
            blocks = refs[1 + 8 * lefts.index(which):1 + 8 * lefts.index(which) + 8]
            loaded = which

            @pl.when(step == first)
            def _(blocks=blocks):
                for j in range(4):
                    left[128 * j:128 * (j + 1), :SEQ] = blocks[j][...].T
                    left[128 * j:128 * (j + 1), SEQ:] = blocks[4 + j][...].T

        here, there = rhs_refs[2 * seg], rhs_refs[2 * seg + 1]

        @pl.when((step >= first) & (step < last))
        def _(here=here, there=there):
            a, b = (here[0], there[0]) if len(here.shape) == 3 else (here[...], there[...])
            out_ref[...] = nn(left[:, :SEQ], a) + nn(left[:, SEQ:], b)


def wgrad_cols(core, lefts, segments):
    plan, specs, args, first = [], [], [], 0
    for mine, partner in lefts:
        for values in (mine, partner):
            for j in range(4):
                specs.append(pl.BlockSpec((SEQ, 128), lambda i, c, j=j: (0, 2 * j + c[0])))
                args.append(values)
    for which, mine, partner in segments:
        tiles = segment_tiles(mine)

        def place(i, c, first=first, tiles=tiles, deep=mine.ndim == 3):
            pos = jnp.clip(i - first, 0, tiles - 1)
            return (pos // 2, 0, pos % 2) if deep else (0, pos)

        shape = (1, SEQ, TILE) if mine.ndim == 3 else (SEQ, TILE)
        specs += [pl.BlockSpec(shape, place)] * 2
        args += [mine, partner]
        plan.append((which, first, first + tiles))
        first += tiles
    return pl.pallas_call(
        functools.partial(wgrad_cols_kernel, tuple(plan)),
        grid_spec=pltpu.PrefetchScalarGridSpec(
            num_scalar_prefetch=1,
            grid=(first,),
            in_specs=specs,
            out_specs=pl.BlockSpec((D // 2, TILE), lambda i, c: (0, i)),
            scratch_shapes=[pltpu.VMEM((D // 2, 2 * SEQ), BF16)],
        ),
        out_shape=jax.ShapeDtypeStruct((D // 2, first * TILE), F32),
        compiler_params=pltpu.CompilerParams(vmem_limit_bytes=VMEM_LIMIT),
        cost_estimate=pl.CostEstimate(flops=2 * SEQ * D * first * TILE, bytes_accessed=3_200_000 * first, transcendentals=0),
        name='wgrad_cols',
    )(core, *args)


def unpack_kernel(scale, *refs):
    srcs, outs = refs[:5], refs[-5:]
    step = pl.program_id(0)
    for slot in range(3):
        @pl.when(step == slot)
        def _(slot=slot):
            outs[slot][0] = (srcs[slot][...] * scale).T

    @pl.when((step >= 3) & (step < 7))
    def _():
        outs[3][0] = srcs[3][...] * scale

    @pl.when(step == 7)
    def _():
        outs[4][0] = srcs[4][...] * scale


def unpack(sources, layer, scale, previous=None):
    def col(i):
        return jnp.clip(i - 3, 0, 3)

    in_specs = []
    for slot, (_, base) in enumerate(sources):
        if slot == 3:
            in_specs.append(pl.BlockSpec((128, D), lambda i, base=base: (0, base + col(i))))
        else:
            in_specs.append(pl.BlockSpec((128, D), lambda i, base=base: (0, base)))
    args = [src for src, _ in sources]
    aliases = {}
    if previous is not None:
        in_specs += [pl.BlockSpec(memory_space=pl.ANY)] * 5
        args += list(previous)
        aliases = {5 + i: i for i in range(5)}
    turned = pl.BlockSpec((1, D, 128), lambda i: (layer, 0, 0))
    return pl.pallas_call(
        functools.partial(unpack_kernel, scale),
        grid=(8,),
        in_specs=in_specs,
        out_specs=[turned] * 3 + [pl.BlockSpec((1, 128, D), lambda i: (layer, 0, col(i))), pl.BlockSpec((1, 128, D), lambda i: (layer, 0, 0))],
        out_shape=[jax.ShapeDtypeStruct((2, D, 128), F32)] * 3 + [jax.ShapeDtypeStruct((2, 128, FF), F32), jax.ShapeDtypeStruct((2, 128, D), F32)],
        input_output_aliases=aliases,
        compiler_params=pltpu.CompilerParams(vmem_limit_bytes=VMEM_LIMIT),
        cost_estimate=pl.CostEstimate(flops=2_000_000, bytes_accessed=8_400_000, transcendentals=0),
        name='unpack',
    )(*args)


def gelu_tanh(values):
    return jax.nn.gelu(values, approximate=True)


def layer_norm(hidden, gain, bias):
    tok = hidden.astype(F32)
    centred = tok - jnp.mean(tok, axis=-1, keepdims=True)
    inv_std = lax.rsqrt(jnp.mean(centred * centred, axis=-1, keepdims=True) + LN_EPS)
    normed = centred * inv_std
    return normed, inv_std, (normed * gain + bias).astype(BF16)


def bar(*values):
    return lax.optimization_barrier(values)


def solution(mesh):
    group_size = mesh.shape[AXIS_NAME]
    batch_spec = P(AXIS_NAME)
    param_specs = (P(None, AXIS_NAME),) * 14
    swap = [(i, i ^ 1) for i in range(group_size)]
    chips = [[i for i in range(group_size) if i % 2 == c] for c in range(2)]

    def exchange(values):
        return lax.ppermute(values, AXIS_NAME, swap)

    def hop(values, offset):
        return lax.ppermute(values, AXIS_NAME, [(i, i ^ offset) for i in range(group_size)])

    def gather(values):
        return lax.all_gather(values, AXIS_NAME, axis=0, tiled=True)

    def scatter(values):
        return lax.psum_scatter(values, AXIS_NAME, scatter_dimension=0, axis_index_groups=chips, tiled=True)

    def step(hidden, positions, grad_out, *shards):
        (ln_gain, ln_bias, w_query, b_query, w_key, b_key, w_value, b_value, w_out, b_out, w_up, b_up, w_down, b_down) = shards
        layers = ln_gain.shape[0]
        token_total = hidden.shape[0] * hidden.shape[1] * group_size
        rank = lax.axis_index(AXIS_NAME)
        core = lax.rem(rank, 2)
        core_arr = core.reshape(1).astype(jnp.int32)
        tables = rope_tables(positions)

        def rows(w, layer):
            return w[layer].reshape(w.shape[1], -1)

        def down_start(shard):
            half = shard.shape[0] // 2
            first, second = shard[:half], shard[half:]
            return first, second, hop(first, 2), hop(first, 4), hop(second, 4), hop(second, 2)

        def down_relay(parts):
            first, second, first_x, first_y, second_y, second_x = parts
            return {0: (first, second), 2: (first_x, second_x), 4: (first_y, second_y), 6: (hop(first_x, 4), hop(second_y, 2))}

        def down_join(pieces):
            half = pieces[0][0].shape[0]
            same = jnp.zeros((4, 2 * half, D), BF16)
            for offset, pair in pieces.items():
                slot = lax.bitwise_xor(rank, offset) // 2
                for pos, piece in enumerate(pair):
                    same = lax.dynamic_update_slice(same, piece[None], (slot, pos * half, 0))
            return same

        def down_whole(same):
            other = exchange(same)
            mine = (jnp.arange(2) == core)[None, :, None, None]
            return jnp.where(mine, same[:, None], other[:, None]).reshape(-1, D)

        wide0 = gather(jnp.concatenate([rows(w, 0) for w in (w_query, w_key, w_value, w_up, w_out)], axis=1))
        down0 = gather(w_down[0])
        up1 = gather(w_up[1])
        qkvo1 = gather(jnp.concatenate([rows(w, 1) for w in (w_query, w_key, w_value, w_out)], axis=1))

        small = jnp.concatenate([b.reshape(layers, -1) for b in (ln_gain, ln_bias, b_query, b_key, b_value, b_out, b_down, b_up)], axis=1)
        small = gather(small[None])

        def split(layer):
            mine = small[:, layer]
            vecs = [mine[:, i * 128:(i + 1) * 128].reshape(1, D).astype(F32) for i in range(7)]
            return vecs + [mine[:, 7 * 128:].reshape(1, FF).astype(F32)]

        def mlp_up(h, wup, bu):
            up_pre = nn(h, wup) + bu
            return up_pre, gelu_tanh(up_pre).astype(BF16)

        def finish(current, mixed, wout, bo, act, wdown, bd):
            return (current.astype(F32) + nn(mixed, wout) + bo + nn(act, wdown) + bd).astype(BF16)

        def mlp_pull(grad, wdown, up_pre):
            grad_act = nt(grad, wdown).astype(BF16)
            grad_pre = jax.vjp(gelu_tanh, up_pre)[1](grad_act.astype(F32))[0]
            return grad_pre.astype(BF16), jnp.sum(grad_pre, axis=0)

        def norm_pull(grad, grad_normed, normed, inv_std, gain):
            grad_hat = grad_normed * gain
            grad_in = inv_std * (grad_hat - jnp.mean(grad_hat, axis=-1, keepdims=True) - normed * jnp.mean(grad_hat * normed, axis=-1, keepdims=True))
            return (grad.astype(F32) + grad_in).astype(BF16), jnp.sum(grad_normed * normed, axis=0), jnp.sum(grad_normed, axis=0)

        def back_qkv(g, weights):
            return sum(nt(g[pos], weights[:, pos * D:(pos + 1) * D]) for pos in range(3))

        def pack(g_gain, g_lbias, g_bias, grad, g_b_up):
            g_bias = g_bias[0].reshape(STEPS, 3, GW)
            pieces = [g_gain, g_lbias] + [g_bias[:, i].reshape(D) for i in range(3)] + [jnp.sum(grad.astype(F32), axis=0)]
            return jnp.concatenate([p.reshape(8, 128) for p in pieces] + [g_b_up.reshape(8, 512)], axis=1)

        up_cols, out_cols = slice(3 * D, 3 * D + FF), slice(3 * D + FF, None)

        x0 = hidden.reshape(SEQ, D)
        gain0, lbias0, bq, bk, bv, bo, bd, bu = split(0)
        normed0, inv0, h0 = layer_norm(x0, gain0, lbias0)
        shard1, wide0 = bar(w_down[1], wide0)
        parts = down_start(shard1)
        qkv0, mixed0, lse0 = attn_fwd(h0, wide0, (bq, bk, bv), tables)
        *parts, mixed0, h0_a = bar(*parts, mixed0, h0)
        pieces = down_relay(parts)
        up_pre0, act0 = mlp_up(h0_a, wide0[:, up_cols], bu)
        x1 = finish(x0, mixed0, wide0[:, out_cols], bo, act0, down0, bd)
        flat, tree = jax.tree.flatten(pieces)
        *flat, x1 = bar(*flat, x1)
        down1 = down_whole(down_join(jax.tree.unflatten(tree, flat)))
        h0x, act0x, mixed0x = exchange(h0), exchange(act0), exchange(mixed0)

        top = grad_out.reshape(SEQ, D)
        topx = exchange(top)
        gain1, lbias1, bq, bk, bv, bo1, bd1, bu = split(1)
        normed1, inv1, h1 = layer_norm(x1, gain1, lbias1)
        up_pre1, act1 = mlp_up(h1, up1, bu)
        h1x, act1x = exchange(h1), exchange(act1)
        pre1, g_bup1 = mlp_pull(top, down1, up_pre1)
        pre1x = exchange(pre1)
        pre1_a, top_a = bar(pre1, top)
        dw, pre1_b = bar(wgrad_rows(core_arr, act1, act1x, top_a, topx), pre1_a)
        rs_down1 = scatter(dw)
        dw, h1_a, top_b = bar(wgrad_cols(core_arr, [(h1, h1x)], [(0, pre1_b, pre1x)]), h1, top_a)
        rs_up1 = scatter(dw)
        qkv1, mixed1, lse1 = attn_fwd(h1_a, qkvo1, (bq, bk, bv), tables)
        mixed1x = exchange(mixed1)
        g1, g_bias1 = attn_bwd(qkv1, nt(top_b, qkvo1[:, 3 * D:]).astype(BF16), lse1, tables)
        g1x = exchange(g1)
        g1_a, pre1_c = bar(g1, pre1_b)
        back1 = nt(pre1_c, up1)
        g1_b, back1 = bar(g1_a, back1)
        dw, g1_c = bar(wgrad_cols(core_arr, [(h1, h1x), (mixed1, mixed1x)], [(0, g1_b, g1x), (1, top, topx)]), g1_b)
        rs_qkvo1 = scatter(dw)
        mid, g_gain, g_lbias = norm_pull(top, back1 + back_qkv(g1_c, qkvo1), normed1, inv1, gain1)
        little1 = pack(g_gain, g_lbias, g_bias1, top, g_bup1)

        midx = exchange(mid)
        pre0, g_bup0 = mlp_pull(mid, down0, up_pre0)
        pre0x = exchange(pre0)
        pre0_a, mid_a = bar(pre0, mid)
        dw, mid_b = bar(wgrad_rows(core_arr, act0, act0x, mid_a, midx), mid_a)
        rs_down0 = scatter(dw)
        g0, g_bias0 = attn_bwd(qkv0, nt(mid_b, wide0[:, out_cols]).astype(BF16), lse0, tables)
        g0x = exchange(g0)
        g0_a, pre0_b = bar(g0, pre0_a)
        back0 = nt(pre0_b, wide0[:, up_cols])
        g0_b, back0 = bar(g0_a, back0)
        dw = wgrad_cols(core_arr, [(h0, h0x), (mixed0, mixed0x)], [(0, g0_b, g0x), (0, pre0_b, pre0x), (1, mid_b, midx)])
        dw, g0_c, mixed1_b, act1_b = bar(dw, g0_b, mixed1, act1)
        rs_wide0 = scatter(dw)
        grad, g_gain, g_lbias = norm_pull(mid, back0 + back_qkv(g0_c, wide0), normed0, inv0, gain0)
        little0 = pack(g_gain, g_lbias, g_bias0, mid, g_bup0)
        current = finish(x1, mixed1_b, qkvo1[:, 3 * D:], bo1, act1_b, down1, bd1)
        little = [little0, little1]

        scale = 1.0 / token_total
        everyone = gather(jnp.stack(little, axis=1)[None])
        own = jnp.sum(lax.dynamic_index_in_dim(everyone, rank, 1, keepdims=False), axis=0) * scale
        vec = [own[:, i * 128:(i + 1) * 128] for i in range(6)]

        done = unpack([(rs_qkvo1, 0), (rs_qkvo1, 1), (rs_qkvo1, 2), (rs_up1, 0), (rs_qkvo1, 3)], 1, scale)
        done = unpack([(rs_wide0, 0), (rs_wide0, 1), (rs_wide0, 2), (rs_wide0, 3), (rs_wide0, 7)], 0, scale, done)
        g_query, g_key, g_value = [g.reshape(layers, 16, HEAD, 128).transpose(0, 3, 1, 2) for g in done[:3]]

        return (current.reshape(hidden.shape), grad.reshape(hidden.shape), vec[0], vec[1],
                g_query, vec[2], g_key, vec[3], g_value, vec[4],
                done[4], vec[5],
                done[3], own[:, 6 * 128:], jnp.stack([rs_down0 * scale, rs_down1 * scale]), vec[5])

    return jax.shard_map(step, mesh=mesh, in_specs=(batch_spec, P(), batch_spec) + param_specs, out_specs=(batch_spec, batch_spec) + param_specs, check_vma=False)
```

```python
import functools

import jax
import jax.numpy as jnp
from jax import lax
from jax.experimental import pallas as pl
from jax.experimental.pallas import tpu as pltpu
from jax.sharding import PartitionSpec as P


ROT = 32
LN_EPS = 1e-5
THETA = 10000.0
AXIS_NAME = 'fsdp'
F32 = jnp.float32
BF16 = jnp.bfloat16
SEQ = 1024
D = 1024
FF = 4096
HEAD = 64
GROUP = 4
GW = GROUP * HEAD
STEPS = 4
QB = 256
VMEM_LIMIT = 60 * 1024 * 1024


def rope_tables(positions):
    half_rot = ROT // 2
    inv_freq = THETA ** (-2.0 * jnp.arange(half_rot, dtype=F32) / ROT)
    angles = positions.astype(F32)[:, None] * inv_freq[None, :]
    cos, sin = jnp.cos(angles), jnp.sin(angles)
    ones = jnp.ones((SEQ, HEAD - ROT), F32)
    zeros = jnp.zeros((SEQ, half_rot), F32)
    wide = jnp.zeros((SEQ, HEAD - ROT), F32)
    keep = jnp.concatenate([cos, cos, ones], axis=1)
    left = jnp.concatenate([-sin, zeros, wide], axis=1)
    right = jnp.concatenate([zeros, sin, wide], axis=1)
    return tuple(jnp.tile(t, (1, GROUP)) for t in (keep, left, right))


def head_mask(head):
    lane = lax.broadcasted_iota(jnp.int32, (1, GW), 1)
    return (lane >= head * HEAD) & (lane < (head + 1) * HEAD)


def causal_mask():
    return lax.broadcasted_iota(jnp.int32, (QB, QB), 0) <= lax.broadcasted_iota(jnp.int32, (QB, QB), 1)


def nt(a, b):
    return lax.dot_general(a, b, (((1,), (1,)), ((), ())), preferred_element_type=F32)


def nn(a, b):
    return lax.dot_general(a, b, (((1,), (0,)), ((), ())), preferred_element_type=F32)


def spin(x, keep, left, right):
    return x * keep + pltpu.roll(x, GW - ROT // 2, 1) * left + pltpu.roll(x, ROT // 2, 1) * right


def unspin(x, keep, left, right):
    return x * keep - pltpu.roll(x, GW - ROT // 2, 1) * left - pltpu.roll(x, ROT // 2, 1) * right


def attn_fwd_kernel(h_ref, wq_ref, wk_ref, wv_ref, bq_ref, bk_ref, bv_ref, keep_ref, left_ref, right_ref, qkv_ref, mixed_ref, lse_ref):
    h = h_ref[...]
    keep, left, right = keep_ref[...], left_ref[...], right_ref[...]
    q = spin(nn(h, wq_ref[...]) + bq_ref[...], keep, left, right).astype(BF16)
    qkv_ref[0] = q
    k = spin(nn(h, wk_ref[...]) + bk_ref[...], keep, left, right).astype(BF16)
    qkv_ref[1] = k
    v = nn(h, wv_ref[...]) + bv_ref[...]
    qkv_ref[2] = v.astype(BF16)
    v_t = v.T.astype(BF16)
    mask = causal_mask()
    for blk in range(SEQ // QB):
        lo, hi = blk * QB, (blk + 1) * QB
        q_blk = q[lo:hi] * jnp.asarray(HEAD ** -0.5, BF16)
        outs = []
        for head in range(GROUP):
            q_h = jnp.where(head_mask(head), q_blk, jnp.zeros_like(q_blk))
            diag = jnp.where(mask, nt(k[lo:hi], q_h), -1e30)
            top = jnp.max(diag, axis=0, keepdims=True)
            if blk:
                off = nt(k[:lo], q_h)
                top = jnp.maximum(top, jnp.max(off, axis=0, keepdims=True))
            e_diag = jnp.exp(diag - top)
            total = jnp.sum(e_diag, axis=0, keepdims=True)
            if blk:
                e_off = jnp.exp(off - top)
                total = total + jnp.sum(e_off, axis=0, keepdims=True)
            inv = 1.0 / total
            rows = slice(head * HEAD, (head + 1) * HEAD)
            out = nn(v_t[rows, lo:hi], (e_diag * inv).astype(BF16))
            if blk:
                out = out + nn(v_t[rows, :lo], (e_off * inv).astype(BF16))
            outs.append(out)
            lse_ref[0, head:head + 1, lo:hi] = top + jnp.log(total)
        mixed_ref[lo:hi, :] = jnp.concatenate(outs, axis=0).T.astype(BF16)


def attn_fwd(h, weights, biases, tables):
    full = pl.BlockSpec((SEQ, D), lambda i: (0, 0))
    table = pl.BlockSpec((SEQ, GW), lambda i: (0, 0))
    w_specs = [pl.BlockSpec((D, GW), lambda i, pos=pos: (0, pos * STEPS + i)) for pos in range(3)]
    b_spec = pl.BlockSpec((1, GW), lambda i: (0, i))
    return pl.pallas_call(
        attn_fwd_kernel,
        grid=(STEPS,),
        in_specs=[full] + w_specs + [b_spec] * 3 + [table] * 3,
        out_specs=[pl.BlockSpec((3, SEQ, GW), lambda i: (0, 0, i)), pl.BlockSpec((SEQ, GW), lambda i: (0, i)), pl.BlockSpec((1, 8, SEQ), lambda i: (i, 0, 0))],
        out_shape=[jax.ShapeDtypeStruct((3, SEQ, D), BF16), jax.ShapeDtypeStruct((SEQ, D), BF16), jax.ShapeDtypeStruct((STEPS, 8, SEQ), F32)],
        compiler_params=pltpu.CompilerParams(vmem_limit_bytes=VMEM_LIMIT),
        cost_estimate=pl.CostEstimate(flops=20_000_000_000, bytes_accessed=20_000_000, transcendentals=10_000_000),
        name='attn_fwd',
    )(h, weights, weights, weights, *biases, *tables)


def attn_bwd_kernel(qkv_ref, go_ref, lse_ref, keep_ref, left_ref, right_ref, g_ref, bias_ref, dq_acc, dk_acc, dv_acc):
    q, k, v = qkv_ref[0], qkv_ref[1], qkv_ref[2]
    k_t = k.astype(F32).T.astype(BF16)
    dk_acc[...] = jnp.zeros_like(dk_acc)
    dv_acc[...] = jnp.zeros_like(dv_acc)
    mask = causal_mask()
    scale = HEAD ** -0.5
    for blk in range(SEQ // QB):
        lo, hi = blk * QB, (blk + 1) * QB
        q_blk = q[lo:hi]
        go_blk = go_ref[lo:hi, :]
        probs, scores, q_heads, go_heads, dq_t = [], [], [], [], []
        for head in range(GROUP):
            keep_lanes = head_mask(head)
            q_h = jnp.where(keep_lanes, q_blk, jnp.zeros_like(q_blk))
            go_h = jnp.where(keep_lanes, go_blk, jnp.zeros_like(go_blk))
            lse = lse_ref[0, head:head + 1, lo:hi]
            q_s = q_h * jnp.asarray(scale, BF16)
            p = jnp.where(mask, jnp.exp(nt(k[lo:hi], q_s) - lse), 0.0)
            dp = nt(v[lo:hi], go_h)
            delta = jnp.sum(p * dp, axis=0, keepdims=True)
            if blk:
                p_off = jnp.exp(nt(k[:lo], q_s) - lse)
                dp_off = nt(v[:lo], go_h)
                delta = delta + jnp.sum(p_off * dp_off, axis=0, keepdims=True)
            ds = ((p * (dp - delta)) * scale).astype(BF16)
            p = p.astype(BF16)
            if blk:
                ds = jnp.concatenate([((p_off * (dp_off - delta)) * scale).astype(BF16), ds], axis=0)
                p = jnp.concatenate([p_off.astype(BF16), p], axis=0)
            probs.append(p)
            scores.append(ds)
            q_heads.append(q_h)
            go_heads.append(go_h)
            dq_t.append(nn(k_t[head * HEAD:(head + 1) * HEAD, :hi], ds))
        dv_acc[:hi, :] += nn(jnp.concatenate(probs, axis=1), jnp.concatenate(go_heads, axis=0))
        dk_acc[:hi, :] += nn(jnp.concatenate(scores, axis=1), jnp.concatenate(q_heads, axis=0))
        dq_acc[lo:hi, :] = jnp.concatenate(dq_t, axis=0).T
    keep, left, right = keep_ref[...], left_ref[...], right_ref[...]
    sums = []
    for pos, grad in enumerate((unspin(dq_acc[...], keep, left, right), unspin(dk_acc[...], keep, left, right), dv_acc[...])):
        g_ref[pos] = grad.astype(BF16)
        sums.append(jnp.sum(grad, axis=0, keepdims=True))
    bias_ref[...] = jnp.concatenate([jnp.concatenate(sums, axis=1), jnp.zeros((7, 3 * GW), F32)], axis=0)


def attn_bwd(qkv, grad_mixed, lse, tables):
    wide = pl.BlockSpec((3, SEQ, GW), lambda i: (0, 0, i))
    table = pl.BlockSpec((SEQ, GW), lambda i: (0, 0))
    return pl.pallas_call(
        attn_bwd_kernel,
        grid=(STEPS,),
        in_specs=[wide, pl.BlockSpec((SEQ, GW), lambda i: (0, i)), pl.BlockSpec((1, 8, SEQ), lambda i: (i, 0, 0)), table, table, table],
        out_specs=[wide, pl.BlockSpec((8, 3 * GW), lambda i: (0, i))],
        out_shape=[jax.ShapeDtypeStruct((3, SEQ, D), BF16), jax.ShapeDtypeStruct((8, 3 * D), F32)],
        scratch_shapes=[pltpu.VMEM((SEQ, GW), F32)] * 3,
        compiler_params=pltpu.CompilerParams(vmem_limit_bytes=VMEM_LIMIT),
        cost_estimate=pl.CostEstimate(flops=50_000_000_000, bytes_accessed=20_000_000, transcendentals=10_000_000),
        name='attn_bwd',
    )(qkv, grad_mixed, lse, *tables)


def wgrad_rows_kernel(core_ref, lhs_ref, lhs2_ref, rhs_ref, rhs2_ref, out_ref):
    out_ref[...] = nn(lhs_ref[...].T, rhs_ref[...]) + nn(lhs2_ref[...].T, rhs2_ref[...])


def wgrad_rows(core, lhs, lhs2, rhs, rhs2):
    tile = 256
    lhs_spec = pl.BlockSpec((SEQ, tile), lambda i, c: (0, (i // 2) * 4 + c[0] * 2 + i % 2))
    rhs_spec = pl.BlockSpec((SEQ, D), lambda i, c: (0, 0))
    return pl.pallas_call(
        wgrad_rows_kernel,
        grid_spec=pltpu.PrefetchScalarGridSpec(
            num_scalar_prefetch=1,
            grid=(FF // 2 // tile,),
            in_specs=[lhs_spec, lhs_spec, rhs_spec, rhs_spec],
            out_specs=pl.BlockSpec((tile, D), lambda i, c: (i, 0)),
        ),
        out_shape=jax.ShapeDtypeStruct((FF // 2, D), F32),
        compiler_params=pltpu.CompilerParams(vmem_limit_bytes=VMEM_LIMIT),
        cost_estimate=pl.CostEstimate(flops=2 * FF * D * SEQ, bytes_accessed=20_000_000, transcendentals=0),
        name='wgrad_rows',
    )(core, lhs, lhs2, rhs, rhs2)


TILE = 512


def segment_tiles(rhs):
    return rhs.size // (SEQ * TILE)


def wgrad_cols_kernel(plan, *refs):
    lefts = sorted({p[0] for p in plan}, reverse=False)
    n_left = 8 * len(lefts)
    rhs_refs = refs[1 + n_left:1 + n_left + 2 * len(plan)]
    out_ref, left = refs[-2], refs[-1]
    step = pl.program_id(0)
    loaded = None
    for seg, (which, first, last) in enumerate(plan):
        if which != loaded:
            blocks = refs[1 + 8 * lefts.index(which):1 + 8 * lefts.index(which) + 8]
            loaded = which

            @pl.when(step == first)
            def _(blocks=blocks):
                for j in range(4):
                    left[128 * j:128 * (j + 1), :SEQ] = blocks[j][...].T
                    left[128 * j:128 * (j + 1), SEQ:] = blocks[4 + j][...].T

        here, there = rhs_refs[2 * seg], rhs_refs[2 * seg + 1]

        @pl.when((step >= first) & (step < last))
        def _(here=here, there=there):
            a, b = (here[0], there[0]) if len(here.shape) == 3 else (here[...], there[...])
            out_ref[...] = nn(left[:, :SEQ], a) + nn(left[:, SEQ:], b)


def wgrad_cols(core, lefts, segments):
    plan, specs, args, first = [], [], [], 0
    for mine, partner in lefts:
        for values in (mine, partner):
            for j in range(4):
                specs.append(pl.BlockSpec((SEQ, 128), lambda i, c, j=j: (0, 2 * j + c[0])))
                args.append(values)
    for which, mine, partner in segments:
        tiles = segment_tiles(mine)

        def place(i, c, first=first, tiles=tiles, deep=mine.ndim == 3):
            pos = jnp.clip(i - first, 0, tiles - 1)
            return (pos // 2, 0, pos % 2) if deep else (0, pos)

        shape = (1, SEQ, TILE) if mine.ndim == 3 else (SEQ, TILE)
        specs += [pl.BlockSpec(shape, place)] * 2
        args += [mine, partner]
        plan.append((which, first, first + tiles))
        first += tiles
    return pl.pallas_call(
        functools.partial(wgrad_cols_kernel, tuple(plan)),
        grid_spec=pltpu.PrefetchScalarGridSpec(
            num_scalar_prefetch=1,
            grid=(first,),
            in_specs=specs,
            out_specs=pl.BlockSpec((D // 2, TILE), lambda i, c: (0, i)),
            scratch_shapes=[pltpu.VMEM((D // 2, 2 * SEQ), BF16)],
        ),
        out_shape=jax.ShapeDtypeStruct((D // 2, first * TILE), F32),
        compiler_params=pltpu.CompilerParams(vmem_limit_bytes=VMEM_LIMIT),
        cost_estimate=pl.CostEstimate(flops=2 * SEQ * D * first * TILE, bytes_accessed=3_200_000 * first, transcendentals=0),
        name='wgrad_cols',
    )(core, *args)


def unpack_kernel(scale, *refs):
    srcs, outs = refs[:5], refs[-5:]
    step = pl.program_id(0)
    for slot in range(3):
        @pl.when(step == slot)
        def _(slot=slot):
            outs[slot][0] = (srcs[slot][...] * scale).T

    @pl.when((step >= 3) & (step < 7))
    def _():
        outs[3][0] = srcs[3][...] * scale

    @pl.when(step == 7)
    def _():
        outs[4][0] = srcs[4][...] * scale


def unpack(sources, layer, scale, previous=None):
    def col(i):
        return jnp.clip(i - 3, 0, 3)

    in_specs = []
    for slot, (_, base) in enumerate(sources):
        if slot == 3:
            in_specs.append(pl.BlockSpec((128, D), lambda i, base=base: (0, base + col(i))))
        else:
            in_specs.append(pl.BlockSpec((128, D), lambda i, base=base: (0, base)))
    args = [src for src, _ in sources]
    aliases = {}
    if previous is not None:
        in_specs += [pl.BlockSpec(memory_space=pl.ANY)] * 5
        args += list(previous)
        aliases = {5 + i: i for i in range(5)}
    turned = pl.BlockSpec((1, D, 128), lambda i: (layer, 0, 0))
    return pl.pallas_call(
        functools.partial(unpack_kernel, scale),
        grid=(8,),
        in_specs=in_specs,
        out_specs=[turned] * 3 + [pl.BlockSpec((1, 128, D), lambda i: (layer, 0, col(i))), pl.BlockSpec((1, 128, D), lambda i: (layer, 0, 0))],
        out_shape=[jax.ShapeDtypeStruct((2, D, 128), F32)] * 3 + [jax.ShapeDtypeStruct((2, 128, FF), F32), jax.ShapeDtypeStruct((2, 128, D), F32)],
        input_output_aliases=aliases,
        compiler_params=pltpu.CompilerParams(vmem_limit_bytes=VMEM_LIMIT),
        cost_estimate=pl.CostEstimate(flops=2_000_000, bytes_accessed=8_400_000, transcendentals=0),
        name='unpack',
    )(*args)


def stack_blocks(ref):
    return jnp.concatenate([ref[:, b * D:(b + 1) * D] for b in range(4)], axis=0)


def finish_kernel(x_ref, mixed_ref, wout_ref, act_ref, wdown_ref, bo_ref, bd_ref, out_ref, acc):
    step = pl.program_id(0)

    @pl.when(step == 0)
    def _():
        acc[...] = x_ref[...].astype(F32) + nn(mixed_ref[...], wout_ref[...]) + bo_ref[...]

    acc[...] += nn(act_ref[...], stack_blocks(wdown_ref))

    @pl.when(step == FF // TILE - 1)
    def _():
        out_ref[...] = (acc[...] + bd_ref[...]).astype(BF16)


def finish(x, mixed, out_from, bo, act, down_from, bd):
    full = pl.BlockSpec((SEQ, D), lambda i: (0, 0))
    row = pl.BlockSpec((1, D), lambda i: (0, 0))
    return pl.pallas_call(
        finish_kernel,
        grid=(FF // TILE,),
        in_specs=[full, full, pl.BlockSpec((D, D), lambda i: (0, out_from[1])), pl.BlockSpec((SEQ, TILE), lambda i: (0, i)),
                  pl.BlockSpec((128, 4 * D), lambda i: (i, down_from[1])), row, row],
        out_specs=full,
        out_shape=jax.ShapeDtypeStruct((SEQ, D), BF16),
        scratch_shapes=[pltpu.VMEM((SEQ, D), F32)],
        compiler_params=pltpu.CompilerParams(vmem_limit_bytes=VMEM_LIMIT),
        cost_estimate=pl.CostEstimate(flops=2 * SEQ * D * (FF + D), bytes_accessed=26_000_000, transcendentals=0),
        name='finish',
    )(x, mixed, out_from[0], act, down_from[0], bo, bd)


def mlp_pull_kernel(grad_ref, wdown_ref, pre_ref, wup_ref, out_ref, bias_ref, back_ref):
    x = pre_ref[...]
    upstream = nt(grad_ref[...], stack_blocks(wdown_ref)).astype(BF16).astype(F32)
    root = 0.7978845608028654
    square = x * x
    t = jnp.tanh(root * (x + 0.044715 * (square * x)))
    slope = 0.5 * (1.0 + t) + (0.5 * x) * ((1.0 - t * t) * (root * (1.0 + (3 * 0.044715) * square)))
    grad = upstream * slope
    bias_ref[...] = jnp.broadcast_to(jnp.sum(grad, axis=0, keepdims=True), bias_ref.shape)
    grad = grad.astype(BF16)
    out_ref[...] = grad
    back = nt(grad, wup_ref[...])

    @pl.when(pl.program_id(0) == 0)
    def _():
        back_ref[...] = back

    @pl.when(pl.program_id(0) > 0)
    def _():
        back_ref[...] += back


def mlp_pull(grad, down_from, up_pre, wup, first):
    full = pl.BlockSpec((SEQ, D), lambda i: (0, 0))
    tile = pl.BlockSpec((SEQ, TILE), lambda i: (0, i))
    pre, bias, back = pl.pallas_call(
        mlp_pull_kernel,
        grid=(FF // TILE,),
        in_specs=[full, pl.BlockSpec((128, 4 * D), lambda i: (i, down_from[1])), tile, pl.BlockSpec((D, TILE), lambda i: (0, first + i))],
        out_specs=[tile, pl.BlockSpec((8, TILE), lambda i: (0, i)), full],
        out_shape=[jax.ShapeDtypeStruct((SEQ, FF), BF16), jax.ShapeDtypeStruct((8, FF), F32), jax.ShapeDtypeStruct((SEQ, D), F32)],
        compiler_params=pltpu.CompilerParams(vmem_limit_bytes=VMEM_LIMIT),
        cost_estimate=pl.CostEstimate(flops=4 * SEQ * D * FF, bytes_accessed=48_000_000, transcendentals=SEQ * FF),
        name='mlp_pull',
    )(grad, down_from[0], up_pre, wup)
    return pre, bias[0], back


def gelu_tanh(values):
    return jax.nn.gelu(values, approximate=True)


def layer_norm(hidden, gain, bias):
    tok = hidden.astype(F32)
    centred = tok - jnp.mean(tok, axis=-1, keepdims=True)
    inv_std = lax.rsqrt(jnp.mean(centred * centred, axis=-1, keepdims=True) + LN_EPS)
    normed = centred * inv_std
    return normed, inv_std, (normed * gain + bias).astype(BF16)


def bar(*values):
    return lax.optimization_barrier(values)


def solution(mesh):
    group_size = mesh.shape[AXIS_NAME]
    batch_spec = P(AXIS_NAME)
    param_specs = (P(None, AXIS_NAME),) * 14
    swap = [(i, i ^ 1) for i in range(group_size)]
    chips = [[i for i in range(group_size) if i % 2 == c] for c in range(2)]

    def exchange(values):
        return lax.ppermute(values, AXIS_NAME, swap)

    def gather(values):
        return lax.all_gather(values, AXIS_NAME, axis=0, tiled=True)

    def scatter(values):
        return lax.psum_scatter(values, AXIS_NAME, scatter_dimension=0, axis_index_groups=chips, tiled=True)

    def step(hidden, positions, grad_out, *shards):
        (ln_gain, ln_bias, w_query, b_query, w_key, b_key, w_value, b_value, w_out, b_out, w_up, b_up, w_down, b_down) = shards
        layers = ln_gain.shape[0]
        token_total = hidden.shape[0] * hidden.shape[1] * group_size
        rank = lax.axis_index(AXIS_NAME)
        core = lax.rem(rank, 2)
        core_arr = core.reshape(1).astype(jnp.int32)
        tables = rope_tables(positions)

        def rows(w, layer):
            return w[layer].reshape(w.shape[1], -1)

        def blocks(layer):
            return [w_down[layer, b * 128:(b + 1) * 128] for b in range(4)]

        wide0 = gather(jnp.concatenate([rows(w, 0) for w in (w_query, w_key, w_value, w_up, w_out)] + blocks(0), axis=1))
        mlp1 = gather(jnp.concatenate([rows(w_up, 1)] + blocks(1), axis=1))
        qkvo1 = gather(jnp.concatenate([rows(w, 1) for w in (w_query, w_key, w_value, w_out)], axis=1))

        small = jnp.concatenate([b.reshape(layers, -1) for b in (ln_gain, ln_bias, b_query, b_key, b_value, b_out, b_down, b_up)], axis=1)
        small = gather(small[None])

        def split(layer):
            mine = small[:, layer]
            vecs = [mine[:, i * 128:(i + 1) * 128].reshape(1, D).astype(F32) for i in range(7)]
            return vecs + [mine[:, 7 * 128:].reshape(1, FF).astype(F32)]

        def mlp_up(h, wup, bu):
            up_pre = nn(h, wup) + bu
            return up_pre, gelu_tanh(up_pre).astype(BF16)

        def norm_pull(grad, grad_normed, normed, inv_std, gain):
            grad_hat = grad_normed * gain
            grad_in = inv_std * (grad_hat - jnp.mean(grad_hat, axis=-1, keepdims=True) - normed * jnp.mean(grad_hat * normed, axis=-1, keepdims=True))
            return (grad.astype(F32) + grad_in).astype(BF16), jnp.sum(grad_normed * normed, axis=0), jnp.sum(grad_normed, axis=0)

        def back_qkv(g, weights):
            return sum(nt(g[pos], weights[:, pos * D:(pos + 1) * D]) for pos in range(3))

        def pack(g_gain, g_lbias, g_bias, grad, g_b_up):
            g_bias = g_bias[0].reshape(STEPS, 3, GW)
            pieces = [g_gain, g_lbias] + [g_bias[:, i].reshape(D) for i in range(3)] + [jnp.sum(grad.astype(F32), axis=0)]
            return jnp.concatenate([p.reshape(8, 128) for p in pieces] + [g_b_up.reshape(8, 512)], axis=1)

        up_cols = slice(3 * D, 3 * D + FF)
        out_cols = slice(3 * D + FF, 4 * D + FF)

        x0 = hidden.reshape(SEQ, D)
        gain0, lbias0, bq, bk, bv, bo, bd, bu = split(0)
        normed0, inv0, h0 = layer_norm(x0, gain0, lbias0)
        qkv0, mixed0, lse0 = attn_fwd(h0, wide0, (bq, bk, bv), tables)
        mixed0, h0_a = bar(mixed0, h0)
        up_pre0, act0 = mlp_up(h0_a, wide0[:, up_cols], bu)
        x1 = finish(x0, mixed0, (wide0, 7), bo, act0, (wide0, 2), bd)
        h0x, act0x, mixed0x = exchange(h0), exchange(act0), exchange(mixed0)

        top = grad_out.reshape(SEQ, D)
        topx = exchange(top)
        gain1, lbias1, bq, bk, bv, bo1, bd1, bu = split(1)
        normed1, inv1, h1 = layer_norm(x1, gain1, lbias1)
        up_pre1, act1 = mlp_up(h1, mlp1[:, :FF], bu)
        h1x, act1x = exchange(h1), exchange(act1)
        pre1, g_bup1, back1 = mlp_pull(top, (mlp1, 1), up_pre1, mlp1, 0)
        pre1x = exchange(pre1)
        pre1_a, top_a = bar(pre1, top)
        dw, pre1_b = bar(wgrad_rows(core_arr, act1, act1x, top_a, topx), pre1_a)
        rs_down1 = scatter(dw)
        dw, h1_a, top_b = bar(wgrad_cols(core_arr, [(h1, h1x)], [(0, pre1_b, pre1x)]), h1, top_a)
        rs_up1 = scatter(dw)
        qkv1, mixed1, lse1 = attn_fwd(h1_a, qkvo1, (bq, bk, bv), tables)
        mixed1x = exchange(mixed1)
        g1, g_bias1 = attn_bwd(qkv1, nt(top_b, qkvo1[:, 3 * D:]).astype(BF16), lse1, tables)
        g1x = exchange(g1)
        g1_a, back1 = bar(g1, back1 + back_qkv(g1, qkvo1))
        dw, back1 = bar(wgrad_cols(core_arr, [(h1, h1x), (mixed1, mixed1x)], [(0, g1_a, g1x), (1, top, topx)]), back1)
        rs_qkvo1 = scatter(dw)
        mid, g_gain, g_lbias = norm_pull(top, back1, normed1, inv1, gain1)
        little1 = pack(g_gain, g_lbias, g_bias1, top, g_bup1)

        midx = exchange(mid)
        pre0, g_bup0, back0 = mlp_pull(mid, (wide0, 2), up_pre0, wide0, 6)
        pre0x = exchange(pre0)
        pre0_a, mid_a = bar(pre0, mid)
        dw, mid_b = bar(wgrad_rows(core_arr, act0, act0x, mid_a, midx), mid_a)
        rs_down0 = scatter(dw)
        g0, g_bias0 = attn_bwd(qkv0, nt(mid_b, wide0[:, out_cols]).astype(BF16), lse0, tables)
        g0x = exchange(g0)
        g0_a, back0 = bar(g0, back0 + back_qkv(g0, wide0))
        dw = wgrad_cols(core_arr, [(h0, h0x), (mixed0, mixed0x)], [(0, g0_a, g0x), (0, pre0_a, pre0x), (1, mid_b, midx)])
        dw, back0, mixed1_b, act1_b = bar(dw, back0, mixed1, act1)
        rs_wide0 = scatter(dw)
        grad, g_gain, g_lbias = norm_pull(mid, back0, normed0, inv0, gain0)
        little0 = pack(g_gain, g_lbias, g_bias0, mid, g_bup0)
        current = finish(x1, mixed1_b, (qkvo1, 3), bo1, act1_b, (mlp1, 1), bd1)
        little = [little0, little1]

        scale = 1.0 / token_total
        everyone = gather(jnp.stack(little, axis=1)[None])
        own = jnp.sum(lax.dynamic_index_in_dim(everyone, rank, 1, keepdims=False), axis=0) * scale
        vec = [own[:, i * 128:(i + 1) * 128] for i in range(6)]

        done = unpack([(rs_qkvo1, 0), (rs_qkvo1, 1), (rs_qkvo1, 2), (rs_up1, 0), (rs_qkvo1, 3)], 1, scale)
        done = unpack([(rs_wide0, 0), (rs_wide0, 1), (rs_wide0, 2), (rs_wide0, 3), (rs_wide0, 7)], 0, scale, done)
        g_query, g_key, g_value = [g.reshape(layers, 16, HEAD, 128).transpose(0, 3, 1, 2) for g in done[:3]]

        return (current.reshape(hidden.shape), grad.reshape(hidden.shape), vec[0], vec[1],
                g_query, vec[2], g_key, vec[3], g_value, vec[4],
                done[4], vec[5],
                done[3], own[:, 6 * 128:], jnp.stack([rs_down0 * scale, rs_down1 * scale]), vec[5])

    return jax.shard_map(step, mesh=mesh, in_specs=(batch_spec, P(), batch_spec) + param_specs, out_specs=(batch_spec, batch_spec) + param_specs, check_vma=False)
```

```python
import functools

import jax
import jax.numpy as jnp
from jax import lax
from jax.experimental import pallas as pl
from jax.experimental.pallas import tpu as pltpu
from jax.sharding import PartitionSpec as P


ROT = 32
LN_EPS = 1e-5
THETA = 10000.0
AXIS_NAME = 'fsdp'
F32 = jnp.float32
BF16 = jnp.bfloat16
SEQ = 1024
D = 1024
FF = 4096
HEAD = 64
GROUP = 4
GW = GROUP * HEAD
STEPS = 4
QB = 256
VMEM_LIMIT = 60 * 1024 * 1024


def rope_tables(positions):
    half_rot = ROT // 2
    inv_freq = THETA ** (-2.0 * jnp.arange(half_rot, dtype=F32) / ROT)
    angles = positions.astype(F32)[:, None] * inv_freq[None, :]
    cos, sin = jnp.cos(angles), jnp.sin(angles)
    ones = jnp.ones((SEQ, HEAD - ROT), F32)
    zeros = jnp.zeros((SEQ, half_rot), F32)
    wide = jnp.zeros((SEQ, HEAD - ROT), F32)
    keep = jnp.concatenate([cos, cos, ones], axis=1)
    left = jnp.concatenate([-sin, zeros, wide], axis=1)
    right = jnp.concatenate([zeros, sin, wide], axis=1)
    return tuple(jnp.tile(t, (1, GROUP)) for t in (keep, left, right))


def head_mask(head):
    lane = lax.broadcasted_iota(jnp.int32, (1, GW), 1)
    return (lane >= head * HEAD) & (lane < (head + 1) * HEAD)


def causal_mask():
    return lax.broadcasted_iota(jnp.int32, (QB, QB), 0) <= lax.broadcasted_iota(jnp.int32, (QB, QB), 1)


def nt(a, b):
    return lax.dot_general(a, b, (((1,), (1,)), ((), ())), preferred_element_type=F32)


def nn(a, b):
    return lax.dot_general(a, b, (((1,), (0,)), ((), ())), preferred_element_type=F32)


def spin(x, keep, left, right):
    return x * keep + pltpu.roll(x, GW - ROT // 2, 1) * left + pltpu.roll(x, ROT // 2, 1) * right


def unspin(x, keep, left, right):
    return x * keep - pltpu.roll(x, GW - ROT // 2, 1) * left - pltpu.roll(x, ROT // 2, 1) * right


def attn_fwd_kernel(h_ref, wq_ref, wk_ref, wv_ref, bq_ref, bk_ref, bv_ref, keep_ref, left_ref, right_ref, qkv_ref, mixed_ref, lse_ref):
    h = h_ref[...]
    keep, left, right = keep_ref[...], left_ref[...], right_ref[...]
    q = spin(nn(h, wq_ref[...]) + bq_ref[...], keep, left, right).astype(BF16)
    qkv_ref[0] = q
    k = spin(nn(h, wk_ref[...]) + bk_ref[...], keep, left, right).astype(BF16)
    qkv_ref[1] = k
    v = nn(h, wv_ref[...]) + bv_ref[...]
    qkv_ref[2] = v.astype(BF16)
    v_t = v.T.astype(BF16)
    mask = causal_mask()
    for blk in range(SEQ // QB):
        lo, hi = blk * QB, (blk + 1) * QB
        q_blk = q[lo:hi] * jnp.asarray(HEAD ** -0.5, BF16)
        outs = []
        for head in range(GROUP):
            q_h = jnp.where(head_mask(head), q_blk, jnp.zeros_like(q_blk))
            diag = jnp.where(mask, nt(k[lo:hi], q_h), -1e30)
            top = jnp.max(diag, axis=0, keepdims=True)
            if blk:
                off = nt(k[:lo], q_h)
                top = jnp.maximum(top, jnp.max(off, axis=0, keepdims=True))
            e_diag = jnp.exp(diag - top)
            total = jnp.sum(e_diag, axis=0, keepdims=True)
            if blk:
                e_off = jnp.exp(off - top)
                total = total + jnp.sum(e_off, axis=0, keepdims=True)
            inv = 1.0 / total
            rows = slice(head * HEAD, (head + 1) * HEAD)
            out = nn(v_t[rows, lo:hi], (e_diag * inv).astype(BF16))
            if blk:
                out = out + nn(v_t[rows, :lo], (e_off * inv).astype(BF16))
            outs.append(out)
            lse_ref[0, head:head + 1, lo:hi] = top + jnp.log(total)
        mixed_ref[lo:hi, :] = jnp.concatenate(outs, axis=0).T.astype(BF16)


def attn_fwd(h, weights, biases, tables):
    full = pl.BlockSpec((SEQ, D), lambda i: (0, 0))
    table = pl.BlockSpec((SEQ, GW), lambda i: (0, 0))
    w_specs = [pl.BlockSpec((D, GW), lambda i, pos=pos: (0, pos * STEPS + i)) for pos in range(3)]
    b_spec = pl.BlockSpec((1, GW), lambda i: (0, i))
    return pl.pallas_call(
        attn_fwd_kernel,
        grid=(STEPS,),
        in_specs=[full] + w_specs + [b_spec] * 3 + [table] * 3,
        out_specs=[pl.BlockSpec((3, SEQ, GW), lambda i: (0, 0, i)), pl.BlockSpec((SEQ, GW), lambda i: (0, i)), pl.BlockSpec((1, 8, SEQ), lambda i: (i, 0, 0))],
        out_shape=[jax.ShapeDtypeStruct((3, SEQ, D), BF16), jax.ShapeDtypeStruct((SEQ, D), BF16), jax.ShapeDtypeStruct((STEPS, 8, SEQ), F32)],
        compiler_params=pltpu.CompilerParams(vmem_limit_bytes=VMEM_LIMIT),
        cost_estimate=pl.CostEstimate(flops=20_000_000_000, bytes_accessed=20_000_000, transcendentals=10_000_000),
        name='attn_fwd',
    )(h, weights, weights, weights, *biases, *tables)


def attn_bwd_kernel(qkv_ref, go_ref, lse_ref, keep_ref, left_ref, right_ref, g_ref, bias_ref, dq_acc, dk_acc, dv_acc):
    q, k, v = qkv_ref[0], qkv_ref[1], qkv_ref[2]
    k_t = k.astype(F32).T.astype(BF16)
    dk_acc[...] = jnp.zeros_like(dk_acc)
    dv_acc[...] = jnp.zeros_like(dv_acc)
    mask = causal_mask()
    scale = HEAD ** -0.5
    for blk in range(SEQ // QB):
        lo, hi = blk * QB, (blk + 1) * QB
        q_blk = q[lo:hi]
        go_blk = go_ref[lo:hi, :]
        probs, scores, q_heads, go_heads, dq_t = [], [], [], [], []
        for head in range(GROUP):
            keep_lanes = head_mask(head)
            q_h = jnp.where(keep_lanes, q_blk, jnp.zeros_like(q_blk))
            go_h = jnp.where(keep_lanes, go_blk, jnp.zeros_like(go_blk))
            lse = lse_ref[0, head:head + 1, lo:hi]
            q_s = q_h * jnp.asarray(scale, BF16)
            p = jnp.where(mask, jnp.exp(nt(k[lo:hi], q_s) - lse), 0.0)
            dp = nt(v[lo:hi], go_h)
            delta = jnp.sum(p * dp, axis=0, keepdims=True)
            if blk:
                p_off = jnp.exp(nt(k[:lo], q_s) - lse)
                dp_off = nt(v[:lo], go_h)
                delta = delta + jnp.sum(p_off * dp_off, axis=0, keepdims=True)
            ds = ((p * (dp - delta)) * scale).astype(BF16)
            p = p.astype(BF16)
            if blk:
                ds = jnp.concatenate([((p_off * (dp_off - delta)) * scale).astype(BF16), ds], axis=0)
                p = jnp.concatenate([p_off.astype(BF16), p], axis=0)
            probs.append(p)
            scores.append(ds)
            q_heads.append(q_h)
            go_heads.append(go_h)
            dq_t.append(nn(k_t[head * HEAD:(head + 1) * HEAD, :hi], ds))
        dv_acc[:hi, :] += nn(jnp.concatenate(probs, axis=1), jnp.concatenate(go_heads, axis=0))
        dk_acc[:hi, :] += nn(jnp.concatenate(scores, axis=1), jnp.concatenate(q_heads, axis=0))
        dq_acc[lo:hi, :] = jnp.concatenate(dq_t, axis=0).T
    keep, left, right = keep_ref[...], left_ref[...], right_ref[...]
    sums = []
    for pos, grad in enumerate((unspin(dq_acc[...], keep, left, right), unspin(dk_acc[...], keep, left, right), dv_acc[...])):
        g_ref[pos] = grad.astype(BF16)
        sums.append(jnp.sum(grad, axis=0, keepdims=True))
    bias_ref[...] = jnp.concatenate([jnp.concatenate(sums, axis=1), jnp.zeros((7, 3 * GW), F32)], axis=0)


def attn_bwd(qkv, grad_mixed, lse, tables):
    wide = pl.BlockSpec((3, SEQ, GW), lambda i: (0, 0, i))
    table = pl.BlockSpec((SEQ, GW), lambda i: (0, 0))
    return pl.pallas_call(
        attn_bwd_kernel,
        grid=(STEPS,),
        in_specs=[wide, pl.BlockSpec((SEQ, GW), lambda i: (0, i)), pl.BlockSpec((1, 8, SEQ), lambda i: (i, 0, 0)), table, table, table],
        out_specs=[wide, pl.BlockSpec((8, 3 * GW), lambda i: (0, i))],
        out_shape=[jax.ShapeDtypeStruct((3, SEQ, D), BF16), jax.ShapeDtypeStruct((8, 3 * D), F32)],
        scratch_shapes=[pltpu.VMEM((SEQ, GW), F32)] * 3,
        compiler_params=pltpu.CompilerParams(vmem_limit_bytes=VMEM_LIMIT),
        cost_estimate=pl.CostEstimate(flops=50_000_000_000, bytes_accessed=20_000_000, transcendentals=10_000_000),
        name='attn_bwd',
    )(qkv, grad_mixed, lse, *tables)


def wgrad_rows_kernel(core_ref, lhs_ref, lhs2_ref, rhs_ref, rhs2_ref, out_ref):
    out_ref[...] = nn(lhs_ref[...].T, rhs_ref[...]) + nn(lhs2_ref[...].T, rhs2_ref[...])


def wgrad_rows(core, lhs, lhs2, rhs, rhs2):
    tile = 256
    lhs_spec = pl.BlockSpec((SEQ, tile), lambda i, c: (0, (i // 2) * 4 + c[0] * 2 + i % 2))
    rhs_spec = pl.BlockSpec((SEQ, D), lambda i, c: (0, 0))
    return pl.pallas_call(
        wgrad_rows_kernel,
        grid_spec=pltpu.PrefetchScalarGridSpec(
            num_scalar_prefetch=1,
            grid=(FF // 2 // tile,),
            in_specs=[lhs_spec, lhs_spec, rhs_spec, rhs_spec],
            out_specs=pl.BlockSpec((tile, D), lambda i, c: (i, 0)),
        ),
        out_shape=jax.ShapeDtypeStruct((FF // 2, D), F32),
        compiler_params=pltpu.CompilerParams(vmem_limit_bytes=VMEM_LIMIT),
        cost_estimate=pl.CostEstimate(flops=2 * FF * D * SEQ, bytes_accessed=20_000_000, transcendentals=0),
        name='wgrad_rows',
    )(core, lhs, lhs2, rhs, rhs2)


TILE = 512


def segment_tiles(rhs):
    return rhs.size // (SEQ * TILE)


def wgrad_cols_kernel(plan, *refs):
    lefts = sorted({p[0] for p in plan}, reverse=False)
    n_left = 8 * len(lefts)
    rhs_refs = refs[1 + n_left:1 + n_left + 2 * len(plan)]
    out_ref, left = refs[-2], refs[-1]
    step = pl.program_id(0)
    loaded = None
    for seg, (which, first, last) in enumerate(plan):
        if which != loaded:
            blocks = refs[1 + 8 * lefts.index(which):1 + 8 * lefts.index(which) + 8]
            loaded = which

            @pl.when(step == first)
            def _(blocks=blocks):
                for j in range(4):
                    left[128 * j:128 * (j + 1), :SEQ] = blocks[j][...].T
                    left[128 * j:128 * (j + 1), SEQ:] = blocks[4 + j][...].T

        here, there = rhs_refs[2 * seg], rhs_refs[2 * seg + 1]

        @pl.when((step >= first) & (step < last))
        def _(here=here, there=there):
            a, b = (here[0], there[0]) if len(here.shape) == 3 else (here[...], there[...])
            out_ref[...] = nn(left[:, :SEQ], a) + nn(left[:, SEQ:], b)


def wgrad_cols(core, lefts, segments):
    plan, specs, args, first = [], [], [], 0
    for mine, partner in lefts:
        for values in (mine, partner):
            for j in range(4):
                specs.append(pl.BlockSpec((SEQ, 128), lambda i, c, j=j: (0, 2 * j + c[0])))
                args.append(values)
    for which, mine, partner in segments:
        tiles = segment_tiles(mine)

        def place(i, c, first=first, tiles=tiles, deep=mine.ndim == 3):
            pos = jnp.clip(i - first, 0, tiles - 1)
            return (pos // 2, 0, pos % 2) if deep else (0, pos)

        shape = (1, SEQ, TILE) if mine.ndim == 3 else (SEQ, TILE)
        specs += [pl.BlockSpec(shape, place)] * 2
        args += [mine, partner]
        plan.append((which, first, first + tiles))
        first += tiles
    return pl.pallas_call(
        functools.partial(wgrad_cols_kernel, tuple(plan)),
        grid_spec=pltpu.PrefetchScalarGridSpec(
            num_scalar_prefetch=1,
            grid=(first,),
            in_specs=specs,
            out_specs=pl.BlockSpec((D // 2, TILE), lambda i, c: (0, i)),
            scratch_shapes=[pltpu.VMEM((D // 2, 2 * SEQ), BF16)],
        ),
        out_shape=jax.ShapeDtypeStruct((D // 2, first * TILE), F32),
        compiler_params=pltpu.CompilerParams(vmem_limit_bytes=VMEM_LIMIT),
        cost_estimate=pl.CostEstimate(flops=2 * SEQ * D * first * TILE, bytes_accessed=3_200_000 * first, transcendentals=0),
        name='wgrad_cols',
    )(core, *args)


def unpack_kernel(scale, *refs):
    srcs, outs = refs[:5], refs[-5:]
    step = pl.program_id(0)
    for slot in range(3):
        @pl.when(step == slot)
        def _(slot=slot):
            outs[slot][0] = (srcs[slot][...] * scale).T

    @pl.when((step >= 3) & (step < 7))
    def _():
        outs[3][0] = srcs[3][...] * scale

    @pl.when(step == 7)
    def _():
        outs[4][0] = srcs[4][...] * scale


def unpack(sources, layer, scale, previous=None):
    def col(i):
        return jnp.clip(i - 3, 0, 3)

    in_specs = []
    for slot, (_, base) in enumerate(sources):
        if slot == 3:
            in_specs.append(pl.BlockSpec((128, D), lambda i, base=base: (0, base + col(i))))
        else:
            in_specs.append(pl.BlockSpec((128, D), lambda i, base=base: (0, base)))
    args = [src for src, _ in sources]
    aliases = {}
    if previous is not None:
        in_specs += [pl.BlockSpec(memory_space=pl.ANY)] * 5
        args += list(previous)
        aliases = {5 + i: i for i in range(5)}
    turned = pl.BlockSpec((1, D, 128), lambda i: (layer, 0, 0))
    return pl.pallas_call(
        functools.partial(unpack_kernel, scale),
        grid=(8,),
        in_specs=in_specs,
        out_specs=[turned] * 3 + [pl.BlockSpec((1, 128, D), lambda i: (layer, 0, col(i))), pl.BlockSpec((1, 128, D), lambda i: (layer, 0, 0))],
        out_shape=[jax.ShapeDtypeStruct((2, D, 128), F32)] * 3 + [jax.ShapeDtypeStruct((2, 128, FF), F32), jax.ShapeDtypeStruct((2, 128, D), F32)],
        input_output_aliases=aliases,
        compiler_params=pltpu.CompilerParams(vmem_limit_bytes=VMEM_LIMIT),
        cost_estimate=pl.CostEstimate(flops=2_000_000, bytes_accessed=8_400_000, transcendentals=0),
        name='unpack',
    )(*args)


def stack_blocks(ref):
    return jnp.concatenate([ref[:, b * D:(b + 1) * D] for b in range(4)], axis=0)


def finish_kernel(base_ref, act_ref, wdown_ref, bd_ref, out_ref, acc):
    step = pl.program_id(0)

    @pl.when(step == 0)
    def _():
        acc[...] = base_ref[...]

    acc[...] += nn(act_ref[...], stack_blocks(wdown_ref))

    @pl.when(step == FF // TILE - 1)
    def _():
        out_ref[...] = (acc[...] + bd_ref[...]).astype(BF16)


def finish(base, act, down_from, bd):
    full = pl.BlockSpec((SEQ, D), lambda i: (0, 0))
    return pl.pallas_call(
        finish_kernel,
        grid=(FF // TILE,),
        in_specs=[full, pl.BlockSpec((SEQ, TILE), lambda i: (0, i)), pl.BlockSpec((128, 4 * D), lambda i: (i, down_from[1])), pl.BlockSpec((1, D), lambda i: (0, 0))],
        out_specs=full,
        out_shape=jax.ShapeDtypeStruct((SEQ, D), BF16),
        scratch_shapes=[pltpu.VMEM((SEQ, D), F32)],
        compiler_params=pltpu.CompilerParams(vmem_limit_bytes=VMEM_LIMIT),
        cost_estimate=pl.CostEstimate(flops=2 * SEQ * D * FF, bytes_accessed=26_000_000, transcendentals=0),
        name='finish',
    )(base, act, down_from[0], bd)


def mlp_pull_kernel(grad_ref, wdown_ref, pre_ref, out_ref, bias_ref):
    root = 0.7978845608028654
    weight = stack_blocks(wdown_ref)
    total = jnp.zeros((8, TILE), F32)
    for base in range(0, SEQ, 256):
        upstream = nt(grad_ref[base:base + 256, :], weight).astype(BF16)
        for low in range(0, 256, 32):
            x = pre_ref[base + low:base + low + 32, :]
            square = x * x
            t = jnp.tanh(x * (root + (root * 0.044715) * square))
            slope = 0.5 * (1.0 + t) + (0.5 * x) * ((1.0 - t * t) * (root + (root * 3 * 0.044715) * square))
            grad = upstream[low:low + 32].astype(F32) * slope
            out_ref[base + low:base + low + 32, :] = grad.astype(BF16)
            total += jnp.sum(grad.reshape(4, 8, TILE), axis=0)
    bias_ref[...] = total


def mlp_pull(grad, down_from, up_pre):
    full = pl.BlockSpec((SEQ, D), lambda i: (0, 0))
    tile = pl.BlockSpec((SEQ, TILE), lambda i: (0, i))
    pre, bias = pl.pallas_call(
        mlp_pull_kernel,
        grid=(FF // TILE,),
        in_specs=[full, pl.BlockSpec((128, 4 * D), lambda i: (i, down_from[1])), tile],
        out_specs=[tile, pl.BlockSpec((8, TILE), lambda i: (0, i))],
        out_shape=[jax.ShapeDtypeStruct((SEQ, FF), BF16), jax.ShapeDtypeStruct((8, FF), F32)],
        compiler_params=pltpu.CompilerParams(vmem_limit_bytes=VMEM_LIMIT),
        cost_estimate=pl.CostEstimate(flops=2 * SEQ * D * FF, bytes_accessed=36_000_000, transcendentals=SEQ * FF),
        name='mlp_pull',
    )(grad, down_from[0], up_pre)
    return pre, jnp.sum(bias, axis=0)


def join_kernel(q_ref, k_ref, v_ref, up_ref, out_w_ref, joined_ref):
    step = pl.program_id(0)
    for slot, ref in enumerate((q_ref, k_ref, v_ref)):
        @pl.when(step == slot)
        def _(ref=ref):
            joined_ref[...] = ref[0].T

    @pl.when((step >= 3) & (step < 7))
    def _():
        joined_ref[...] = up_ref[0]

    @pl.when(step == 7)
    def _():
        joined_ref[...] = out_w_ref[0]


def join(w_query, w_key, w_value, w_up, w_out, layer):
    turned = [w.transpose(0, 2, 3, 1).reshape(2, D, 128) for w in (w_query, w_key, w_value)]
    turned_spec = pl.BlockSpec((1, D, 128), lambda i: (layer, 0, 0))
    return pl.pallas_call(
        join_kernel,
        grid=(8,),
        in_specs=[turned_spec] * 3 + [pl.BlockSpec((1, 128, D), lambda i: (layer, 0, jnp.clip(i - 3, 0, 3))), pl.BlockSpec((1, 128, D), lambda i: (layer, 0, 0))],
        out_specs=pl.BlockSpec((128, D), lambda i: (0, i)),
        out_shape=jax.ShapeDtypeStruct((128, 8 * D), BF16),
        cost_estimate=pl.CostEstimate(flops=1_000_000, bytes_accessed=4_200_000, transcendentals=0),
        name='join',
    )(*turned, w_up, w_out)


def gelu_tanh(values):
    return jax.nn.gelu(values, approximate=True)


def layer_norm(hidden, gain, bias):
    tok = hidden.astype(F32)
    centred = tok - jnp.mean(tok, axis=-1, keepdims=True)
    inv_std = lax.rsqrt(jnp.mean(centred * centred, axis=-1, keepdims=True) + LN_EPS)
    normed = centred * inv_std
    return normed, inv_std, (normed * gain + bias).astype(BF16)


def bar(*values):
    return lax.optimization_barrier(values)


def solution(mesh):
    group_size = mesh.shape[AXIS_NAME]
    batch_spec = P(AXIS_NAME)
    param_specs = (P(None, AXIS_NAME),) * 14
    swap = [(i, i ^ 1) for i in range(group_size)]
    chips = [[i for i in range(group_size) if i % 2 == c] for c in range(2)]

    def exchange(values):
        return lax.ppermute(values, AXIS_NAME, swap)

    def gather(values):
        return lax.all_gather(values, AXIS_NAME, axis=0, tiled=True)

    def scatter(values):
        return lax.psum_scatter(values, AXIS_NAME, scatter_dimension=0, axis_index_groups=chips, tiled=True)

    def step(hidden, positions, grad_out, *shards):
        (ln_gain, ln_bias, w_query, b_query, w_key, b_key, w_value, b_value, w_out, b_out, w_up, b_up, w_down, b_down) = shards
        layers = ln_gain.shape[0]
        token_total = hidden.shape[0] * hidden.shape[1] * group_size
        rank = lax.axis_index(AXIS_NAME)
        core = lax.rem(rank, 2)
        core_arr = core.reshape(1).astype(jnp.int32)
        tables = rope_tables(positions)

        def rows(w, layer):
            return w[layer].reshape(w.shape[1], -1)

        def blocks(layer):
            return [w_down[layer, b * 128:(b + 1) * 128] for b in range(4)]

        wide0 = gather(join(w_query, w_key, w_value, w_up, w_out, 0))
        second = gather(jnp.concatenate([rows(w_up, 1)] + blocks(0), axis=1))
        third = gather(jnp.concatenate([rows(w, 1) for w in (w_query, w_key, w_value, w_out)] + blocks(1), axis=1))

        small = jnp.concatenate([b.reshape(layers, -1) for b in (ln_gain, ln_bias, b_query, b_key, b_value, b_out, b_down, b_up)], axis=1)
        small = gather(small[None])

        def split(layer):
            mine = small[:, layer]
            vecs = [mine[:, i * 128:(i + 1) * 128].reshape(1, D).astype(F32) for i in range(7)]
            return vecs + [mine[:, 7 * 128:].reshape(1, FF).astype(F32)]

        def mlp_up(h, wup, bu):
            up_pre = nn(h, wup) + bu
            return up_pre, gelu_tanh(up_pre).astype(BF16)

        def norm_pull(grad, grad_normed, normed, inv_std, gain):
            grad_hat = grad_normed * gain
            grad_in = inv_std * (grad_hat - jnp.mean(grad_hat, axis=-1, keepdims=True) - normed * jnp.mean(grad_hat * normed, axis=-1, keepdims=True))
            return (grad.astype(F32) + grad_in).astype(BF16), jnp.sum(grad_normed * normed, axis=0), jnp.sum(grad_normed, axis=0)

        def back_qkv(g, weights):
            return sum(nt(g[pos], weights[:, pos * D:(pos + 1) * D]) for pos in range(3))

        def pack(g_gain, g_lbias, g_bias, grad, g_b_up):
            g_bias = g_bias[0].reshape(STEPS, 3, GW)
            pieces = [g_gain, g_lbias] + [g_bias[:, i].reshape(D) for i in range(3)] + [jnp.sum(grad.astype(F32), axis=0)]
            return jnp.concatenate([p.reshape(8, 128) for p in pieces] + [g_b_up.reshape(8, 512)], axis=1)

        up_cols = slice(3 * D, 3 * D + FF)
        out_cols = slice(3 * D + FF, 4 * D + FF)

        def base_sum(x, mixed, wout, bo):
            return x.astype(F32) + nn(mixed, wout) + bo

        x0 = hidden.reshape(SEQ, D)
        gain0, lbias0, bq, bk, bv, bo, bd, bu = split(0)
        normed0, inv0, h0 = layer_norm(x0, gain0, lbias0)
        qkv0, mixed0, lse0 = attn_fwd(h0, wide0, (bq, bk, bv), tables)
        mixed0, h0_a = bar(mixed0, h0)
        up_pre0, act0 = mlp_up(h0_a, wide0[:, up_cols], bu)
        base0, act0 = bar(base_sum(x0, mixed0, wide0[:, out_cols], bo), act0)
        x1 = finish(base0, act0, (second, 1), bd)
        h0x, act0x, mixed0x = exchange(h0), exchange(act0), exchange(mixed0)

        top = grad_out.reshape(SEQ, D)
        topx = exchange(top)
        gain1, lbias1, bq, bk, bv, bo1, bd1, bu = split(1)
        normed1, inv1, h1 = layer_norm(x1, gain1, lbias1)
        up_pre1, act1 = mlp_up(h1, second[:, :FF], bu)
        h1x, act1x = exchange(h1), exchange(act1)
        dw, top_a = bar(wgrad_rows(core_arr, act1, act1x, top, topx), top)
        rs_down1 = scatter(dw)
        pre1, g_bup1 = mlp_pull(top_a, (third, 1), up_pre1)
        pre1x = exchange(pre1)
        pre1_a, h1_a = bar(pre1, h1)
        qkv1, mixed1, lse1 = attn_fwd(h1_a, third, (bq, bk, bv), tables)
        mixed1, pre1_b = bar(mixed1, pre1_a)
        mixed1x = exchange(mixed1)
        dw, top_b = bar(wgrad_cols(core_arr, [(h1, h1x)], [(0, pre1_b, pre1x)]), top_a)
        rs_up1 = scatter(dw)
        g1, g_bias1 = attn_bwd(qkv1, nt(top_b, third[:, 3 * D:4 * D]).astype(BF16), lse1, tables)
        g1x = exchange(g1)
        g1_a, pre1_c = bar(g1, pre1_b)
        g1_b, back1 = bar(g1_a, nt(pre1_c, second[:, :FF]))
        dw, g1_c, back1 = bar(wgrad_cols(core_arr, [(h1, h1x), (mixed1, mixed1x)], [(0, g1_b, g1x), (1, top, topx)]), g1_b, back1)
        rs_qkvo1 = scatter(dw)
        mid, g_gain, g_lbias = norm_pull(top, back1 + back_qkv(g1_c, third), normed1, inv1, gain1)
        little1 = pack(g_gain, g_lbias, g_bias1, top, g_bup1)

        midx = exchange(mid)
        pre0, g_bup0 = mlp_pull(mid, (second, 1), up_pre0)
        pre0x = exchange(pre0)
        pre0_a, mid_a = bar(pre0, mid)
        dw, mid_b = bar(wgrad_rows(core_arr, act0, act0x, mid_a, midx), mid_a)
        rs_down0 = scatter(dw)
        g0, g_bias0 = attn_bwd(qkv0, nt(mid_b, wide0[:, out_cols]).astype(BF16), lse0, tables)
        g0x = exchange(g0)
        g0_a, pre0_b = bar(g0, pre0_a)
        g0_b, back0 = bar(g0_a, nt(pre0_b, wide0[:, up_cols]))
        dw = wgrad_cols(core_arr, [(h0, h0x), (mixed0, mixed0x)], [(0, g0_b, g0x), (0, pre0_b, pre0x), (1, mid_b, midx)])
        dw, g0_c, back0, mixed1_b, act1_b = bar(dw, g0_b, back0, mixed1, act1)
        rs_wide0 = scatter(dw)
        grad, g_gain, g_lbias = norm_pull(mid, back0 + back_qkv(g0_c, wide0), normed0, inv0, gain0)
        little0 = pack(g_gain, g_lbias, g_bias0, mid, g_bup0)
        current = finish(base_sum(x1, mixed1_b, third[:, 3 * D:4 * D], bo1), act1_b, (third, 1), bd1)
        little = [little0, little1]

        scale = 1.0 / token_total
        everyone = gather(jnp.stack(little, axis=1)[None])
        own = jnp.sum(lax.dynamic_index_in_dim(everyone, rank, 1, keepdims=False), axis=0) * scale
        vec = [own[:, i * 128:(i + 1) * 128] for i in range(6)]

        done = unpack([(rs_qkvo1, 0), (rs_qkvo1, 1), (rs_qkvo1, 2), (rs_up1, 0), (rs_qkvo1, 3)], 1, scale)
        done = unpack([(rs_wide0, 0), (rs_wide0, 1), (rs_wide0, 2), (rs_wide0, 3), (rs_wide0, 7)], 0, scale, done)
        g_query, g_key, g_value = [g.reshape(layers, 16, HEAD, 128).transpose(0, 3, 1, 2) for g in done[:3]]

        return (current.reshape(hidden.shape), grad.reshape(hidden.shape), vec[0], vec[1],
                g_query, vec[2], g_key, vec[3], g_value, vec[4],
                done[4], vec[5],
                done[3], own[:, 6 * 128:], jnp.stack([rs_down0 * scale, rs_down1 * scale]), vec[5])

    return jax.shard_map(step, mesh=mesh, in_specs=(batch_spec, P(), batch_spec) + param_specs, out_specs=(batch_spec, batch_spec) + param_specs, check_vma=False)
```

```python
import functools

import jax
import jax.numpy as jnp
from jax import lax
from jax.experimental import pallas as pl
from jax.experimental.pallas import tpu as pltpu
from jax.sharding import PartitionSpec as P


ROT = 32
LN_EPS = 1e-5
THETA = 10000.0
AXIS_NAME = 'fsdp'
F32 = jnp.float32
BF16 = jnp.bfloat16
SEQ = 1024
D = 1024
FF = 4096
HEAD = 64
GROUP = 4
GW = GROUP * HEAD
STEPS = 4
QB = 256
VMEM_LIMIT = 60 * 1024 * 1024


def rope_tables(positions):
    half_rot = ROT // 2
    inv_freq = THETA ** (-2.0 * jnp.arange(half_rot, dtype=F32) / ROT)
    angles = positions.astype(F32)[:, None] * inv_freq[None, :]
    cos, sin = jnp.cos(angles), jnp.sin(angles)
    ones = jnp.ones((SEQ, HEAD - ROT), F32)
    zeros = jnp.zeros((SEQ, half_rot), F32)
    wide = jnp.zeros((SEQ, HEAD - ROT), F32)
    keep = jnp.concatenate([cos, cos, ones], axis=1)
    left = jnp.concatenate([-sin, zeros, wide], axis=1)
    right = jnp.concatenate([zeros, sin, wide], axis=1)
    return tuple(jnp.tile(t, (1, GROUP)) for t in (keep, left, right))


def head_mask(head):
    lane = lax.broadcasted_iota(jnp.int32, (1, GW), 1)
    return (lane >= head * HEAD) & (lane < (head + 1) * HEAD)


def causal_mask():
    return lax.broadcasted_iota(jnp.int32, (QB, QB), 0) <= lax.broadcasted_iota(jnp.int32, (QB, QB), 1)


def nt(a, b):
    return lax.dot_general(a, b, (((1,), (1,)), ((), ())), preferred_element_type=F32)


def nn(a, b):
    return lax.dot_general(a, b, (((1,), (0,)), ((), ())), preferred_element_type=F32)


def spin(x, keep, left, right):
    return x * keep + pltpu.roll(x, GW - ROT // 2, 1) * left + pltpu.roll(x, ROT // 2, 1) * right


def unspin(x, keep, left, right):
    return x * keep - pltpu.roll(x, GW - ROT // 2, 1) * left - pltpu.roll(x, ROT // 2, 1) * right


def attn_fwd_kernel(h_ref, wq_ref, wk_ref, wv_ref, bq_ref, bk_ref, bv_ref, keep_ref, left_ref, right_ref, qkv_ref, mixed_ref, lse_ref):
    h = h_ref[...]
    keep, left, right = keep_ref[...], left_ref[...], right_ref[...]
    q = spin(nn(h, wq_ref[...]) + bq_ref[...], keep, left, right).astype(BF16)
    qkv_ref[0] = q
    k = spin(nn(h, wk_ref[...]) + bk_ref[...], keep, left, right).astype(BF16)
    qkv_ref[1] = k
    v = nn(h, wv_ref[...]) + bv_ref[...]
    qkv_ref[2] = v.astype(BF16)
    v_t = v.T.astype(BF16)
    mask = causal_mask()
    for blk in range(SEQ // QB):
        lo, hi = blk * QB, (blk + 1) * QB
        q_blk = q[lo:hi] * jnp.asarray(HEAD ** -0.5, BF16)
        outs = []
        for head in range(GROUP):
            q_h = jnp.where(head_mask(head), q_blk, jnp.zeros_like(q_blk))
            diag = jnp.where(mask, nt(k[lo:hi], q_h), -1e30)
            top = jnp.max(diag, axis=0, keepdims=True)
            if blk:
                off = nt(k[:lo], q_h)
                top = jnp.maximum(top, jnp.max(off, axis=0, keepdims=True))
            e_diag = jnp.exp(diag - top)
            total = jnp.sum(e_diag, axis=0, keepdims=True)
            if blk:
                e_off = jnp.exp(off - top)
                total = total + jnp.sum(e_off, axis=0, keepdims=True)
            inv = 1.0 / total
            rows = slice(head * HEAD, (head + 1) * HEAD)
            out = nn(v_t[rows, lo:hi], (e_diag * inv).astype(BF16))
            if blk:
                out = out + nn(v_t[rows, :lo], (e_off * inv).astype(BF16))
            outs.append(out)
            lse_ref[0, head:head + 1, lo:hi] = top + jnp.log(total)
        mixed_ref[lo:hi, :] = jnp.concatenate(outs, axis=0).T.astype(BF16)


def attn_fwd(h, weights, biases, tables):
    full = pl.BlockSpec((SEQ, D), lambda i: (0, 0))
    table = pl.BlockSpec((SEQ, GW), lambda i: (0, 0))
    w_specs = [pl.BlockSpec((D, GW), lambda i, pos=pos: (0, pos * STEPS + i)) for pos in range(3)]
    b_spec = pl.BlockSpec((1, GW), lambda i: (0, i))
    return pl.pallas_call(
        attn_fwd_kernel,
        grid=(STEPS,),
        in_specs=[full] + w_specs + [b_spec] * 3 + [table] * 3,
        out_specs=[pl.BlockSpec((3, SEQ, GW), lambda i: (0, 0, i)), pl.BlockSpec((SEQ, GW), lambda i: (0, i)), pl.BlockSpec((1, 8, SEQ), lambda i: (i, 0, 0))],
        out_shape=[jax.ShapeDtypeStruct((3, SEQ, D), BF16), jax.ShapeDtypeStruct((SEQ, D), BF16), jax.ShapeDtypeStruct((STEPS, 8, SEQ), F32)],
        compiler_params=pltpu.CompilerParams(vmem_limit_bytes=VMEM_LIMIT),
        cost_estimate=pl.CostEstimate(flops=20_000_000_000, bytes_accessed=20_000_000, transcendentals=10_000_000),
        name='attn_fwd',
    )(h, weights, weights, weights, *biases, *tables)


def attn_bwd_kernel(qkv_ref, go_ref, lse_ref, keep_ref, left_ref, right_ref, g_ref, bias_ref, dq_acc, dk_acc, dv_acc):
    q, k, v = qkv_ref[0], qkv_ref[1], qkv_ref[2]
    k_t = k.astype(F32).T.astype(BF16)
    dk_acc[...] = jnp.zeros_like(dk_acc)
    dv_acc[...] = jnp.zeros_like(dv_acc)
    mask = causal_mask()
    scale = HEAD ** -0.5
    for blk in range(SEQ // QB):
        lo, hi = blk * QB, (blk + 1) * QB
        q_blk = q[lo:hi]
        go_blk = go_ref[lo:hi, :]
        probs, scores, q_heads, go_heads, dq_t = [], [], [], [], []
        for head in range(GROUP):
            keep_lanes = head_mask(head)
            q_h = jnp.where(keep_lanes, q_blk, jnp.zeros_like(q_blk))
            go_h = jnp.where(keep_lanes, go_blk, jnp.zeros_like(go_blk))
            lse = lse_ref[0, head:head + 1, lo:hi]
            q_s = q_h * jnp.asarray(scale, BF16)
            p = jnp.where(mask, jnp.exp(nt(k[lo:hi], q_s) - lse), 0.0)
            dp = nt(v[lo:hi], go_h)
            delta = jnp.sum(p * dp, axis=0, keepdims=True)
            if blk:
                p_off = jnp.exp(nt(k[:lo], q_s) - lse)
                dp_off = nt(v[:lo], go_h)
                delta = delta + jnp.sum(p_off * dp_off, axis=0, keepdims=True)
            ds = ((p * (dp - delta)) * scale).astype(BF16)
            p = p.astype(BF16)
            if blk:
                ds = jnp.concatenate([((p_off * (dp_off - delta)) * scale).astype(BF16), ds], axis=0)
                p = jnp.concatenate([p_off.astype(BF16), p], axis=0)
            probs.append(p)
            scores.append(ds)
            q_heads.append(q_h)
            go_heads.append(go_h)
            dq_t.append(nn(k_t[head * HEAD:(head + 1) * HEAD, :hi], ds))
        dv_acc[:hi, :] += nn(jnp.concatenate(probs, axis=1), jnp.concatenate(go_heads, axis=0))
        dk_acc[:hi, :] += nn(jnp.concatenate(scores, axis=1), jnp.concatenate(q_heads, axis=0))
        dq_acc[lo:hi, :] = jnp.concatenate(dq_t, axis=0).T
    keep, left, right = keep_ref[...], left_ref[...], right_ref[...]
    sums = []
    for pos, grad in enumerate((unspin(dq_acc[...], keep, left, right), unspin(dk_acc[...], keep, left, right), dv_acc[...])):
        g_ref[pos] = grad.astype(BF16)
        sums.append(jnp.sum(grad, axis=0, keepdims=True))
    bias_ref[...] = jnp.concatenate([jnp.concatenate(sums, axis=1), jnp.zeros((7, 3 * GW), F32)], axis=0)


def attn_bwd(qkv, grad_mixed, lse, tables):
    wide = pl.BlockSpec((3, SEQ, GW), lambda i: (0, 0, i))
    table = pl.BlockSpec((SEQ, GW), lambda i: (0, 0))
    return pl.pallas_call(
        attn_bwd_kernel,
        grid=(STEPS,),
        in_specs=[wide, pl.BlockSpec((SEQ, GW), lambda i: (0, i)), pl.BlockSpec((1, 8, SEQ), lambda i: (i, 0, 0)), table, table, table],
        out_specs=[wide, pl.BlockSpec((8, 3 * GW), lambda i: (0, i))],
        out_shape=[jax.ShapeDtypeStruct((3, SEQ, D), BF16), jax.ShapeDtypeStruct((8, 3 * D), F32)],
        scratch_shapes=[pltpu.VMEM((SEQ, GW), F32)] * 3,
        compiler_params=pltpu.CompilerParams(vmem_limit_bytes=VMEM_LIMIT),
        cost_estimate=pl.CostEstimate(flops=50_000_000_000, bytes_accessed=20_000_000, transcendentals=10_000_000),
        name='attn_bwd',
    )(qkv, grad_mixed, lse, *tables)


def wgrad_rows_kernel(core_ref, lhs_ref, lhs2_ref, rhs_ref, rhs2_ref, out_ref):
    out_ref[...] = nn(lhs_ref[...].T, rhs_ref[...]) + nn(lhs2_ref[...].T, rhs2_ref[...])


def wgrad_rows(core, lhs, lhs2, rhs, rhs2):
    tile = 256
    lhs_spec = pl.BlockSpec((SEQ, tile), lambda i, c: (0, (i // 2) * 4 + c[0] * 2 + i % 2))
    rhs_spec = pl.BlockSpec((SEQ, D), lambda i, c: (0, 0))
    return pl.pallas_call(
        wgrad_rows_kernel,
        grid_spec=pltpu.PrefetchScalarGridSpec(
            num_scalar_prefetch=1,
            grid=(FF // 2 // tile,),
            in_specs=[lhs_spec, lhs_spec, rhs_spec, rhs_spec],
            out_specs=pl.BlockSpec((tile, D), lambda i, c: (i, 0)),
        ),
        out_shape=jax.ShapeDtypeStruct((FF // 2, D), F32),
        compiler_params=pltpu.CompilerParams(vmem_limit_bytes=VMEM_LIMIT),
        cost_estimate=pl.CostEstimate(flops=2 * FF * D * SEQ, bytes_accessed=20_000_000, transcendentals=0),
        name='wgrad_rows',
    )(core, lhs, lhs2, rhs, rhs2)


TILE = 512


def segment_tiles(rhs):
    return rhs.size // (SEQ * TILE)


def wgrad_cols_kernel(plan, *refs):
    lefts = sorted({p[0] for p in plan}, reverse=False)
    n_left = 8 * len(lefts)
    rhs_refs = refs[1 + n_left:1 + n_left + 2 * len(plan)]
    out_ref, left = refs[-2], refs[-1]
    step = pl.program_id(0)
    loaded = None
    for seg, (which, first, last) in enumerate(plan):
        if which != loaded:
            blocks = refs[1 + 8 * lefts.index(which):1 + 8 * lefts.index(which) + 8]
            loaded = which

            @pl.when(step == first)
            def _(blocks=blocks):
                for j in range(4):
                    left[128 * j:128 * (j + 1), :SEQ] = blocks[j][...].T
                    left[128 * j:128 * (j + 1), SEQ:] = blocks[4 + j][...].T

        here, there = rhs_refs[2 * seg], rhs_refs[2 * seg + 1]

        @pl.when((step >= first) & (step < last))
        def _(here=here, there=there):
            a, b = (here[0], there[0]) if len(here.shape) == 3 else (here[...], there[...])
            out_ref[...] = nn(left[:, :SEQ], a) + nn(left[:, SEQ:], b)


def wgrad_cols(core, lefts, segments):
    plan, specs, args, first = [], [], [], 0
    for mine, partner in lefts:
        for values in (mine, partner):
            for j in range(4):
                specs.append(pl.BlockSpec((SEQ, 128), lambda i, c, j=j: (0, 2 * j + c[0])))
                args.append(values)
    for which, mine, partner in segments:
        tiles = segment_tiles(mine)

        def place(i, c, first=first, tiles=tiles, deep=mine.ndim == 3):
            pos = jnp.clip(i - first, 0, tiles - 1)
            return (pos // 2, 0, pos % 2) if deep else (0, pos)

        shape = (1, SEQ, TILE) if mine.ndim == 3 else (SEQ, TILE)
        specs += [pl.BlockSpec(shape, place)] * 2
        args += [mine, partner]
        plan.append((which, first, first + tiles))
        first += tiles
    return pl.pallas_call(
        functools.partial(wgrad_cols_kernel, tuple(plan)),
        grid_spec=pltpu.PrefetchScalarGridSpec(
            num_scalar_prefetch=1,
            grid=(first,),
            in_specs=specs,
            out_specs=pl.BlockSpec((D // 2, TILE), lambda i, c: (0, i)),
            scratch_shapes=[pltpu.VMEM((D // 2, 2 * SEQ), BF16)],
        ),
        out_shape=jax.ShapeDtypeStruct((D // 2, first * TILE), F32),
        compiler_params=pltpu.CompilerParams(vmem_limit_bytes=VMEM_LIMIT),
        cost_estimate=pl.CostEstimate(flops=2 * SEQ * D * first * TILE, bytes_accessed=3_200_000 * first, transcendentals=0),
        name='wgrad_cols',
    )(core, *args)


def unpack_kernel(scale, *refs):
    srcs, outs = refs[:5], refs[-5:]
    step = pl.program_id(0)
    for slot in range(3):
        @pl.when(step == slot)
        def _(slot=slot):
            outs[slot][0] = (srcs[slot][...] * scale).T

    @pl.when((step >= 3) & (step < 7))
    def _():
        outs[3][0] = srcs[3][...] * scale

    @pl.when(step == 7)
    def _():
        outs[4][0] = srcs[4][...] * scale


def unpack(sources, layer, scale, previous=None):
    def col(i):
        return jnp.clip(i - 3, 0, 3)

    in_specs = []
    for slot, (_, base) in enumerate(sources):
        if slot == 3:
            in_specs.append(pl.BlockSpec((128, D), lambda i, base=base: (0, base + col(i))))
        else:
            in_specs.append(pl.BlockSpec((128, D), lambda i, base=base: (0, base)))
    args = [src for src, _ in sources]
    aliases = {}
    if previous is not None:
        in_specs += [pl.BlockSpec(memory_space=pl.ANY)] * 5
        args += list(previous)
        aliases = {5 + i: i for i in range(5)}
    turned = pl.BlockSpec((1, D, 128), lambda i: (layer, 0, 0))
    return pl.pallas_call(
        functools.partial(unpack_kernel, scale),
        grid=(8,),
        in_specs=in_specs,
        out_specs=[turned] * 3 + [pl.BlockSpec((1, 128, D), lambda i: (layer, 0, col(i))), pl.BlockSpec((1, 128, D), lambda i: (layer, 0, 0))],
        out_shape=[jax.ShapeDtypeStruct((2, D, 128), F32)] * 3 + [jax.ShapeDtypeStruct((2, 128, FF), F32), jax.ShapeDtypeStruct((2, 128, D), F32)],
        input_output_aliases=aliases,
        compiler_params=pltpu.CompilerParams(vmem_limit_bytes=VMEM_LIMIT),
        cost_estimate=pl.CostEstimate(flops=2_000_000, bytes_accessed=8_400_000, transcendentals=0),
        name='unpack',
    )(*args)


def stack_blocks(ref):
    return jnp.concatenate([ref[:, b * D:(b + 1) * D] for b in range(4)], axis=0)


def finish_kernel(base_ref, act_ref, wdown_ref, bd_ref, out_ref, acc):
    step = pl.program_id(0)

    @pl.when(step == 0)
    def _():
        acc[...] = base_ref[...]

    acc[...] += nn(act_ref[...], stack_blocks(wdown_ref))

    @pl.when(step == FF // TILE - 1)
    def _():
        out_ref[...] = (acc[...] + bd_ref[...]).astype(BF16)


def finish(base, act, down_from, bd):
    full = pl.BlockSpec((SEQ, D), lambda i: (0, 0))
    return pl.pallas_call(
        finish_kernel,
        grid=(FF // TILE,),
        in_specs=[full, pl.BlockSpec((SEQ, TILE), lambda i: (0, i)), pl.BlockSpec((128, 4 * D), lambda i: (i, down_from[1])), pl.BlockSpec((1, D), lambda i: (0, 0))],
        out_specs=full,
        out_shape=jax.ShapeDtypeStruct((SEQ, D), BF16),
        scratch_shapes=[pltpu.VMEM((SEQ, D), F32)],
        compiler_params=pltpu.CompilerParams(vmem_limit_bytes=VMEM_LIMIT),
        cost_estimate=pl.CostEstimate(flops=2 * SEQ * D * FF, bytes_accessed=26_000_000, transcendentals=0),
        name='finish',
    )(base, act, down_from[0], bd)


def mlp_pull_kernel(grad_ref, wdown_ref, pre_ref, out_ref, bias_ref):
    root = 0.7978845608028654
    weight = stack_blocks(wdown_ref)
    total = jnp.zeros((8, TILE), F32)
    for base in range(0, SEQ, 256):
        upstream = nt(grad_ref[base:base + 256, :], weight).astype(BF16)
        for low in range(0, 256, 32):
            x = pre_ref[base + low:base + low + 32, :]
            square = x * x
            t = jnp.tanh(x * (root + (root * 0.044715) * square))
            slope = 0.5 * (1.0 + t) + (0.5 * x) * ((1.0 - t * t) * (root + (root * 3 * 0.044715) * square))
            grad = upstream[low:low + 32].astype(F32) * slope
            out_ref[base + low:base + low + 32, :] = grad.astype(BF16)
            total += jnp.sum(grad.reshape(4, 8, TILE), axis=0)
    bias_ref[...] = total


def mlp_pull(grad, down_from, up_pre):
    full = pl.BlockSpec((SEQ, D), lambda i: (0, 0))
    tile = pl.BlockSpec((SEQ, TILE), lambda i: (0, i))
    pre, bias = pl.pallas_call(
        mlp_pull_kernel,
        grid=(FF // TILE,),
        in_specs=[full, pl.BlockSpec((128, 4 * D), lambda i: (i, down_from[1])), tile],
        out_specs=[tile, pl.BlockSpec((8, TILE), lambda i: (0, i))],
        out_shape=[jax.ShapeDtypeStruct((SEQ, FF), BF16), jax.ShapeDtypeStruct((8, FF), F32)],
        compiler_params=pltpu.CompilerParams(vmem_limit_bytes=VMEM_LIMIT),
        cost_estimate=pl.CostEstimate(flops=2 * SEQ * D * FF, bytes_accessed=36_000_000, transcendentals=SEQ * FF),
        name='mlp_pull',
    )(grad, down_from[0], up_pre)
    return pre, jnp.sum(bias, axis=0)


def join_kernel(q_ref, k_ref, v_ref, up_ref, out_w_ref, joined_ref):
    step = pl.program_id(0)
    for slot, ref in enumerate((q_ref, k_ref, v_ref)):
        @pl.when(step == slot)
        def _(ref=ref):
            joined_ref[...] = ref[0].T

    @pl.when((step >= 3) & (step < 7))
    def _():
        joined_ref[...] = up_ref[0]

    @pl.when(step == 7)
    def _():
        joined_ref[...] = out_w_ref[0]


def join(w_query, w_key, w_value, w_up, w_out, layer):
    turned = [w.transpose(0, 2, 3, 1).reshape(2, D, 128) for w in (w_query, w_key, w_value)]
    turned_spec = pl.BlockSpec((1, D, 128), lambda i: (layer, 0, 0))
    return pl.pallas_call(
        join_kernel,
        grid=(8,),
        in_specs=[turned_spec] * 3 + [pl.BlockSpec((1, 128, D), lambda i: (layer, 0, jnp.clip(i - 3, 0, 3))), pl.BlockSpec((1, 128, D), lambda i: (layer, 0, 0))],
        out_specs=pl.BlockSpec((128, D), lambda i: (0, i)),
        out_shape=jax.ShapeDtypeStruct((128, 8 * D), BF16),
        cost_estimate=pl.CostEstimate(flops=1_000_000, bytes_accessed=4_200_000, transcendentals=0),
        name='join',
    )(*turned, w_up, w_out)


def gelu_tanh(values):
    return jax.nn.gelu(values, approximate=True)


def layer_norm(hidden, gain, bias):
    tok = hidden.astype(F32)
    centred = tok - jnp.mean(tok, axis=-1, keepdims=True)
    inv_std = lax.rsqrt(jnp.mean(centred * centred, axis=-1, keepdims=True) + LN_EPS)
    normed = centred * inv_std
    return normed, inv_std, (normed * gain + bias).astype(BF16)


def bar(*values):
    return lax.optimization_barrier(values)


def solution(mesh):
    group_size = mesh.shape[AXIS_NAME]
    batch_spec = P(AXIS_NAME)
    param_specs = (P(None, AXIS_NAME),) * 14
    swap = [(i, i ^ 1) for i in range(group_size)]
    chips = [[i for i in range(group_size) if i % 2 == c] for c in range(2)]

    def exchange(values):
        return lax.ppermute(values, AXIS_NAME, swap)

    def hop(values, offset):
        return lax.ppermute(values, AXIS_NAME, [(i, i ^ offset) for i in range(group_size)])

    def gather(values):
        return lax.all_gather(values, AXIS_NAME, axis=0, tiled=True)

    def scatter(values):
        return lax.psum_scatter(values, AXIS_NAME, scatter_dimension=0, axis_index_groups=chips, tiled=True)

    def step(hidden, positions, grad_out, *shards):
        (ln_gain, ln_bias, w_query, b_query, w_key, b_key, w_value, b_value, w_out, b_out, w_up, b_up, w_down, b_down) = shards
        layers = ln_gain.shape[0]
        token_total = hidden.shape[0] * hidden.shape[1] * group_size
        rank = lax.axis_index(AXIS_NAME)
        core = lax.rem(rank, 2)
        core_arr = core.reshape(1).astype(jnp.int32)
        tables = rope_tables(positions)

        def rows(w, layer):
            return w[layer].reshape(w.shape[1], -1)

        def blocks(layer):
            return [w_down[layer, b * 128:(b + 1) * 128] for b in range(4)]

        wide0 = gather(join(w_query, w_key, w_value, w_up, w_out, 0))
        second = gather(jnp.concatenate([rows(w_up, 1)] + blocks(0), axis=1))
        third = gather(jnp.concatenate([rows(w, 1) for w in (w_query, w_key, w_value, w_out)] + blocks(1), axis=1))

        small = jnp.concatenate([b.reshape(layers, -1) for b in (ln_gain, ln_bias, b_query, b_key, b_value, b_out, b_down, b_up)], axis=1)
        small = gather(small[None])

        def split(layer):
            mine = small[:, layer]
            vecs = [mine[:, i * 128:(i + 1) * 128].reshape(1, D).astype(F32) for i in range(7)]
            return vecs + [mine[:, 7 * 128:].reshape(1, FF).astype(F32)]

        def mlp_up(h, wup, bu):
            up_pre = nn(h, wup) + bu
            return up_pre, gelu_tanh(up_pre).astype(BF16)

        def norm_pull(grad, grad_normed, normed, inv_std, gain):
            grad_hat = grad_normed * gain
            grad_in = inv_std * (grad_hat - jnp.mean(grad_hat, axis=-1, keepdims=True) - normed * jnp.mean(grad_hat * normed, axis=-1, keepdims=True))
            return (grad.astype(F32) + grad_in).astype(BF16), jnp.sum(grad_normed * normed, axis=0), jnp.sum(grad_normed, axis=0)

        def back_qkv(g, weights, slots=(0, 1, 2)):
            return sum(nt(g[pos], weights[:, pos * D:(pos + 1) * D]) for pos in slots)

        along_x, along_y = lax.rem(rank // 2, 2), rank // 4

        def pick(values, index, axis):
            return lax.dynamic_index_in_dim(values, index, axis, keepdims=False)

        def ring_send(dw):
            parts = dw.reshape(2, 2, 2, dw.shape[0] // 8, dw.shape[1])
            first, second = parts[:, :, 0], parts[:, :, 1]
            send_first, send_second = pick(first, 1 - along_x, 1), pick(second, 1 - along_y, 0)
            got_first = hop(send_first, 2)
            got_second = hop(send_second, 4)
            return first, second, got_first, got_second

        def ring_turn(first, second, got_first, got_second):
            sum_first = pick(first, along_x, 1) + got_first
            sum_second = pick(second, along_y, 0) + got_second
            kept = pick(sum_first, along_y, 0), pick(sum_second, along_x, 0)
            return kept + (hop(pick(sum_first, 1 - along_y, 0), 4), hop(pick(sum_second, 1 - along_x, 0), 2))

        def ring_end(kept_first, kept_second, got_first, got_second):
            return jnp.concatenate([kept_first + got_first, kept_second + got_second], axis=0)

        def pack(g_gain, g_lbias, g_bias, grad, g_b_up):
            g_bias = g_bias[0].reshape(STEPS, 3, GW)
            pieces = [g_gain, g_lbias] + [g_bias[:, i].reshape(D) for i in range(3)] + [jnp.sum(grad.astype(F32), axis=0)]
            return jnp.concatenate([p.reshape(8, 128) for p in pieces] + [g_b_up.reshape(8, 512)], axis=1)

        up_cols = slice(3 * D, 3 * D + FF)
        out_cols = slice(3 * D + FF, 4 * D + FF)

        def base_sum(x, mixed, wout, bo):
            return x.astype(F32) + nn(mixed, wout) + bo

        x0 = hidden.reshape(SEQ, D)
        gain0, lbias0, bq, bk, bv, bo, bd, bu = split(0)
        normed0, inv0, h0 = layer_norm(x0, gain0, lbias0)
        qkv0, mixed0, lse0 = attn_fwd(h0, wide0, (bq, bk, bv), tables)
        mixed0, h0_a = bar(mixed0, h0)
        up_pre0, act0 = mlp_up(h0_a, wide0[:, up_cols], bu)
        base0, act0 = bar(base_sum(x0, mixed0, wide0[:, out_cols], bo), act0)
        x1 = finish(base0, act0, (second, 1), bd)
        h0x, act0x, mixed0x = exchange(h0), exchange(act0), exchange(mixed0)

        top = grad_out.reshape(SEQ, D)
        topx = exchange(top)
        gain1, lbias1, bq, bk, bv, bo1, bd1, bu = split(1)
        normed1, inv1, h1 = layer_norm(x1, gain1, lbias1)
        up_pre1, act1 = mlp_up(h1, second[:, :FF], bu)
        h1x, act1x = exchange(h1), exchange(act1)
        dw, top_a = bar(wgrad_rows(core_arr, act1, act1x, top, topx), top)
        rs_down1 = scatter(dw)
        pre1, g_bup1 = mlp_pull(top_a, (third, 1), up_pre1)
        pre1x = exchange(pre1)
        pre1_a, h1_a = bar(pre1, h1)
        qkv1, mixed1, lse1 = attn_fwd(h1_a, third, (bq, bk, bv), tables)
        mixed1, pre1_b = bar(mixed1, pre1_a)
        mixed1x = exchange(mixed1)
        dw, top_b = bar(wgrad_cols(core_arr, [(h1, h1x)], [(0, pre1_b, pre1x)]), top_a)
        rs_up1 = scatter(dw)
        g1, g_bias1 = attn_bwd(qkv1, nt(top_b, third[:, 3 * D:4 * D]).astype(BF16), lse1, tables)
        g1x = exchange(g1)
        g1_b, back1 = bar(g1, back_qkv(g1, third, (0, 1)))
        dw, g1_c, back1, pre1_c = bar(wgrad_cols(core_arr, [(h1, h1x), (mixed1, mixed1x)], [(0, g1_b, g1x), (1, top, topx)]), g1_b, back1, pre1_b)
        rs_qkvo1 = scatter(dw)
        mid, g_gain, g_lbias = norm_pull(top, back1 + back_qkv(g1_c, third, (2,)) + nt(pre1_c, second[:, :FF]), normed1, inv1, gain1)
        little1 = pack(g_gain, g_lbias, g_bias1, top, g_bup1)

        midx = exchange(mid)
        pre0, g_bup0 = mlp_pull(mid, (second, 1), up_pre0)
        pre0x = exchange(pre0)
        pre0_a, mid_a = bar(pre0, mid)
        sent = ring_send(wgrad_rows(core_arr, act0, act0x, mid_a, midx))
        first, second_half, got_first, got_second = sent
        first, second_half, mid_b, pre0_b = bar(first, second_half, mid_a, pre0_a)
        sent = (first, second_half, got_first, got_second)
        go0 = nt(mid_b, wide0[:, out_cols]).astype(BF16)
        dw = wgrad_cols(core_arr, [(h0, h0x)], [(0, pre0_b, pre0x)])
        dw, go0 = bar(dw, go0)
        rs_up0 = scatter(dw)
        g0, g_bias0 = attn_bwd(qkv0, go0, lse0, tables)
        g0x = exchange(g0)
        *sent, g0_a, pre0_c = bar(*sent, g0, pre0_b)
        turned = ring_turn(*sent)
        g0_b, back0 = bar(g0_a, nt(pre0_c, wide0[:, up_cols]))
        dw = wgrad_cols(core_arr, [(h0, h0x), (mixed0, mixed0x)], [(0, g0_b, g0x), (1, mid_b, midx)])
        dw, g0_c, back0, mixed1_b, act1_b = bar(dw, g0_b, back0, mixed1, act1)
        rs_qkvo0 = scatter(dw)
        grad, g_gain, g_lbias = norm_pull(mid, back0 + back_qkv(g0_c, wide0), normed0, inv0, gain0)
        *turned, grad = bar(*turned, grad)
        rs_down0 = ring_end(*turned)
        little0 = pack(g_gain, g_lbias, g_bias0, mid, g_bup0)
        current = finish(base_sum(x1, mixed1_b, third[:, 3 * D:4 * D], bo1), act1_b, (third, 1), bd1)
        little = [little0, little1]

        scale = 1.0 / token_total
        everyone = gather(jnp.stack(little, axis=1)[None])
        own = jnp.sum(lax.dynamic_index_in_dim(everyone, rank, 1, keepdims=False), axis=0) * scale
        vec = [own[:, i * 128:(i + 1) * 128] for i in range(6)]

        done = unpack([(rs_qkvo1, 0), (rs_qkvo1, 1), (rs_qkvo1, 2), (rs_up1, 0), (rs_qkvo1, 3)], 1, scale)
        done = unpack([(rs_qkvo0, 0), (rs_qkvo0, 1), (rs_qkvo0, 2), (rs_up0, 0), (rs_qkvo0, 3)], 0, scale, done)
        g_query, g_key, g_value = [g.reshape(layers, 16, HEAD, 128).transpose(0, 3, 1, 2) for g in done[:3]]

        return (current.reshape(hidden.shape), grad.reshape(hidden.shape), vec[0], vec[1],
                g_query, vec[2], g_key, vec[3], g_value, vec[4],
                done[4], vec[5],
                done[3], own[:, 6 * 128:], jnp.stack([rs_down0 * scale, rs_down1 * scale]), vec[5])

    return jax.shard_map(step, mesh=mesh, in_specs=(batch_spec, P(), batch_spec) + param_specs, out_specs=(batch_spec, batch_spec) + param_specs, check_vma=False)
```

```python
import functools

import jax
import jax.numpy as jnp
from jax import lax
from jax.experimental import pallas as pl
from jax.experimental.pallas import tpu as pltpu
from jax.sharding import PartitionSpec as P


ROT = 32
LN_EPS = 1e-5
THETA = 10000.0
AXIS_NAME = 'fsdp'
F32 = jnp.float32
BF16 = jnp.bfloat16
SEQ = 1024
D = 1024
FF = 4096
HEAD = 64
GROUP = 4
GW = GROUP * HEAD
STEPS = 4
QB = 256
VMEM_LIMIT = 60 * 1024 * 1024


def rope_tables(positions):
    half_rot = ROT // 2
    inv_freq = THETA ** (-2.0 * jnp.arange(half_rot, dtype=F32) / ROT)
    angles = positions.astype(F32)[:, None] * inv_freq[None, :]
    cos, sin = jnp.cos(angles), jnp.sin(angles)
    ones = jnp.ones((SEQ, HEAD - ROT), F32)
    zeros = jnp.zeros((SEQ, half_rot), F32)
    wide = jnp.zeros((SEQ, HEAD - ROT), F32)
    keep = jnp.concatenate([cos, cos, ones], axis=1)
    left = jnp.concatenate([-sin, zeros, wide], axis=1)
    right = jnp.concatenate([zeros, sin, wide], axis=1)
    return tuple(jnp.tile(t, (1, GROUP)) for t in (keep, left, right))


def head_mask(head):
    lane = lax.broadcasted_iota(jnp.int32, (1, GW), 1)
    return (lane >= head * HEAD) & (lane < (head + 1) * HEAD)


def causal_mask():
    return lax.broadcasted_iota(jnp.int32, (QB, QB), 0) <= lax.broadcasted_iota(jnp.int32, (QB, QB), 1)


def nt(a, b):
    return lax.dot_general(a, b, (((1,), (1,)), ((), ())), preferred_element_type=F32)


def nn(a, b):
    return lax.dot_general(a, b, (((1,), (0,)), ((), ())), preferred_element_type=F32)


def spin(x, keep, left, right):
    return x * keep + pltpu.roll(x, GW - ROT // 2, 1) * left + pltpu.roll(x, ROT // 2, 1) * right


def unspin(x, keep, left, right):
    return x * keep - pltpu.roll(x, GW - ROT // 2, 1) * left - pltpu.roll(x, ROT // 2, 1) * right


def attn_fwd_kernel(h_ref, wq_ref, wk_ref, wv_ref, bq_ref, bk_ref, bv_ref, keep_ref, left_ref, right_ref, qkv_ref, mixed_ref, lse_ref):
    h = h_ref[...]
    keep, left, right = keep_ref[...], left_ref[...], right_ref[...]
    q = spin(nn(h, wq_ref[...]) + bq_ref[...], keep, left, right).astype(BF16)
    qkv_ref[0] = q
    k = spin(nn(h, wk_ref[...]) + bk_ref[...], keep, left, right).astype(BF16)
    qkv_ref[1] = k
    v = nn(h, wv_ref[...]) + bv_ref[...]
    qkv_ref[2] = v.astype(BF16)
    v_t = v.T.astype(BF16)
    mask = causal_mask()
    for blk in range(SEQ // QB):
        lo, hi = blk * QB, (blk + 1) * QB
        q_blk = q[lo:hi] * jnp.asarray(HEAD ** -0.5, BF16)
        outs = []
        for head in range(GROUP):
            q_h = jnp.where(head_mask(head), q_blk, jnp.zeros_like(q_blk))
            diag = jnp.where(mask, nt(k[lo:hi], q_h), -1e30)
            top = jnp.max(diag, axis=0, keepdims=True)
            if blk:
                off = nt(k[:lo], q_h)
                top = jnp.maximum(top, jnp.max(off, axis=0, keepdims=True))
            e_diag = jnp.exp(diag - top)
            total = jnp.sum(e_diag, axis=0, keepdims=True)
            if blk:
                e_off = jnp.exp(off - top)
                total = total + jnp.sum(e_off, axis=0, keepdims=True)
            inv = 1.0 / total
            rows = slice(head * HEAD, (head + 1) * HEAD)
            out = nn(v_t[rows, lo:hi], (e_diag * inv).astype(BF16))
            if blk:
                out = out + nn(v_t[rows, :lo], (e_off * inv).astype(BF16))
            outs.append(out)
            lse_ref[0, head:head + 1, lo:hi] = top + jnp.log(total)
        mixed_ref[lo:hi, :] = jnp.concatenate(outs, axis=0).T.astype(BF16)


def attn_fwd(h, weights, biases, tables):
    full = pl.BlockSpec((SEQ, D), lambda i: (0, 0))
    table = pl.BlockSpec((SEQ, GW), lambda i: (0, 0))
    w_specs = [pl.BlockSpec((D, GW), lambda i, pos=pos: (0, pos * STEPS + i)) for pos in range(3)]
    b_spec = pl.BlockSpec((1, GW), lambda i: (0, i))
    return pl.pallas_call(
        attn_fwd_kernel,
        grid=(STEPS,),
        in_specs=[full] + w_specs + [b_spec] * 3 + [table] * 3,
        out_specs=[pl.BlockSpec((3, SEQ, GW), lambda i: (0, 0, i)), pl.BlockSpec((SEQ, GW), lambda i: (0, i)), pl.BlockSpec((1, 8, SEQ), lambda i: (i, 0, 0))],
        out_shape=[jax.ShapeDtypeStruct((3, SEQ, D), BF16), jax.ShapeDtypeStruct((SEQ, D), BF16), jax.ShapeDtypeStruct((STEPS, 8, SEQ), F32)],
        compiler_params=pltpu.CompilerParams(vmem_limit_bytes=VMEM_LIMIT),
        cost_estimate=pl.CostEstimate(flops=20_000_000_000, bytes_accessed=20_000_000, transcendentals=10_000_000),
        name='attn_fwd',
    )(h, weights, weights, weights, *biases, *tables)


def attn_bwd_kernel(qkv_ref, go_ref, lse_ref, keep_ref, left_ref, right_ref, g_ref, bias_ref, dq_acc, dk_acc, dv_acc):
    q, k, v = qkv_ref[0], qkv_ref[1], qkv_ref[2]
    k_t = k.astype(F32).T.astype(BF16)
    dk_acc[...] = jnp.zeros_like(dk_acc)
    dv_acc[...] = jnp.zeros_like(dv_acc)
    mask = causal_mask()
    scale = HEAD ** -0.5
    for blk in range(SEQ // QB):
        lo, hi = blk * QB, (blk + 1) * QB
        q_blk = q[lo:hi]
        go_blk = go_ref[lo:hi, :]
        probs, scores, q_heads, go_heads, dq_t = [], [], [], [], []
        for head in range(GROUP):
            keep_lanes = head_mask(head)
            q_h = jnp.where(keep_lanes, q_blk, jnp.zeros_like(q_blk))
            go_h = jnp.where(keep_lanes, go_blk, jnp.zeros_like(go_blk))
            lse = lse_ref[0, head:head + 1, lo:hi]
            q_s = q_h * jnp.asarray(scale, BF16)
            p = jnp.where(mask, jnp.exp(nt(k[lo:hi], q_s) - lse), 0.0)
            dp = nt(v[lo:hi], go_h)
            delta = jnp.sum(p * dp, axis=0, keepdims=True)
            if blk:
                p_off = jnp.exp(nt(k[:lo], q_s) - lse)
                dp_off = nt(v[:lo], go_h)
                delta = delta + jnp.sum(p_off * dp_off, axis=0, keepdims=True)
            ds = ((p * (dp - delta)) * scale).astype(BF16)
            p = p.astype(BF16)
            if blk:
                ds = jnp.concatenate([((p_off * (dp_off - delta)) * scale).astype(BF16), ds], axis=0)
                p = jnp.concatenate([p_off.astype(BF16), p], axis=0)
            probs.append(p)
            scores.append(ds)
            q_heads.append(q_h)
            go_heads.append(go_h)
            dq_t.append(nn(k_t[head * HEAD:(head + 1) * HEAD, :hi], ds))
        dv_acc[:hi, :] += nn(jnp.concatenate(probs, axis=1), jnp.concatenate(go_heads, axis=0))
        dk_acc[:hi, :] += nn(jnp.concatenate(scores, axis=1), jnp.concatenate(q_heads, axis=0))
        dq_acc[lo:hi, :] = jnp.concatenate(dq_t, axis=0).T
    keep, left, right = keep_ref[...], left_ref[...], right_ref[...]
    sums = []
    for pos, grad in enumerate((unspin(dq_acc[...], keep, left, right), unspin(dk_acc[...], keep, left, right), dv_acc[...])):
        g_ref[pos] = grad.astype(BF16)
        sums.append(jnp.sum(grad, axis=0, keepdims=True))
    bias_ref[...] = jnp.concatenate([jnp.concatenate(sums, axis=1), jnp.zeros((7, 3 * GW), F32)], axis=0)


def attn_bwd(qkv, grad_mixed, lse, tables):
    wide = pl.BlockSpec((3, SEQ, GW), lambda i: (0, 0, i))
    table = pl.BlockSpec((SEQ, GW), lambda i: (0, 0))
    return pl.pallas_call(
        attn_bwd_kernel,
        grid=(STEPS,),
        in_specs=[wide, pl.BlockSpec((SEQ, GW), lambda i: (0, i)), pl.BlockSpec((1, 8, SEQ), lambda i: (i, 0, 0)), table, table, table],
        out_specs=[wide, pl.BlockSpec((8, 3 * GW), lambda i: (0, i))],
        out_shape=[jax.ShapeDtypeStruct((3, SEQ, D), BF16), jax.ShapeDtypeStruct((8, 3 * D), F32)],
        scratch_shapes=[pltpu.VMEM((SEQ, GW), F32)] * 3,
        compiler_params=pltpu.CompilerParams(vmem_limit_bytes=VMEM_LIMIT),
        cost_estimate=pl.CostEstimate(flops=50_000_000_000, bytes_accessed=20_000_000, transcendentals=10_000_000),
        name='attn_bwd',
    )(qkv, grad_mixed, lse, *tables)


def wgrad_rows_kernel(core_ref, lhs_ref, lhs2_ref, rhs_ref, rhs2_ref, out_ref):
    out_ref[...] = nn(lhs_ref[...].T, rhs_ref[...]) + nn(lhs2_ref[...].T, rhs2_ref[...])


def wgrad_rows(core, lhs, lhs2, rhs, rhs2):
    tile = 256
    lhs_spec = pl.BlockSpec((SEQ, tile), lambda i, c: (0, (i // 2) * 4 + c[0] * 2 + i % 2))
    rhs_spec = pl.BlockSpec((SEQ, D), lambda i, c: (0, 0))
    return pl.pallas_call(
        wgrad_rows_kernel,
        grid_spec=pltpu.PrefetchScalarGridSpec(
            num_scalar_prefetch=1,
            grid=(FF // 2 // tile,),
            in_specs=[lhs_spec, lhs_spec, rhs_spec, rhs_spec],
            out_specs=pl.BlockSpec((tile, D), lambda i, c: (i, 0)),
        ),
        out_shape=jax.ShapeDtypeStruct((FF // 2, D), F32),
        compiler_params=pltpu.CompilerParams(vmem_limit_bytes=VMEM_LIMIT),
        cost_estimate=pl.CostEstimate(flops=2 * FF * D * SEQ, bytes_accessed=20_000_000, transcendentals=0),
        name='wgrad_rows',
    )(core, lhs, lhs2, rhs, rhs2)


TILE = 512


def segment_tiles(rhs):
    return rhs.size // (SEQ * TILE)


def wgrad_cols_kernel(plan, *refs):
    lefts = sorted({p[0] for p in plan}, reverse=False)
    n_left = 8 * len(lefts)
    rhs_refs = refs[1 + n_left:1 + n_left + 2 * len(plan)]
    out_ref, left = refs[-2], refs[-1]
    step = pl.program_id(0)
    loaded = None
    for seg, (which, first, last) in enumerate(plan):
        if which != loaded:
            blocks = refs[1 + 8 * lefts.index(which):1 + 8 * lefts.index(which) + 8]
            loaded = which

            @pl.when(step == first)
            def _(blocks=blocks):
                for j in range(4):
                    left[128 * j:128 * (j + 1), :SEQ] = blocks[j][...].T
                    left[128 * j:128 * (j + 1), SEQ:] = blocks[4 + j][...].T

        here, there = rhs_refs[2 * seg], rhs_refs[2 * seg + 1]

        @pl.when((step >= first) & (step < last))
        def _(here=here, there=there):
            a, b = (here[0], there[0]) if len(here.shape) == 3 else (here[...], there[...])
            out_ref[...] = nn(left[:, :SEQ], a) + nn(left[:, SEQ:], b)


def wgrad_cols(core, lefts, segments):
    plan, specs, args, first = [], [], [], 0
    for mine, partner in lefts:
        for values in (mine, partner):
            for j in range(4):
                specs.append(pl.BlockSpec((SEQ, 128), lambda i, c, j=j: (0, 2 * j + c[0])))
                args.append(values)
    for which, mine, partner in segments:
        tiles = segment_tiles(mine)

        def place(i, c, first=first, tiles=tiles, deep=mine.ndim == 3):
            pos = jnp.clip(i - first, 0, tiles - 1)
            return (pos // 2, 0, pos % 2) if deep else (0, pos)

        shape = (1, SEQ, TILE) if mine.ndim == 3 else (SEQ, TILE)
        specs += [pl.BlockSpec(shape, place)] * 2
        args += [mine, partner]
        plan.append((which, first, first + tiles))
        first += tiles
    return pl.pallas_call(
        functools.partial(wgrad_cols_kernel, tuple(plan)),
        grid_spec=pltpu.PrefetchScalarGridSpec(
            num_scalar_prefetch=1,
            grid=(first,),
            in_specs=specs,
            out_specs=pl.BlockSpec((D // 2, TILE), lambda i, c: (0, i)),
            scratch_shapes=[pltpu.VMEM((D // 2, 2 * SEQ), BF16)],
        ),
        out_shape=jax.ShapeDtypeStruct((D // 2, first * TILE), F32),
        compiler_params=pltpu.CompilerParams(vmem_limit_bytes=VMEM_LIMIT),
        cost_estimate=pl.CostEstimate(flops=2 * SEQ * D * first * TILE, bytes_accessed=3_200_000 * first, transcendentals=0),
        name='wgrad_cols',
    )(core, *args)


def unpack_kernel(scale, *refs):
    srcs, outs = refs[:5], refs[-5:]
    step = pl.program_id(0)
    for slot in range(3):
        @pl.when(step == slot)
        def _(slot=slot):
            outs[slot][0] = (srcs[slot][...] * scale).T

    @pl.when((step >= 3) & (step < 7))
    def _():
        outs[3][0] = srcs[3][...] * scale

    @pl.when(step == 7)
    def _():
        outs[4][0] = srcs[4][...] * scale


def unpack(sources, layer, scale, previous=None):
    def col(i):
        return jnp.clip(i - 3, 0, 3)

    in_specs = []
    for slot, (_, base) in enumerate(sources):
        if slot == 3:
            in_specs.append(pl.BlockSpec((128, D), lambda i, base=base: (0, base + col(i))))
        else:
            in_specs.append(pl.BlockSpec((128, D), lambda i, base=base: (0, base)))
    args = [src for src, _ in sources]
    aliases = {}
    if previous is not None:
        in_specs += [pl.BlockSpec(memory_space=pl.ANY)] * 5
        args += list(previous)
        aliases = {5 + i: i for i in range(5)}
    turned = pl.BlockSpec((1, D, 128), lambda i: (layer, 0, 0))
    return pl.pallas_call(
        functools.partial(unpack_kernel, scale),
        grid=(8,),
        in_specs=in_specs,
        out_specs=[turned] * 3 + [pl.BlockSpec((1, 128, D), lambda i: (layer, 0, col(i))), pl.BlockSpec((1, 128, D), lambda i: (layer, 0, 0))],
        out_shape=[jax.ShapeDtypeStruct((2, D, 128), F32)] * 3 + [jax.ShapeDtypeStruct((2, 128, FF), F32), jax.ShapeDtypeStruct((2, 128, D), F32)],
        input_output_aliases=aliases,
        compiler_params=pltpu.CompilerParams(vmem_limit_bytes=VMEM_LIMIT),
        cost_estimate=pl.CostEstimate(flops=2_000_000, bytes_accessed=8_400_000, transcendentals=0),
        name='unpack',
    )(*args)


def stack_blocks(ref):
    return jnp.concatenate([ref[:, b * D:(b + 1) * D] for b in range(4)], axis=0)


def finish_kernel(base_ref, act_ref, wdown_ref, bd_ref, out_ref, acc):
    step = pl.program_id(0)

    @pl.when(step == 0)
    def _():
        acc[...] = base_ref[...]

    acc[...] += nn(act_ref[...], stack_blocks(wdown_ref))

    @pl.when(step == FF // TILE - 1)
    def _():
        out_ref[...] = (acc[...] + bd_ref[...]).astype(BF16)


def finish(base, act, down_from, bd):
    full = pl.BlockSpec((SEQ, D), lambda i: (0, 0))
    return pl.pallas_call(
        finish_kernel,
        grid=(FF // TILE,),
        in_specs=[full, pl.BlockSpec((SEQ, TILE), lambda i: (0, i)), pl.BlockSpec((128, 4 * D), lambda i: (i, down_from[1])), pl.BlockSpec((1, D), lambda i: (0, 0))],
        out_specs=full,
        out_shape=jax.ShapeDtypeStruct((SEQ, D), BF16),
        scratch_shapes=[pltpu.VMEM((SEQ, D), F32)],
        compiler_params=pltpu.CompilerParams(vmem_limit_bytes=VMEM_LIMIT),
        cost_estimate=pl.CostEstimate(flops=2 * SEQ * D * FF, bytes_accessed=26_000_000, transcendentals=0),
        name='finish',
    )(base, act, down_from[0], bd)


def mlp_pull_kernel(grad_ref, wdown_ref, pre_ref, out_ref, bias_ref):
    root = 0.7978845608028654
    weight = stack_blocks(wdown_ref)
    total = jnp.zeros((8, TILE), F32)
    for base in range(0, SEQ, 256):
        upstream = nt(grad_ref[base:base + 256, :], weight).astype(BF16)
        for low in range(0, 256, 32):
            x = pre_ref[base + low:base + low + 32, :]
            square = x * x
            t = jnp.tanh(x * (root + (root * 0.044715) * square))
            slope = 0.5 * (1.0 + t) + (0.5 * x) * ((1.0 - t * t) * (root + (root * 3 * 0.044715) * square))
            grad = upstream[low:low + 32].astype(F32) * slope
            out_ref[base + low:base + low + 32, :] = grad.astype(BF16)
            total += jnp.sum(grad.reshape(4, 8, TILE), axis=0)
    bias_ref[...] = total


def mlp_pull(grad, down_from, up_pre):
    full = pl.BlockSpec((SEQ, D), lambda i: (0, 0))
    tile = pl.BlockSpec((SEQ, TILE), lambda i: (0, i))
    pre, bias = pl.pallas_call(
        mlp_pull_kernel,
        grid=(FF // TILE,),
        in_specs=[full, pl.BlockSpec((128, 4 * D), lambda i: (i, down_from[1])), tile],
        out_specs=[tile, pl.BlockSpec((8, TILE), lambda i: (0, i))],
        out_shape=[jax.ShapeDtypeStruct((SEQ, FF), BF16), jax.ShapeDtypeStruct((8, FF), F32)],
        compiler_params=pltpu.CompilerParams(vmem_limit_bytes=VMEM_LIMIT),
        cost_estimate=pl.CostEstimate(flops=2 * SEQ * D * FF, bytes_accessed=36_000_000, transcendentals=SEQ * FF),
        name='mlp_pull',
    )(grad, down_from[0], up_pre)
    return pre, jnp.sum(bias, axis=0)


def join_kernel(q_ref, k_ref, v_ref, up_ref, out_w_ref, joined_ref):
    step = pl.program_id(0)
    for slot, ref in enumerate((q_ref, k_ref, v_ref)):
        @pl.when(step == slot)
        def _(ref=ref):
            joined_ref[...] = ref[0].T

    @pl.when((step >= 3) & (step < 7))
    def _():
        joined_ref[...] = up_ref[0]

    @pl.when(step == 7)
    def _():
        joined_ref[...] = out_w_ref[0]


def join(w_query, w_key, w_value, w_up, w_out, layer):
    turned = [w.transpose(0, 2, 3, 1).reshape(2, D, 128) for w in (w_query, w_key, w_value)]
    turned_spec = pl.BlockSpec((1, D, 128), lambda i: (layer, 0, 0))
    return pl.pallas_call(
        join_kernel,
        grid=(8,),
        in_specs=[turned_spec] * 3 + [pl.BlockSpec((1, 128, D), lambda i: (layer, 0, jnp.clip(i - 3, 0, 3))), pl.BlockSpec((1, 128, D), lambda i: (layer, 0, 0))],
        out_specs=pl.BlockSpec((128, D), lambda i: (0, i)),
        out_shape=jax.ShapeDtypeStruct((128, 8 * D), BF16),
        cost_estimate=pl.CostEstimate(flops=1_000_000, bytes_accessed=4_200_000, transcendentals=0),
        name='join',
    )(*turned, w_up, w_out)


def gelu_tanh(values):
    return jax.nn.gelu(values, approximate=True)


def layer_norm(hidden, gain, bias):
    tok = hidden.astype(F32)
    centred = tok - jnp.mean(tok, axis=-1, keepdims=True)
    inv_std = lax.rsqrt(jnp.mean(centred * centred, axis=-1, keepdims=True) + LN_EPS)
    normed = centred * inv_std
    return normed, inv_std, (normed * gain + bias).astype(BF16)


def bar(*values):
    return lax.optimization_barrier(values)


def solution(mesh):
    group_size = mesh.shape[AXIS_NAME]
    batch_spec = P(AXIS_NAME)
    param_specs = (P(None, AXIS_NAME),) * 14
    swap = [(i, i ^ 1) for i in range(group_size)]
    chips = [[i for i in range(group_size) if i % 2 == c] for c in range(2)]

    def exchange(values):
        return lax.ppermute(values, AXIS_NAME, swap)

    def hop(values, offset):
        return lax.ppermute(values, AXIS_NAME, [(i, i ^ offset) for i in range(group_size)])

    def gather(values):
        return lax.all_gather(values, AXIS_NAME, axis=0, tiled=True)

    def scatter(values):
        return lax.psum_scatter(values, AXIS_NAME, scatter_dimension=0, axis_index_groups=chips, tiled=True)

    def step(hidden, positions, grad_out, *shards):
        (ln_gain, ln_bias, w_query, b_query, w_key, b_key, w_value, b_value, w_out, b_out, w_up, b_up, w_down, b_down) = shards
        layers = ln_gain.shape[0]
        token_total = hidden.shape[0] * hidden.shape[1] * group_size
        rank = lax.axis_index(AXIS_NAME)
        core = lax.rem(rank, 2)
        core_arr = core.reshape(1).astype(jnp.int32)
        tables = rope_tables(positions)

        def rows(w, layer):
            return w[layer].reshape(w.shape[1], -1)

        def blocks(layer):
            return [w_down[layer, b * 128:(b + 1) * 128] for b in range(4)]

        wide0 = gather(join(w_query, w_key, w_value, w_up, w_out, 0))
        second = gather(jnp.concatenate([rows(w_up, 1)] + blocks(0), axis=1))
        third = gather(jnp.concatenate([rows(w, 1) for w in (w_query, w_key, w_value, w_out)] + blocks(1), axis=1))

        small = jnp.concatenate([b.reshape(layers, -1) for b in (ln_gain, ln_bias, b_query, b_key, b_value, b_out, b_down, b_up)], axis=1)
        small = gather(small[None])

        def split(layer):
            mine = small[:, layer]
            vecs = [mine[:, i * 128:(i + 1) * 128].reshape(1, D).astype(F32) for i in range(7)]
            return vecs + [mine[:, 7 * 128:].reshape(1, FF).astype(F32)]

        def mlp_up(h, wup, bu):
            up_pre = nn(h, wup) + bu
            return up_pre, gelu_tanh(up_pre).astype(BF16)

        def norm_pull(grad, grad_normed, normed, inv_std, gain):
            grad_hat = grad_normed * gain
            grad_in = inv_std * (grad_hat - jnp.mean(grad_hat, axis=-1, keepdims=True) - normed * jnp.mean(grad_hat * normed, axis=-1, keepdims=True))
            return (grad.astype(F32) + grad_in).astype(BF16), jnp.sum(grad_normed * normed, axis=0), jnp.sum(grad_normed, axis=0)

        def back_qkv(g, weights, slots=(0, 1, 2)):
            return sum(nt(g[pos], weights[:, pos * D:(pos + 1) * D]) for pos in slots)

        along_x, along_y = lax.rem(rank // 2, 2), rank // 4

        def pick(values, index, axis):
            return lax.dynamic_index_in_dim(values, index, axis, keepdims=False)

        def ring_send(dw):
            parts = dw.reshape(2, 2, 2, dw.shape[0] // 8, dw.shape[1])
            first, second = parts[:, :, 0], parts[:, :, 1]
            send_first, send_second = pick(first, 1 - along_x, 1), pick(second, 1 - along_y, 0)
            got_first = hop(send_first, 2)
            got_second = hop(send_second, 4)
            return dw, got_first, got_second

        def ring_turn(dw, got_first, got_second):
            parts = dw.reshape(2, 2, 2, dw.shape[0] // 8, dw.shape[1])
            first, second = parts[:, :, 0], parts[:, :, 1]
            sum_first = pick(first, along_x, 1) + got_first
            sum_second = pick(second, along_y, 0) + got_second
            kept = pick(sum_first, along_y, 0), pick(sum_second, along_x, 0)
            return kept + (hop(pick(sum_first, 1 - along_y, 0), 4), hop(pick(sum_second, 1 - along_x, 0), 2))

        def ring_end(kept_first, kept_second, got_first, got_second):
            return jnp.concatenate([kept_first + got_first, kept_second + got_second], axis=0)

        def pack(g_gain, g_lbias, g_bias, grad, g_b_up):
            g_bias = g_bias[0].reshape(STEPS, 3, GW)
            pieces = [g_gain, g_lbias] + [g_bias[:, i].reshape(D) for i in range(3)] + [jnp.sum(grad.astype(F32), axis=0)]
            return jnp.concatenate([p.reshape(8, 128) for p in pieces] + [g_b_up.reshape(8, 512)], axis=1)

        up_cols = slice(3 * D, 3 * D + FF)
        out_cols = slice(3 * D + FF, 4 * D + FF)

        def base_sum(x, mixed, wout, bo):
            return x.astype(F32) + nn(mixed, wout) + bo

        x0 = hidden.reshape(SEQ, D)
        gain0, lbias0, bq, bk, bv, bo, bd, bu = split(0)
        normed0, inv0, h0 = layer_norm(x0, gain0, lbias0)
        qkv0, mixed0, lse0 = attn_fwd(h0, wide0, (bq, bk, bv), tables)
        mixed0, h0_a = bar(mixed0, h0)
        up_pre0, act0 = mlp_up(h0_a, wide0[:, up_cols], bu)
        base0, act0 = bar(base_sum(x0, mixed0, wide0[:, out_cols], bo), act0)
        x1 = finish(base0, act0, (second, 1), bd)
        h0x, act0x, mixed0x = exchange(h0), exchange(act0), exchange(mixed0)

        top = grad_out.reshape(SEQ, D)
        topx = exchange(top)
        gain1, lbias1, bq, bk, bv, bo1, bd1, bu = split(1)
        normed1, inv1, h1 = layer_norm(x1, gain1, lbias1)
        up_pre1, act1 = mlp_up(h1, second[:, :FF], bu)
        h1x, act1x = exchange(h1), exchange(act1)
        dw, top_a = bar(wgrad_rows(core_arr, act1, act1x, top, topx), top)
        rs_down1 = scatter(dw)
        pre1, g_bup1 = mlp_pull(top_a, (third, 1), up_pre1)
        pre1x = exchange(pre1)
        pre1_a, h1_a = bar(pre1, h1)
        qkv1, mixed1, lse1 = attn_fwd(h1_a, third, (bq, bk, bv), tables)
        mixed1, pre1_b = bar(mixed1, pre1_a)
        mixed1x = exchange(mixed1)
        dw, top_b = bar(wgrad_cols(core_arr, [(h1, h1x)], [(0, pre1_b, pre1x)]), top_a)
        rs_up1 = scatter(dw)
        g1, g_bias1 = attn_bwd(qkv1, nt(top_b, third[:, 3 * D:4 * D]).astype(BF16), lse1, tables)
        g1x = exchange(g1)
        g1_b, back1 = bar(g1, back_qkv(g1, third, (0, 1)))
        dw, g1_c, back1, pre1_c = bar(wgrad_cols(core_arr, [(h1, h1x), (mixed1, mixed1x)], [(0, g1_b, g1x), (1, top, topx)]), g1_b, back1, pre1_b)
        rs_qkvo1 = scatter(dw)
        mid, g_gain, g_lbias = norm_pull(top, back1 + back_qkv(g1_c, third, (2,)) + nt(pre1_c, second[:, :FF]), normed1, inv1, gain1)
        little1 = pack(g_gain, g_lbias, g_bias1, top, g_bup1)

        midx = exchange(mid)
        mid, midx = bar(mid, midx)
        pre0, g_bup0 = mlp_pull(mid, (second, 1), up_pre0)
        pre0x = exchange(pre0)
        pre0_a, mid_a = bar(pre0, mid)
        sent = ring_send(wgrad_rows(core_arr, act0, act0x, mid_a, midx))
        mid_b, pre0_b = mid_a, pre0_a
        go0 = nt(mid_b, wide0[:, out_cols]).astype(BF16)
        dw = wgrad_cols(core_arr, [(h0, h0x)], [(0, pre0_b, pre0x)])
        dw, go0 = bar(dw, go0)
        rs_up0 = scatter(dw)
        g0, g_bias0 = attn_bwd(qkv0, go0, lse0, tables)
        g0x = exchange(g0)
        *sent, g0_a, pre0_c = bar(*sent, g0, pre0_b)
        turned = ring_turn(*sent)
        g0_b, back0 = bar(g0_a, nt(pre0_c, wide0[:, up_cols]))
        dw = wgrad_cols(core_arr, [(h0, h0x), (mixed0, mixed0x)], [(0, g0_b, g0x), (1, mid_b, midx)])
        dw, g0_c, back0, mixed1_b, act1_b = bar(dw, g0_b, back0, mixed1, act1)
        rs_qkvo0 = scatter(dw)
        grad, g_gain, g_lbias = norm_pull(mid, back0 + back_qkv(g0_c, wide0), normed0, inv0, gain0)
        *turned, grad = bar(*turned, grad)
        rs_down0 = ring_end(*turned)
        little0 = pack(g_gain, g_lbias, g_bias0, mid, g_bup0)
        current = finish(base_sum(x1, mixed1_b, third[:, 3 * D:4 * D], bo1), act1_b, (third, 1), bd1)
        little = [little0, little1]

        scale = 1.0 / token_total
        everyone = gather(jnp.stack(little, axis=1)[None])
        own = jnp.sum(lax.dynamic_index_in_dim(everyone, rank, 1, keepdims=False), axis=0) * scale
        vec = [own[:, i * 128:(i + 1) * 128] for i in range(6)]

        done = unpack([(rs_qkvo1, 0), (rs_qkvo1, 1), (rs_qkvo1, 2), (rs_up1, 0), (rs_qkvo1, 3)], 1, scale)
        done = unpack([(rs_qkvo0, 0), (rs_qkvo0, 1), (rs_qkvo0, 2), (rs_up0, 0), (rs_qkvo0, 3)], 0, scale, done)
        g_query, g_key, g_value = [g.reshape(layers, 16, HEAD, 128).transpose(0, 3, 1, 2) for g in done[:3]]

        return (current.reshape(hidden.shape), grad.reshape(hidden.shape), vec[0], vec[1],
                g_query, vec[2], g_key, vec[3], g_value, vec[4],
                done[4], vec[5],
                done[3], own[:, 6 * 128:], jnp.stack([rs_down0 * scale, rs_down1 * scale]), vec[5])

    return jax.shard_map(step, mesh=mesh, in_specs=(batch_spec, P(), batch_spec) + param_specs, out_specs=(batch_spec, batch_spec) + param_specs, check_vma=False)
```
